8 devices in a mesh: batch: 1 (over z), col: 2 (over y), row: 4 (over x, core).
Axes of the slice: x: 2, y: 2, z: 1, core: 2. Of those that a mesh axis runs over, the one named last changes fastest.
Arguments:
- field: float32 [2048, 1024, 4], P(('batch', 'row'), 'col')
- x_lower: float32 [2048, 1024], P(('batch', 'row'), 'col')
- x_diag: float32 [2048, 1024], P(('batch', 'row'), 'col')
- x_upper: float32 [2048, 1024], P(('batch', 'row'), 'col')
- y_lower: float32 [2048, 1024], P(('batch', 'row'), 'col')
- y_diag: float32 [2048, 1024], P(('batch', 'row'), 'col')
- y_upper: float32 [2048, 1024], P(('batch', 'row'), 'col')
Outputs:
- output: float32 [2048, 1024, 4], P(('batch', 'row'), 'col')
All inputs are finite; a program needn't handle non-finite values.
Results may differ from the reference program's by a relative error of at most 0.001.
Values sent between devices are 32-bit elements.
A program may use at most 1 GiB of HBM per device.

```python
import jax
import jax.numpy as jnp
from jax import lax

NX = 2048
NY = 1024
F = 4


def stiffness_map(freq_x, freq_y):
    pos_x = jnp.arange(NX, dtype=jnp.float32)[:, None] / NX
    pos_y = jnp.arange(NY, dtype=jnp.float32)[None, :] / NY
    wave = jnp.sin(2.0 * jnp.pi * (freq_x * pos_x + freq_y * pos_y))
    return 8.0 * jnp.exp(jnp.log(32.0) * (0.5 + 0.5 * wave))


def line_coeffs(base_key, strength):
    key_low, key_up, key_diag = jax.random.split(base_key, 3)
    lower = -strength * (0.4 + 0.1 * jax.random.uniform(key_low, (NX, NY), jnp.float32))
    upper = -strength * (0.4 + 0.1 * jax.random.uniform(key_up, (NX, NY), jnp.float32))
    diagonal = strength * (1.0 + 0.2 * jax.random.uniform(key_diag, (NX, NY), jnp.float32)) + 0.1
    return lower, diagonal, upper


def setup_inputs(seed: int = 0, part: int = 0) -> dict:
    base_key = jax.random.fold_in(jax.random.key(seed), part)
    key_field, key_x, key_y = jax.random.split(base_key, 3)
    x_lower, x_diag, x_upper = line_coeffs(key_x, stiffness_map(2.0, 1.0))
    y_lower, y_diag, y_upper = line_coeffs(key_y, stiffness_map(1.0, 3.0))
    field = jax.random.normal(key_field, (NX, NY, F), jnp.float32)
    return {"field": field, "x_lower": x_lower, "x_diag": x_diag, "x_upper": x_upper,
            "y_lower": y_lower, "y_diag": y_diag, "y_upper": y_upper}


def thomas_solve(lower, main, upper, rhs):
    def forward(state, row_in):
        prev_cp, prev_g = state
        low_row, mid_row, upp_row, rhs_row = row_in
        denom = mid_row - low_row * prev_cp
        next_cp = upp_row / denom
        next_g = (rhs_row - low_row[..., None] * prev_g) / denom[..., None]
        return (next_cp, next_g), (next_cp, next_g)
    start = (jnp.zeros(rhs.shape[1:-1], jnp.float32), jnp.zeros(rhs.shape[1:], jnp.float32))
    _, (all_cp, all_g) = lax.scan(forward, start, (lower, main, upper, rhs))

    def backward(next_x, row_in):
        cp_row, g_row = row_in
        value = g_row - cp_row[..., None] * next_x
        return value, value
    _, solved = lax.scan(backward, jnp.zeros(rhs.shape[1:], jnp.float32), (all_cp, all_g), reverse=True)
    return solved


def reference(field, x_lower, x_diag, x_upper, y_lower, y_diag, y_upper):
    zero_col = jnp.zeros((NX, 1, F), jnp.float32)
    next_y = jnp.concatenate([field[:, 1:], zero_col], axis=1)
    prev_y = jnp.concatenate([zero_col, field[:, :-1]], axis=1)
    rhs_one = field - (y_lower[:, :, None] * prev_y + y_diag[:, :, None] * field + y_upper[:, :, None] * next_y)
    shift_val = -(1.0 + x_diag[0])
    corner_up = x_lower[0]
    corner_low = x_upper[NX - 1]
    main_x = (1.0 + x_diag).at[0].add(-shift_val).at[NX - 1].add(-(corner_low * corner_up / shift_val))
    extra_rhs = jnp.zeros((NX, NY), jnp.float32).at[0].set(shift_val).at[NX - 1].set(corner_low)
    solved = thomas_solve(x_lower, main_x, x_upper, jnp.concatenate([rhs_one, extra_rhs[:, :, None]], axis=2))
    y_sol = solved[:, :, :F]
    z_sol = solved[:, :, F:]
    ratio = (corner_up / shift_val)[:, None]
    sm_factor = (y_sol[0] + ratio * y_sol[NX - 1]) / (1.0 + z_sol[0] + ratio * z_sol[NX - 1])
    u_star = y_sol - z_sol * sm_factor[None]
    prev_x = jnp.roll(u_star, 1, axis=0)
    next_x = jnp.roll(u_star, -1, axis=0)
    rhs_two = u_star - (x_lower[:, :, None] * prev_x + x_diag[:, :, None] * u_star + x_upper[:, :, None] * next_x)
    sol_t = thomas_solve(y_lower.T, 1.0 + y_diag.T, y_upper.T, jnp.swapaxes(rhs_two, 0, 1))
    return jnp.swapaxes(sol_t, 0, 1)
```

```python
import functools

import jax
import jax.numpy as jnp
from jax import lax
from jax.experimental import pallas as pl
from jax.experimental.pallas import tpu as pltpu
from jax.sharding import PartitionSpec as P

MESH = pl.DeviceIdType.MESH
F32 = jnp.float32

T = 512
F = 4
C = 65
PAD = 8
ROWS = T + PAD
NB = T // 128
UNROLL = 5

DIAG, LOW, UPP = 0, 1, 2
INV, NA, NC, V, PR = 0, 1, 2, 3, 4


def join(left, right):
    la0, la1, la2, lb0, lb1, lb2 = left
    ra0, ra1, ra2, rb0, rb1, rb2 = right
    inv = 1.0 / (1.0 - ra1 * lb2)
    e0 = inv * (ra0 + ra1 * lb0)
    e1 = inv * (ra1 * lb1)
    e2 = inv * ra2
    m0 = lb0 + lb2 * e0
    m1 = lb1 + lb2 * e1
    m2 = lb2 * e2
    whole = (la0 + la2 * e0, la1 + la2 * e1, la2 * e2, rb0 + rb1 * m0, rb1 * m1, rb2 + rb1 * m2)
    return whole, (e0, e1, e2), (m0, m1, m2)


def chunk_rows(t):
    return pl.ds(t, 8, stride=C)


def factor(k, summ):
    sub = lax.broadcasted_iota(jnp.int32, (8, 128), 0)
    zero = jnp.zeros((8, 128), F32)

    def step(t, state):
        out = []
        for b in range(NB):
            nc, v, pr, f1 = state[4 * b:4 * b + 4]
            rows = chunk_rows(t)
            low = k[LOW, b, rows, :]
            den = (1.0 + k[DIAG, b, rows, :]) + low * nc
            inv = 1.0 / den
            na = -(low * inv)
            nc = -(k[UPP, b, rows, :] * inv)
            v = na * v
            k[INV, b, rows, :] = inv
            k[NA, b, rows, :] = na
            k[NC, b, rows, :] = nc
            k[V, b, rows, :] = v
            k[PR, b, rows, :] = pr
            f1 = f1 + pr * v
            pr = pr * nc
            out += [nc, v, pr, f1]
        return tuple(out)

    state = (zero, zero + 1.0, jnp.where(sub == 0, 0.0, 1.0), zero) * NB
    state = lax.fori_loop(0, PAD, step, state)
    state = list(state)
    for b in range(NB):
        state[4 * b + 2] = jnp.where(sub == 0, 1.0, state[4 * b + 2])
    state = lax.fori_loop(PAD, C, step, tuple(state))
    for b in range(NB):
        nc, v, pr, f1 = state[4 * b:4 * b + 4]
        for f in range(F):
            r = f * NB + b
            summ[1 * 16 + r] = f1
            summ[2 * 16 + r] = pr
            summ[4 * 16 + r] = v
            summ[5 * 16 + r] = nc


def forward(k, rhs_of, g, summ):
    zero = jnp.zeros((8, 128), F32)

    def step(t, state):
        state = list(state)
        rows = chunk_rows(t)
        for b, rhs in rhs_of(t):
            inv = k[INV, b, rows, :]
            na = k[NA, b, rows, :]
            pr = k[PR, b, rows, :]
            for f in range(F):
                n = 2 * (f * NB + b)
                gv = inv * rhs[f] + na * state[n]
                g[b, f, rows, :] = gv
                state[n] = gv
                state[n + 1] = state[n + 1] + pr * gv
        return tuple(state)

    def steps(i, state):
        for u in range(UNROLL):
            state = step(i * UNROLL + u, state)
        return state

    state = lax.fori_loop(0, C // UNROLL, steps, (zero,) * (2 * F * NB))
    for r in range(F * NB):
        summ[0 * 16 + r] = state[2 * r + 1]
        summ[3 * 16 + r] = state[2 * r]


def reduce_chunks(summ2, send):
    def chunk(s):
        return tuple(summ2[pl.ds(q * 128 + s, 16, stride=8), :] for q in range(6))
    whole = chunk(0)
    inner = []
    for s in range(1, 8):
        whole, e, m = join(whole, chunk(s))
        inner.append((e, m))
    for q in range(6):
        send[q * 16:(q + 1) * 16, :] = whole[q]
    return whole, inner


def spread(inner, before, after, edge):
    nxt = after
    edge[1, pl.ds(7, 16, stride=8), :] = after
    edge[0, pl.ds(0, 16, stride=8), :] = before
    for s in range(7, 0, -1):
        e, m = inner[s - 1]
        last = m[0] + m[1] * before + m[2] * nxt
        nxt = e[0] + e[1] * before + e[2] * nxt
        edge[0, pl.ds(s, 16, stride=8), :] = last
        edge[1, pl.ds(s - 1, 16, stride=8), :] = nxt


def backward(k, g, edge, put):
    def step(t, state):
        state = list(state)
        rows = chunk_rows(t)
        for b in range(NB):
            v = k[V, b, rows, :]
            nc = k[NC, b, rows, :]
            for f in range(F):
                r = f * NB + b
                x = (g[b, f, rows, :] + v * edge[0, r * 8:r * 8 + 8, :]) + nc * state[r]
                put(b, f, rows, x)
                state[r] = x
        return tuple(state)

    def steps(i, state):
        for u in range(UNROLL):
            state = step(C - 1 - (i * UNROLL + u), state)
        return state

    lax.fori_loop(0, C // UNROLL, steps, tuple(edge[1, r * 8:r * 8 + 8, :] for r in range(F * NB)))


def kernel(row_count, field, xl, xd, xu, yl, yd, yu, out,
           u, xk, yn, yk, r1, g, y, o, summ, edge, pack, send, recv, ysend, yrecv,
           in_sem, out_sem, ps, pr, xs, xr, ys, yr):
    row = lax.axis_index("row")
    col = lax.axis_index("col")
    other = 1 - col
    lane = lax.broadcasted_iota(jnp.int32, (8, 128), 1)
    zero = jnp.zeros((8, 128), F32)
    summ2 = summ.reshape(6 * 128, 128)

    copies = {}
    count = 0
    for name, refs, dst in (("x", (xd, xl, xu), xk), ("u", (field,), u), ("y", (yd, yl, yu), yn)):
        copies[name] = []
        for n, ref in enumerate(refs):
            for b in range(NB):
                if name == "u":
                    cp = pltpu.make_async_copy(ref.at[:, b], dst.at[b, pl.ds(PAD * F, T * F)].reshape(T, F, 128), in_sem.at[count])
                else:
                    cp = pltpu.make_async_copy(ref.at[:, pl.ds(b * 128, 128)], dst.at[n, b, pl.ds(PAD, T)], in_sem.at[count])
                cp.start()
                copies[name].append(cp)
                count += 1

    barrier = pltpu.get_barrier_semaphore()
    for d in range(1, row_count):
        pl.semaphore_signal(barrier, inc=1, device_id={"row": lax.rem(row + d, row_count)}, device_id_type=MESH)
    pl.semaphore_signal(barrier, inc=1, device_id={"col": other}, device_id_type=MESH)
    pl.semaphore_wait(barrier, row_count)

    for b in range(NB):
        for n in range(3):
            yn[n, b, 0:PAD, :] = zero
            xk[n, b, 0:PAD, :] = zero - 1.0 if n == LOW else zero
            yk[n, b, 0:PAD, :] = zero - 1.0 if n == LOW else zero
        for f in range(F):
            y[b, f, 0:PAD, :] = zero
    for b in range(NB + 1):
        for n in range(F):
            u[b, n * 8:n * 8 + 8, :] = zero

    for cp in copies["u"]:
        cp.wait()
    src_block = (NB - 1) * other
    src_lane = 127 * other

    def pack_step(i, acc):
        acc = list(acc)
        for n in range(8):
            p = i * 8 + n
            for h in range(2):
                w = u[src_block, pl.ds(pl.multiple_of(PAD * F + 8 * (h * 128 + p), 8), 8), :]
                w = pltpu.roll(w, lax.rem(p - src_lane + 128, 128), 1)
                acc[h] = jnp.where(lane == p, w, acc[h])
        return tuple(acc)

    packed = lax.fori_loop(0, 16, pack_step, (zero, zero))
    for h in range(2):
        pack[0, h * 8:h * 8 + 8, :] = packed[h]
    column = pltpu.make_async_remote_copy(pack.at[0], pack.at[1], ps, pr, device_id={"col": other}, device_id_type=MESH)
    column.start()

    for cp in copies["x"]:
        cp.wait()
    factor(xk, summ)

    column.wait()
    dst_lane = 127 * col
    here = lane == dst_lane

    def unpack_step(i, carry):
        for n in range(8):
            p = i * 8 + n
            for h in range(2):
                w = pltpu.roll(pack[1, h * 8:h * 8 + 8, :], lax.rem(dst_lane - p + 128, 128), 1)
                u[NB, pl.ds(pl.multiple_of(PAD * F + 8 * (h * 128 + p), 8), 8), :] = jnp.where(here, w, 0.0)
        return carry

    lax.fori_loop(0, 16, unpack_step, 0)
    for cp in copies["y"]:
        cp.wait()

    def rhs_x(t):
        rows = chunk_rows(t)
        def words(b, f):
            return u[b, pl.ds(t * F + f, 8, stride=C * F), :]
        mid = [[words(b, f) for f in range(F)] for b in range(NB)]
        end = [words(NB, f) for f in range(F)]
        up = [[pltpu.roll(v, 127, 1) for v in block] for block in mid + [end]]
        down = [[pltpu.roll(v, 1, 1) for v in block] for block in [end] + mid]
        for b in range(NB):
            cd = 1.0 - yn[DIAG, b, rows, :]
            cl = yn[LOW, b, rows, :]
            cu = yn[UPP, b, rows, :]
            rhs = []
            for f in range(F):
                nxt = jnp.where(lane == 127, up[b + 1][f], up[b][f])
                prv = jnp.where(lane == 0, down[b][f], down[b + 1][f])
                v = (cd * mid[b][f] - cl * prv) - cu * nxt
                r1[b, f, rows, :] = v
                rhs.append(v)
            yield b, rhs

    forward(xk, rhs_x, g, summ)
    whole, inner = reduce_chunks(summ2, send)
    sends = []
    for d in range(1, row_count):
        cp = pltpu.make_async_remote_copy(send, recv.at[d - 1], xs.at[d - 1], xr.at[d - 1],
                                          device_id={"row": lax.rem(row + d, row_count)}, device_id_type=MESH)
        cp.start()
        sends.append(cp)

    def turn_step(i, carry):
        b, c = i // NB, i % NB
        for n in range(3):
            yk[n, c, pl.ds(pl.multiple_of(PAD + b * 128, 8), 128), :] = (
                yn[n, b, pl.ds(pl.multiple_of(PAD + c * 128, 8), 128), :].T)
        return carry

    lax.fori_loop(0, NB * NB, turn_step, 0)
    factor(yk, summ)

    for cp in sends:
        cp.wait()

    def received(n):
        return tuple(recv[n, q * 16:(q + 1) * 16, :] for q in range(6))
    rest = received(row_count - 2)
    for n in range(row_count - 3, -1, -1):
        rest, _, _ = join(rest, received(n))
    a0, a1, a2, b0, b1, b2 = whole
    p0, p1, p2, q0, q1, q2 = rest
    m11 = 1.0 - (p1 * b2 + p2 * a2)
    m12 = p1 * b1 + p2 * a1
    m21 = q1 * b2 + q2 * a2
    m22 = 1.0 - (q1 * b1 + q2 * a1)
    s1 = p0 + p1 * b0 + p2 * a0
    s2 = q0 + q1 * b0 + q2 * a0
    i11 = 1.0 / m11
    before = (s2 + m21 * (i11 * s1)) / (m22 - m21 * (i11 * m12))
    after = i11 * (s1 + m12 * before)
    spread(inner, before, after, edge)

    def put_x(b, f, rows, x):
        r1[b, f, rows, :] = (x + x) - r1[b, f, rows, :]

    backward(xk, g, edge, put_x)

    def turn_in(i, carry):
        b, c = i // NB, i % NB
        for f in range(F):
            y[c, f, pl.ds(pl.multiple_of(PAD + b * 128, 8), 128), :] = (
                r1[b, f, pl.ds(pl.multiple_of(PAD + c * 128, 8), 128), :].T)
        return carry

    lax.fori_loop(0, NB * NB, turn_in, 0)

    def rhs_y(t):
        rows = chunk_rows(t)
        for b in range(NB):
            yield b, [y[b, f, rows, :] for f in range(F)]

    forward(yk, rhs_y, g, summ)
    whole, inner = reduce_chunks(summ2, ysend)
    cp = pltpu.make_async_remote_copy(ysend, yrecv, ys, yr, device_id={"col": other}, device_id_type=MESH)
    cp.start()
    cp.wait()
    theirs = tuple(yrecv[q * 16:(q + 1) * 16, :] for q in range(6))
    first = col == 0
    left = [jnp.where(first, a, b) for a, b in zip(whole, theirs)]
    right = [jnp.where(first, b, a) for a, b in zip(whole, theirs)]
    last_left = (left[3] + left[5] * right[0]) / (1.0 - left[5] * right[1])
    first_right = right[0] + right[1] * last_left
    spread(inner, jnp.where(first, 0.0, last_left), jnp.where(first, first_right, 0.0), edge)

    def put_y(b, f, rows, x):
        y[b, f, rows, :] = x

    backward(yk, g, edge, put_y)

    def turn_out(i, carry):
        b, c = i // NB, i % NB
        for f in range(F):
            o[b, pl.ds(c * 128 * F + f, 128, stride=F), :] = (
                y[c, f, pl.ds(pl.multiple_of(PAD + b * 128, 8), 128), :].T)
        return carry

    outs = []
    for b in range(NB):
        lax.fori_loop(b * NB, b * NB + NB, turn_out, 0)
        cp = pltpu.make_async_copy(o.at[b].reshape(T, F, 128), out.at[:, b], out_sem.at[b])
        cp.start()
        outs.append(cp)
    for cp in outs:
        cp.wait()


def solution(mesh):
    row_count = mesh.shape["row"]
    field_spec = P(("batch", "row"), "col", None)
    coef_spec = P(("batch", "row"), "col")

    def local_step(field, x_lower, x_diag, x_upper, y_lower, y_diag, y_upper):
        words = field.reshape(T, NB, 128, F).transpose(0, 1, 3, 2)
        plane = (NB, ROWS, 128)
        solved = pl.pallas_call(
            functools.partial(kernel, row_count),
            out_shape=jax.ShapeDtypeStruct((T, NB, F, 128), F32),
            in_specs=[pl.BlockSpec(memory_space=pl.ANY)] * 7,
            out_specs=pl.BlockSpec(memory_space=pl.ANY),
            scratch_shapes=[
                pltpu.VMEM((NB + 1, ROWS * F, 128), F32),
                pltpu.VMEM((5,) + plane, F32),
                pltpu.VMEM((3,) + plane, F32),
                pltpu.VMEM((5,) + plane, F32),
                pltpu.VMEM((NB, F, ROWS, 128), F32),
                pltpu.VMEM((NB, F, ROWS, 128), F32),
                pltpu.VMEM((NB, F, ROWS, 128), F32),
                pltpu.VMEM((NB, T * F, 128), F32),
                pltpu.VMEM((96, 8, 128), F32),
                pltpu.VMEM((2, 128, 128), F32),
                pltpu.VMEM((2, 16, 128), F32),
                pltpu.VMEM((96, 128), F32),
                pltpu.VMEM((row_count - 1, 96, 128), F32),
                pltpu.VMEM((96, 128), F32),
                pltpu.VMEM((96, 128), F32),
                pltpu.SemaphoreType.DMA((28,)),
                pltpu.SemaphoreType.DMA((NB,)),
                pltpu.SemaphoreType.DMA,
                pltpu.SemaphoreType.DMA,
                pltpu.SemaphoreType.DMA((row_count - 1,)),
                pltpu.SemaphoreType.DMA((row_count - 1,)),
                pltpu.SemaphoreType.DMA,
                pltpu.SemaphoreType.DMA,
            ],
            compiler_params=pltpu.CompilerParams(
                collective_id=0, has_side_effects=True, vmem_limit_bytes=60 * 1024 * 1024),
        )(words, x_lower, x_diag, x_upper, y_lower, y_diag, y_upper)
        return solved.transpose(0, 1, 3, 2).reshape(T, T, F)

    return jax.shard_map(local_step, mesh=mesh, in_specs=(field_spec,) + (coef_spec,) * 6,
                         out_specs=field_spec, check_vma=False)
```

```python
import functools

import jax
import jax.numpy as jnp
from jax import lax
from jax.experimental import pallas as pl
from jax.experimental.pallas import tpu as pltpu
from jax.sharding import PartitionSpec as P

MESH = pl.DeviceIdType.MESH
F32 = jnp.float32

T = 512
F = 4
C = 65
PAD = 8
ROWS = T + PAD
NB = T // 128
R = F * NB
UNROLL = 5

DIAG, LOW, UPP = 0, 1, 2
INV, NA, PR = 0, 1, 2
V, NC = 0, 1
A0, A1, A2, B0, B1, B2 = range(6)


def chunk_rows(t):
    return pl.ds(t, 8, stride=C)


def factor(k, kb, summ):
    sub = lax.broadcasted_iota(jnp.int32, (8, 128), 0)
    zero = jnp.zeros((8, 128), F32)

    def step(t, state):
        out = []
        for b in range(NB):
            nc, v, pr, a1 = state[4 * b:4 * b + 4]
            rows = chunk_rows(t)
            low = k[LOW, b, rows, :]
            den = (1.0 + k[DIAG, b, rows, :]) + low * nc
            inv = 1.0 / den
            na = -(low * inv)
            nc = -(k[UPP, b, rows, :] * inv)
            v = na * v
            k[INV, b, rows, :] = inv
            k[NA, b, rows, :] = na
            k[PR, b, rows, :] = pr
            kb[NC, b, rows, :] = nc
            kb[V, b, rows, :] = v
            a1 = a1 + pr * v
            pr = pr * nc
            out += [nc, v, pr, a1]
        return tuple(out)

    state = (zero, zero + 1.0, jnp.where(sub == 0, 0.0, 1.0), zero) * NB
    state = lax.fori_loop(0, PAD, step, state)
    state = list(state)
    for b in range(NB):
        state[4 * b + 2] = jnp.where(sub == 0, 1.0, state[4 * b + 2])
    state = lax.fori_loop(PAD, C, step, tuple(state))
    for b in range(NB):
        nc, v, pr, a1 = state[4 * b:4 * b + 4]
        for f in range(F):
            r = f * NB + b
            summ[A1 * R + r] = a1
            summ[A2 * R + r] = pr
            summ[B1 * R + r] = v
            summ[B2 * R + r] = nc


def of_chunk(summ, q, s):
    return summ.reshape(6 * R * 8, 128)[pl.ds(q * R * 8 + s, R, stride=8), :]


def join_coef(la1, la2, lb1, lb2, ra1, ra2, rb1, rb2):
    inv = 1.0 / (1.0 - ra1 * lb2)
    w = inv * ra1
    e1 = w * lb1
    e2 = inv * ra2
    m1 = lb1 + lb2 * e1
    m2 = lb2 * e2
    return (la1 + la2 * e1, la2 * e2, rb1 * m1, rb2 + rb1 * m2), (inv, w, lb2, la2, rb1), (e1, e2, m1, m2)


def join_rhs(part, la0, lb0, ra0, rb0):
    inv, w, lb2, la2, rb1 = part
    e0 = inv * ra0 + w * lb0
    m0 = lb0 + lb2 * e0
    return la0 + la2 * e0, rb0 + rb1 * m0, e0, m0


def reduce_coef(summ, co, send):
    def chunk(s):
        return tuple(of_chunk(summ, q, s) for q in (A1, A2, B1, B2))
    whole = chunk(0)
    for s in range(1, 8):
        whole, part, inner = join_coef(*whole, *chunk(s))
        for n, v in enumerate(part + inner):
            co[s - 1, n] = v
    for n, v in enumerate(whole):
        co[7, n] = v
        send[n * 8:n * 8 + 8, :] = v[0:8]


def reduce_rhs(summ, co, send):
    a0, b0 = of_chunk(summ, A0, 0), of_chunk(summ, B0, 0)
    for s in range(1, 8):
        part = tuple(co[s - 1, n] for n in range(5))
        a0, b0, e0, m0 = join_rhs(part, a0, b0, of_chunk(summ, A0, s), of_chunk(summ, B0, s))
        co[s - 1, 9] = e0
        co[s - 1, 10] = m0
    send[0:R, :] = a0
    send[R:2 * R, :] = b0
    return a0, b0


def spread(co, before, after, edge):
    nxt = after
    edge[1, pl.ds(7, R, stride=8), :] = after
    edge[0, pl.ds(0, R, stride=8), :] = before
    for s in range(7, 0, -1):
        e1, e2, m1, m2, e0, m0 = (co[s - 1, n] for n in range(5, 11))
        edge[0, pl.ds(s, R, stride=8), :] = (m0 + m1 * before) + m2 * nxt
        nxt = (e0 + e1 * before) + e2 * nxt
        edge[1, pl.ds(s - 1, R, stride=8), :] = nxt


def sweep(blocks, step, state, unroll=UNROLL):
    def steps(i, state):
        for n in range(unroll):
            state = step(blocks, i * unroll + n, state)
        return state
    return lax.fori_loop(0, C // unroll, steps, state)


def forward(k, rhs_of, g, summ, group, unroll=UNROLL):
    zero = jnp.zeros((8, 128), F32)

    def step(blocks, t, state):
        out = []
        rows = chunk_rows(t)
        for j, b in enumerate(blocks):
            inv = k[INV, b, rows, :]
            na = k[NA, b, rows, :]
            pr = k[PR, b, rows, :]
            rhs = rhs_of(t, b)
            for f in range(F):
                last, first = state[2 * (j * F + f):2 * (j * F + f) + 2]
                last = inv * rhs[f] + na * last
                g[b, f, rows, :] = last
                out += [last, first + pr * last]
        return tuple(out)

    for b in range(0, NB, group):
        blocks = range(b, b + group)
        state = sweep(blocks, step, (zero,) * (2 * F * group), unroll)
        for j, c in enumerate(blocks):
            for f in range(F):
                summ[B0 * R + f * NB + c] = state[2 * (j * F + f)]
                summ[A0 * R + f * NB + c] = state[2 * (j * F + f) + 1]


def backward(kb, g, edge, put, group):
    def beside(side, b, f):
        r = f * NB + b
        return edge[side, r * 8:r * 8 + 8, :]

    def step(blocks, n, state):
        out = []
        rows = chunk_rows(C - 1 - n)
        for j, b in enumerate(blocks):
            v = kb[V, b, rows, :]
            nc = kb[NC, b, rows, :]
            for f in range(F):
                x = (g[b, f, rows, :] + v * beside(0, b, f)) + nc * state[j * F + f]
                put(b, f, rows, x)
                out.append(x)
        return tuple(out)

    for b in range(0, NB, group):
        blocks = range(b, b + group)
        sweep(blocks, step, tuple(beside(1, c, f) for c in blocks for f in range(F)))


def main_kernel(row_count, field, xl, xd, xu, yl, yd, yu, g, yb, edge,
                u, xk, xb, yn, yk, r1, y, sx, sy, cx, cy, pack,
                xcs, xcr, xrs, xrr, ycs, ycr, yrs, yrr,
                in_sem, ps, pr, xcss, xcrs, xrss, xrrs, yss, yrsem):
    row = lax.axis_index("row")
    col = lax.axis_index("col")
    other = 1 - col
    lane = lax.broadcasted_iota(jnp.int32, (8, 128), 1)
    zero = jnp.zeros((8, 128), F32)
    src_block = (NB - 1) * other
    src_lane = 127 * other
    dst_lane = 127 * col

    count = 0

    def fetch(src, dst):
        nonlocal count
        cp = pltpu.make_async_copy(src, dst, in_sem.at[count])
        cp.start()
        count += 1
        return cp

    def fetch_field(b):
        return fetch(field.at[:, b], u.at[b, pl.ds(PAD * F, T * F)].reshape(T, F, 128))

    def fetch_coef(refs, dst):
        return [fetch(ref.at[:, pl.ds(b * 128, 128)], dst.at[n, b, pl.ds(PAD, T)]) for n, ref in enumerate(refs) for b in range(NB)]

    in_edge = fetch_field(src_block)
    in_x = fetch_coef((xd, xl, xu), xk)
    in_u = [fetch_field(lax.rem(src_block + d, NB)) for d in range(1, NB)]
    in_y = fetch_coef((yd, yl, yu), yn)

    barrier = pltpu.get_barrier_semaphore()
    for d in range(1, row_count):
        pl.semaphore_signal(barrier, inc=1, device_id={"row": lax.rem(row + d, row_count)}, device_id_type=MESH)
    pl.semaphore_signal(barrier, inc=1, device_id={"col": other}, device_id_type=MESH)

    for b in range(NB):
        for n in range(3):
            yn[n, b, 0:PAD, :] = zero
            xk[n, b, 0:PAD, :] = zero - 1.0 if n == LOW else zero
            yk[n, b, 0:PAD, :] = zero - 1.0 if n == LOW else zero
        for f in range(F):
            y[b, f, 0:PAD, :] = zero
    for b in range(NB + 1):
        for n in range(F):
            u[b, n * 8:n * 8 + 8, :] = zero

    in_edge.wait()
    from_src = jnp.bitwise_and(lane - src_lane, 127)
    for h in range(2):
        acc = zero
        for p in range(128):
            w = PAD * F + 8 * (h * 128 + p)
            acc = jnp.where(from_src == p, pltpu.roll(u[src_block, w:w + 8, :], p, 1), acc)
        pack[0, h * 8:h * 8 + 8, :] = acc
    pl.semaphore_wait(barrier, row_count)
    column = pltpu.make_async_remote_copy(pack.at[0], pack.at[1], ps, pr, device_id={"col": other}, device_id_type=MESH)
    column.start()

    def to_line(send, recv, send_sem, recv_sem):
        copies = []
        for d in range(1, row_count):
            cp = pltpu.make_async_remote_copy(send, recv.at[d - 1], send_sem.at[d - 1], recv_sem.at[d - 1],
                                              device_id={"row": lax.rem(row + d, row_count)}, device_id_type=MESH)
            cp.start()
            copies.append(cp)
        return copies

    def to_pair(n, send, recv):
        cp = pltpu.make_async_remote_copy(send, recv, yss.at[n], yrsem.at[n], device_id={"col": other}, device_id_type=MESH)
        cp.start()
        return cp

    for cp in in_x:
        cp.wait()
    factor(xk, xb, sx)
    reduce_coef(sx, cx, xcs)
    coef_sends = to_line(xcs, xcr, xcss, xcrs)

    column.wait()
    here = lane == dst_lane

    for h in range(2):
        got = pack[1, h * 8:h * 8 + 8, :]
        for p in range(128):
            w = PAD * F + 8 * (h * 128 + p)
            u[NB, w:w + 8, :] = jnp.where(here, pltpu.roll(got, (128 - p) % 128, 1), 0.0)
    for cp in in_u + in_y:
        cp.wait()

    def rhs_x(t, b):
        rows = chunk_rows(t)
        cd = 1.0 - yn[DIAG, b, rows, :]
        cl = yn[LOW, b, rows, :]
        cu = yn[UPP, b, rows, :]
        rhs = []
        for f in range(F):
            words = pl.ds(t * F + f, 8, stride=C * F)
            mid = u[b, words, :]
            prv = pltpu.roll(jnp.where(lane == 127, u[b - 1 if b else NB, words, :], mid), 1, 1)
            nxt = pltpu.roll(jnp.where(lane == 0, u[b + 1, words, :], mid), 127, 1)
            v = (cd * mid - cl * prv) - cu * nxt
            r1[b, f, rows, :] = v
            rhs.append(v)
        return rhs

    forward(xk, rhs_x, g, sx, 1, 13)
    a0, b0 = reduce_rhs(sx, cx, xrs)
    rhs_sends = to_line(xrs, xrr, xrss, xrrs)

    def turn_step(i, carry):
        b, c = i // NB, i % NB
        for n in range(3):
            yk[n, c, pl.ds(pl.multiple_of(PAD + b * 128, 8), 128), :] = (
                yn[n, b, pl.ds(pl.multiple_of(PAD + c * 128, 8), 128), :].T)
        return carry

    lax.fori_loop(0, NB * NB, turn_step, 0)
    factor(yk, yb, sy)
    reduce_coef(sy, cy, ycs)
    y_coef = to_pair(0, ycs, ycr)

    for cp in coef_sends:
        cp.wait()

    def coef_of(ref, n=None):
        view = ref if n is None else ref.at[n]
        return tuple(jnp.concatenate([view[q * 8:q * 8 + 8, :]] * 2, axis=0) for q in range(4))

    rest = coef_of(xcr, row_count - 2)
    parts = []
    for n in range(row_count - 3, -1, -1):
        rest, part, _ = join_coef(*rest, *coef_of(xcr, n))
        parts.append(part)
    p1, p2, q1, q2 = rest
    a1, a2, b1, b2 = (cx[7, n] for n in range(4))
    m12 = p1 * b1 + p2 * a1
    m21 = q1 * b2 + q2 * a2
    i11 = 1.0 / (1.0 - (p1 * b2 + p2 * a2))
    m21 = m21 * i11
    i22 = 1.0 / ((1.0 - (q1 * b1 + q2 * a1)) - m21 * m12)

    for cp in rhs_sends:
        cp.wait()
    p0, q0 = xrr[row_count - 2, 0:R, :], xrr[row_count - 2, R:2 * R, :]
    for part, n in zip(parts, range(row_count - 3, -1, -1)):
        p0, q0, _, _ = join_rhs(part, p0, q0, xrr[n, 0:R, :], xrr[n, R:2 * R, :])
    s1 = (p0 + p1 * b0) + p2 * a0
    s2 = (q0 + q1 * b0) + q2 * a0
    before = i22 * (s2 + m21 * s1)
    after = i11 * (s1 + m12 * before)
    spread(cx, before, after, edge)

    def put_x(b, f, rows, x):
        r1[b, f, rows, :] = (x + x) - r1[b, f, rows, :]

    backward(xb, g, edge, put_x, 2)

    def turn_in(i, carry):
        b, c = i // NB, i % NB
        for f in range(F):
            y[c, f, pl.ds(pl.multiple_of(PAD + b * 128, 8), 128), :] = (
                r1[b, f, pl.ds(pl.multiple_of(PAD + c * 128, 8), 128), :].T)
        return carry

    lax.fori_loop(0, NB * NB, turn_in, 0)

    def rhs_y(t, b):
        return [y[b, f, chunk_rows(t), :] for f in range(F)]

    forward(yk, rhs_y, g, sy, 2)
    a0, b0 = reduce_rhs(sy, cy, yrs)
    y_rhs = to_pair(1, yrs, yrr)

    y_coef.wait()
    first = col == 0
    a1, a2, b1, b2 = (cy[7, n] for n in range(4))
    c1, c2, d1, d2 = coef_of(ycr)
    lb2 = jnp.where(first, b2, d2)
    ra1 = jnp.where(first, c1, a1)
    inv = 1.0 / (1.0 - lb2 * ra1)
    y_rhs.wait()
    c0, d0 = yrr[0:R, :], yrr[R:2 * R, :]
    lb0 = jnp.where(first, b0, d0)
    ra0 = jnp.where(first, c0, a0)
    last_left = inv * (lb0 + lb2 * ra0)
    first_right = ra0 + ra1 * last_left
    spread(cy, jnp.where(first, 0.0, last_left), jnp.where(first, first_right, 0.0), edge)


def last_kernel(g, yb, edge, out, y, o, out_sem):
    def put_y(b, f, rows, x):
        y[b, f, rows, :] = x

    backward(yb, g, edge, put_y, 2)

    def turn_out(i, carry):
        b, c = i // NB, i % NB
        for f in range(F):
            o[b, pl.ds(c * 128 * F + f, 128, stride=F), :] = (
                y[c, f, pl.ds(pl.multiple_of(PAD + b * 128, 8), 128), :].T)
        return carry

    outs = []
    for b in range(NB):
        lax.fori_loop(b * NB, b * NB + NB, turn_out, 0)
        cp = pltpu.make_async_copy(o.at[b].reshape(T, F, 128), out.at[:, b], out_sem.at[b])
        cp.start()
        outs.append(cp)
    for cp in outs:
        cp.wait()


def solution(mesh):
    row_count = mesh.shape["row"]
    field_spec = P(("batch", "row"), "col", None)
    coef_spec = P(("batch", "row"), "col")

    def local_step(field, x_lower, x_diag, x_upper, y_lower, y_diag, y_upper):
        words = field.reshape(T, NB, 128, F).transpose(0, 1, 3, 2)
        plane = (NB, ROWS, 128)
        fields = (NB, F, ROWS, 128)
        peers = row_count - 1
        in_vmem = pl.BlockSpec(memory_space=pltpu.VMEM)
        in_hbm = pl.BlockSpec(memory_space=pl.ANY)
        dma = pltpu.SemaphoreType.DMA
        parts = pl.pallas_call(
            functools.partial(main_kernel, row_count),
            out_shape=[pltpu.VMEM(fields, F32), pltpu.VMEM((2,) + plane, F32), pltpu.VMEM((2, R * 8, 128), F32)],
            in_specs=[in_hbm] * 7,
            out_specs=[in_vmem] * 3,
            scratch_shapes=[
                pltpu.VMEM((NB + 1, ROWS * F, 128), F32),
                pltpu.VMEM((3,) + plane, F32),
                pltpu.VMEM((2,) + plane, F32),
                pltpu.VMEM((3,) + plane, F32),
                pltpu.VMEM((3,) + plane, F32),
                pltpu.VMEM(fields, F32),
                pltpu.VMEM(fields, F32),
                pltpu.VMEM((6 * R, 8, 128), F32),
                pltpu.VMEM((6 * R, 8, 128), F32),
                pltpu.VMEM((8, 11, R, 128), F32),
                pltpu.VMEM((8, 11, R, 128), F32),
                pltpu.VMEM((2, 16, 128), F32),
                pltpu.VMEM((32, 128), F32),
                pltpu.VMEM((peers, 32, 128), F32),
                pltpu.VMEM((2 * R, 128), F32),
                pltpu.VMEM((peers, 2 * R, 128), F32),
                pltpu.VMEM((32, 128), F32),
                pltpu.VMEM((32, 128), F32),
                pltpu.VMEM((2 * R, 128), F32),
                pltpu.VMEM((2 * R, 128), F32),
                dma((28,)), dma, dma, dma((peers,)), dma((peers,)), dma((peers,)), dma((peers,)), dma((2,)), dma((2,)),
            ],
            compiler_params=pltpu.CompilerParams(
                collective_id=0, has_side_effects=True, vmem_limit_bytes=57 << 20),
        )(words, x_lower, x_diag, x_upper, y_lower, y_diag, y_upper)
        solved = pl.pallas_call(
            last_kernel,
            out_shape=jax.ShapeDtypeStruct((T, NB, F, 128), F32),
            in_specs=[in_vmem] * 3,
            out_specs=in_hbm,
            scratch_shapes=[pltpu.VMEM(fields, F32), pltpu.VMEM((NB, T * F, 128), F32), dma((NB,))],
            compiler_params=pltpu.CompilerParams(vmem_limit_bytes=20 << 20),
        )(*parts)
        return solved.transpose(0, 1, 3, 2).reshape(T, T, F)

    return jax.shard_map(local_step, mesh=mesh, in_specs=(field_spec,) + (coef_spec,) * 6,
                         out_specs=field_spec, check_vma=False)
```

```python
import functools

import jax
import jax.numpy as jnp
from jax import lax
from jax.experimental import pallas as pl
from jax.experimental.pallas import tpu as pltpu
from jax.sharding import PartitionSpec as P

MESH = pl.DeviceIdType.MESH
F32 = jnp.float32

T = 512
F = 4
C = 65
PAD = 8
ROWS = T + PAD
NB = T // 128
R = F * NB
UNROLL = 5

DIAG, LOW, UPP = 0, 1, 2
INV, NA, PR = 0, 1, 2
V, NC = 0, 1
A0, A1, A2, B0, B1, B2 = range(6)


def chunk_rows(t):
    return pl.ds(t, 8, stride=C)


def sweep(blocks, step, state, unroll=UNROLL):
    def steps(i, state):
        for n in range(unroll):
            state = step(blocks, i * unroll + n, state)
        return state
    return lax.fori_loop(0, C // unroll, steps, state)


def factor(k, kb, summ, beside=None):
    sub = lax.broadcasted_iota(jnp.int32, (8, 128), 0)
    zero = jnp.zeros((8, 128), F32)

    def step(blocks, t, state):
        out = []
        fresh = sub == jnp.where(t == PAD, 0, 8)
        for b in blocks:
            nc, v, pr, a1 = state[4 * b:4 * b + 4]
            rows = chunk_rows(t)
            low = k[LOW, b, rows, :]
            den = (1.0 + k[DIAG, b, rows, :]) + low * nc
            inv = 1.0 / den
            na = -(low * inv)
            nc = -(k[UPP, b, rows, :] * inv)
            v = na * v
            pr = jnp.where(fresh, 1.0, pr)
            k[INV, b, rows, :] = inv
            k[NA, b, rows, :] = na
            k[PR, b, rows, :] = pr
            kb[NC, b, rows, :] = nc
            kb[V, b, rows, :] = v
            a1 = a1 + pr * v
            pr = pr * nc
            out += [nc, v, pr, a1]
        if beside is not None:
            beside(t)
        return tuple(out)

    state = (zero, zero + 1.0, jnp.where(sub == 0, 0.0, 1.0), zero) * NB
    state = sweep(range(NB), step, state)
    for b in range(NB):
        nc, v, pr, a1 = state[4 * b:4 * b + 4]
        for f in range(F):
            r = f * NB + b
            summ[A1 * R + r] = a1
            summ[A2 * R + r] = pr
            summ[B1 * R + r] = v
            summ[B2 * R + r] = nc


def of_chunk(summ, q, s):
    return summ.reshape(6 * R * 8, 128)[pl.ds(q * R * 8 + s, R, stride=8), :]


def join_coef(la1, la2, lb1, lb2, ra1, ra2, rb1, rb2):
    inv = 1.0 / (1.0 - ra1 * lb2)
    w = inv * ra1
    e1 = w * lb1
    e2 = inv * ra2
    m1 = lb1 + lb2 * e1
    m2 = lb2 * e2
    return (la1 + la2 * e1, la2 * e2, rb1 * m1, rb2 + rb1 * m2), (inv, w, lb2, la2, rb1), (e1, e2, m1, m2)


def join_rhs(part, la0, lb0, ra0, rb0):
    inv, w, lb2, la2, rb1 = part
    e0 = inv * ra0 + w * lb0
    m0 = lb0 + lb2 * e0
    return la0 + la2 * e0, rb0 + rb1 * m0, e0, m0


def reduce_coef(summ, co, send):
    def chunk(s):
        return tuple(of_chunk(summ, q, s) for q in (A1, A2, B1, B2))
    whole = chunk(0)
    for s in range(1, 8):
        whole, part, inner = join_coef(*whole, *chunk(s))
        for n, v in enumerate(part + inner):
            co[s - 1, n] = v
    for n, v in enumerate(whole):
        co[7, n] = v
        send[n * 8:n * 8 + 8, :] = v[0:8]


def reduce_rhs(summ, co, send):
    a0, b0 = of_chunk(summ, A0, 0), of_chunk(summ, B0, 0)
    for s in range(1, 8):
        part = tuple(co[s - 1, n] for n in range(5))
        a0, b0, e0, m0 = join_rhs(part, a0, b0, of_chunk(summ, A0, s), of_chunk(summ, B0, s))
        co[s - 1, 9] = e0
        co[s - 1, 10] = m0
    send[0:R, :] = a0
    send[R:2 * R, :] = b0
    return a0, b0


def spread(co, before, after, edge):
    nxt = after
    edge[1, pl.ds(7, R, stride=8), :] = after
    edge[0, pl.ds(0, R, stride=8), :] = before
    for s in range(7, 0, -1):
        e1, e2, m1, m2, e0, m0 = (co[s - 1, n] for n in range(5, 11))
        edge[0, pl.ds(s, R, stride=8), :] = (m0 + m1 * before) + m2 * nxt
        nxt = (e0 + e1 * before) + e2 * nxt
        edge[1, pl.ds(s - 1, R, stride=8), :] = nxt


def forward(k, rhs_of, g, summ, group, unroll=UNROLL):
    zero = jnp.zeros((8, 128), F32)

    def step(blocks, t, state):
        out = []
        rows = chunk_rows(t)
        for j, b in enumerate(blocks):
            inv = k[INV, b, rows, :]
            na = k[NA, b, rows, :]
            pr = k[PR, b, rows, :]
            rhs = rhs_of(t, b)
            for f in range(F):
                last, first = state[2 * (j * F + f):2 * (j * F + f) + 2]
                last = inv * rhs[f] + na * last
                g[b, f, rows, :] = last
                out += [last, first + pr * last]
        return tuple(out)

    for b in range(0, NB, group):
        blocks = range(b, b + group)
        state = sweep(blocks, step, (zero,) * (2 * F * group), unroll)
        for j, c in enumerate(blocks):
            for f in range(F):
                summ[B0 * R + f * NB + c] = state[2 * (j * F + f)]
                summ[A0 * R + f * NB + c] = state[2 * (j * F + f) + 1]


def backward(kb, g, edge, put, turn):
    def start(b):
        return tuple(edge[1, pl.ds(pl.multiple_of((f * NB + b) * 8, 8), 8), :] for f in range(F))

    def step(b, n, state):
        out = []
        rows = chunk_rows(C - 1 - n)
        v = kb[V, b, rows, :]
        nc = kb[NC, b, rows, :]
        for f in range(F):
            near = edge[0, pl.ds(pl.multiple_of((f * NB + b) * 8, 8), 8), :]
            x = (g[b, f, rows, :] + v * near) + nc * state[f]
            put(b, f, rows, x)
            out.append(x)
        return tuple(out)

    sweep(0, step, start(0))

    def both(b, carry):
        state = step(b, 0, start(b))
        for n in range(NB * F):
            turn(b - 1, n)
            for m in range(4):
                state = step(b, 1 + 4 * n + m, state)
        return carry

    lax.fori_loop(1, NB, both, 0)
    for n in range(NB * F):
        turn(NB - 1, n)


def main_kernel(row_count, field, xl, xd, xu, yl, yd, yu, g, yb, edge,
                u, xk, xb, yn, yk, r1, y, sx, sy, cx, cy, pack,
                xcs, xcr, xrs, xrr, ycs, ycr, yrs, yrr,
                in_sem, ps, pr, xcss, xcrs, xrss, xrrs, yss, yrsem):
    row = lax.axis_index("row")
    col = lax.axis_index("col")
    other = 1 - col
    lane = lax.broadcasted_iota(jnp.int32, (8, 128), 1)
    zero = jnp.zeros((8, 128), F32)
    src_block = (NB - 1) * other
    src_lane = 127 * other
    dst_lane = 127 * col

    count = 0

    def fetch(src, dst):
        nonlocal count
        cp = pltpu.make_async_copy(src, dst, in_sem.at[count])
        cp.start()
        count += 1
        return cp

    def fetch_field(b):
        return fetch(field.at[:, b], u.at[b, pl.ds(PAD * F, T * F)].reshape(T, F, 128))

    def fetch_coef(refs, dst):
        return [fetch(ref.at[:, pl.ds(b * 128, 128)], dst.at[n, b, pl.ds(PAD, T)]) for n, ref in enumerate(refs) for b in range(NB)]

    in_edge = fetch_field(src_block)
    in_u = [fetch_field(lax.rem(src_block + d, NB)) for d in range(1, NB)]
    in_y = fetch_coef((yd, yl, yu), yn)
    in_x = fetch_coef((xd, xl, xu), xk)

    barrier = pltpu.get_barrier_semaphore()
    for d in range(1, row_count):
        pl.semaphore_signal(barrier, inc=1, device_id={"row": lax.rem(row + d, row_count)}, device_id_type=MESH)
    pl.semaphore_signal(barrier, inc=1, device_id={"col": other}, device_id_type=MESH)

    for b in range(NB):
        for n in range(3):
            yn[n, b, 0:PAD, :] = zero
            xk[n, b, 0:PAD, :] = zero - 1.0 if n == LOW else zero
            yk[n, b, 0:PAD, :] = zero - 1.0 if n == LOW else zero
        for f in range(F):
            y[b, f, 0:PAD, :] = zero
    for b in range(NB):
        u[b, 0:PAD * F, :] = jnp.zeros((PAD * F, 128), F32)
    u[NB] = jnp.zeros((ROWS * F, 128), F32)

    in_edge.wait()
    from_src = jnp.bitwise_and(lane - src_lane, 127)
    for h in range(2):
        acc = zero
        for p in range(128):
            w = PAD * F + 8 * (h * 128 + p)
            acc = jnp.where(from_src == p, pltpu.roll(u[src_block, w:w + 8, :], p, 1), acc)
        pack[0, h * 8:h * 8 + 8, :] = acc
    pl.semaphore_wait(barrier, row_count)
    column = pltpu.make_async_remote_copy(pack.at[0], pack.at[1], ps, pr, device_id={"col": other}, device_id_type=MESH)
    column.start()

    def to_line(send, recv, send_sem, recv_sem):
        copies = []
        for d in range(1, row_count):
            cp = pltpu.make_async_remote_copy(send, recv.at[d - 1], send_sem.at[d - 1], recv_sem.at[d - 1],
                                              device_id={"row": lax.rem(row + d, row_count)}, device_id_type=MESH)
            cp.start()
            copies.append(cp)
        return copies

    def to_pair(n, send, recv):
        cp = pltpu.make_async_remote_copy(send, recv, yss.at[n], yrsem.at[n], device_id={"col": other}, device_id_type=MESH)
        cp.start()
        return cp

    def stencil(b, t):
        rows = chunk_rows(t)
        cd = 1.0 - yn[DIAG, b, rows, :]
        cl = yn[LOW, b, rows, :]
        cu = yn[UPP, b, rows, :]
        left = lax.rem(b + NB, NB + 1)
        for f in range(F):
            words = pl.ds(t * F + f, 8, stride=C * F)
            mid = u[b, words, :]
            prv = pltpu.roll(jnp.where(lane == 127, u[left, words, :], mid), 1, 1)
            nxt = pltpu.roll(jnp.where(lane == 0, u[b + 1, words, :], mid), 127, 1)
            r1[b, f, rows, :] = (cd * mid - cl * prv) - cu * nxt

    for cp in in_u + in_y:
        cp.wait()

    def stencil_block(d, carry):
        b = lax.rem(src_block + d, NB)

        def step(blocks, t, state):
            stencil(b, t)
            return state

        sweep(None, step, carry, 13)
        return carry

    lax.fori_loop(1, NB - 1, stencil_block, 0)

    column.wait()
    here = lane == dst_lane
    for h in range(2):
        got = pack[1, h * 8:h * 8 + 8, :]
        for p in range(128):
            w = PAD * F + 8 * (h * 128 + p)
            u[NB, w:w + 8, :] = jnp.where(here, pltpu.roll(got, (128 - p) % 128, 1), 0.0)

    for cp in in_x:
        cp.wait()

    def rest_of_stencil(t):
        stencil(lax.rem(src_block + NB - 1, NB), t)
        stencil(src_block, t)

    factor(xk, xb, sx, rest_of_stencil)
    reduce_coef(sx, cx, xcs)
    coef_sends = to_line(xcs, xcr, xcss, xcrs)

    def rhs_x(t, b):
        return [r1[b, f, chunk_rows(t), :] for f in range(F)]

    forward(xk, rhs_x, g, sx, 2)
    a0, b0 = reduce_rhs(sx, cx, xrs)
    rhs_sends = to_line(xrs, xrr, xrss, xrrs)

    for b in range(NB):
        for c in range(NB):
            for n in range(3):
                yk[n, c, PAD + b * 128:PAD + b * 128 + 128, :] = yn[n, b, PAD + c * 128:PAD + c * 128 + 128, :].T
    factor(yk, yb, sy)
    reduce_coef(sy, cy, ycs)
    y_coef = to_pair(0, ycs, ycr)

    for cp in coef_sends:
        cp.wait()

    def coef_of(ref, n=None):
        view = ref if n is None else ref.at[n]
        return tuple(jnp.concatenate([view[q * 8:q * 8 + 8, :]] * 2, axis=0) for q in range(4))

    rest = coef_of(xcr, row_count - 2)
    parts = []
    for n in range(row_count - 3, -1, -1):
        rest, part, _ = join_coef(*rest, *coef_of(xcr, n))
        parts.append(part)
    p1, p2, q1, q2 = rest
    a1, a2, b1, b2 = (cx[7, n] for n in range(4))
    m12 = p1 * b1 + p2 * a1
    m21 = q1 * b2 + q2 * a2
    i11 = 1.0 / (1.0 - (p1 * b2 + p2 * a2))
    m21 = m21 * i11
    i22 = 1.0 / ((1.0 - (q1 * b1 + q2 * a1)) - m21 * m12)

    for cp in rhs_sends:
        cp.wait()
    p0, q0 = xrr[row_count - 2, 0:R, :], xrr[row_count - 2, R:2 * R, :]
    for part, n in zip(parts, range(row_count - 3, -1, -1)):
        p0, q0, _, _ = join_rhs(part, p0, q0, xrr[n, 0:R, :], xrr[n, R:2 * R, :])
    s1 = (p0 + p1 * b0) + p2 * a0
    s2 = (q0 + q1 * b0) + q2 * a0
    before = i22 * (s2 + m21 * s1)
    after = i11 * (s1 + m12 * before)
    spread(cx, before, after, edge)

    def put_x(b, f, rows, x):
        r1[b, f, rows, :] = (x + x) - r1[b, f, rows, :]

    def turn_in(b, n):
        c, f = n // F, n % F
        y[c, f, pl.ds(pl.multiple_of(PAD + b * 128, 8), 128), :] = r1[b, f, PAD + c * 128:PAD + c * 128 + 128, :].T

    backward(xb, g, edge, put_x, turn_in)

    def rhs_y(t, b):
        return [y[b, f, chunk_rows(t), :] for f in range(F)]

    forward(yk, rhs_y, g, sy, 2)
    a0, b0 = reduce_rhs(sy, cy, yrs)
    y_rhs = to_pair(1, yrs, yrr)

    y_coef.wait()
    first = col == 0
    a1, a2, b1, b2 = (cy[7, n] for n in range(4))
    c1, c2, d1, d2 = coef_of(ycr)
    lb2 = jnp.where(first, b2, d2)
    ra1 = jnp.where(first, c1, a1)
    inv = 1.0 / (1.0 - lb2 * ra1)
    y_rhs.wait()
    c0, d0 = yrr[0:R, :], yrr[R:2 * R, :]
    lb0 = jnp.where(first, b0, d0)
    ra0 = jnp.where(first, c0, a0)
    last_left = inv * (lb0 + lb2 * ra0)
    first_right = ra0 + ra1 * last_left
    spread(cy, jnp.where(first, 0.0, last_left), jnp.where(first, first_right, 0.0), edge)


def last_kernel(g, yb, edge, out, y, o, out_sem):
    def put_y(b, f, rows, x):
        y[b, f, rows, :] = x

    def turn_out(c, n):
        b, f = n // F, n % F
        o[b, pl.ds(c * 128 * F + f, 128, stride=F), :] = y[c, f, PAD + b * 128:PAD + b * 128 + 128, :].T
        if f == F - 1:
            cp = pltpu.make_async_copy(o.at[b, pl.ds(pl.multiple_of(c * 128 * F, 8), 128 * F)].reshape(128, F, 128),
                                       out.at[pl.ds(c * 128, 128), b], out_sem.at[c, b])
            cp.start()

    backward(yb, g, edge, put_y, turn_out)
    for c in range(NB):
        for b in range(NB):
            pltpu.make_async_copy(o.at[b, c * 128 * F:(c + 1) * 128 * F].reshape(128, F, 128),
                                  out.at[c * 128:(c + 1) * 128, b], out_sem.at[c, b]).wait()


def solution(mesh):
    row_count = mesh.shape["row"]
    field_spec = P(("batch", "row"), "col", None)
    coef_spec = P(("batch", "row"), "col")

    def local_step(field, x_lower, x_diag, x_upper, y_lower, y_diag, y_upper):
        words = field.reshape(T, NB, 128, F).transpose(0, 1, 3, 2)
        plane = (NB, ROWS, 128)
        fields = (NB, F, ROWS, 128)
        peers = row_count - 1
        in_vmem = pl.BlockSpec(memory_space=pltpu.VMEM)
        in_hbm = pl.BlockSpec(memory_space=pl.ANY)
        dma = pltpu.SemaphoreType.DMA
        parts = pl.pallas_call(
            functools.partial(main_kernel, row_count),
            out_shape=[pltpu.VMEM(fields, F32), pltpu.VMEM((2,) + plane, F32), pltpu.VMEM((2, R * 8, 128), F32)],
            in_specs=[in_hbm] * 7,
            out_specs=[in_vmem] * 3,
            scratch_shapes=[
                pltpu.VMEM((NB + 1, ROWS * F, 128), F32),
                pltpu.VMEM((3,) + plane, F32),
                pltpu.VMEM((2,) + plane, F32),
                pltpu.VMEM((3,) + plane, F32),
                pltpu.VMEM((3,) + plane, F32),
                pltpu.VMEM(fields, F32),
                pltpu.VMEM(fields, F32),
                pltpu.VMEM((6 * R, 8, 128), F32),
                pltpu.VMEM((6 * R, 8, 128), F32),
                pltpu.VMEM((8, 11, R, 128), F32),
                pltpu.VMEM((8, 11, R, 128), F32),
                pltpu.VMEM((2, 16, 128), F32),
                pltpu.VMEM((32, 128), F32),
                pltpu.VMEM((peers, 32, 128), F32),
                pltpu.VMEM((2 * R, 128), F32),
                pltpu.VMEM((peers, 2 * R, 128), F32),
                pltpu.VMEM((32, 128), F32),
                pltpu.VMEM((32, 128), F32),
                pltpu.VMEM((2 * R, 128), F32),
                pltpu.VMEM((2 * R, 128), F32),
                dma((28,)), dma, dma, dma((peers,)), dma((peers,)), dma((peers,)), dma((peers,)), dma((2,)), dma((2,)),
            ],
            compiler_params=pltpu.CompilerParams(
                collective_id=0, has_side_effects=True, vmem_limit_bytes=57 << 20),
        )(words, x_lower, x_diag, x_upper, y_lower, y_diag, y_upper)
        solved = pl.pallas_call(
            last_kernel,
            out_shape=jax.ShapeDtypeStruct((T, NB, F, 128), F32),
            in_specs=[in_vmem] * 3,
            out_specs=in_hbm,
            scratch_shapes=[pltpu.VMEM(fields, F32), pltpu.VMEM((NB, T * F, 128), F32), dma((NB, NB))],
            compiler_params=pltpu.CompilerParams(vmem_limit_bytes=20 << 20),
        )(*parts)
        return solved.transpose(0, 1, 3, 2).reshape(T, T, F)

    return jax.shard_map(local_step, mesh=mesh, in_specs=(field_spec,) + (coef_spec,) * 6,
                         out_specs=field_spec, check_vma=False)
```

```python
import functools

import jax
import jax.numpy as jnp
from jax import lax
from jax.experimental import pallas as pl
from jax.experimental.pallas import tpu as pltpu
from jax.sharding import PartitionSpec as P

MESH = pl.DeviceIdType.MESH
F32 = jnp.float32

T = 512
F = 4
C = 65
PAD = 8
ROWS = T + PAD
NB = T // 128
R = F * NB
UNROLL = 5
X_UNROLL = 13

DIAG, LOW, UPP = 0, 1, 2
INV, NA, PR = 0, 1, 2
V, NC = 0, 1
A0, A1, A2, B0, B1, B2 = range(6)


H = R // 2


def chunk_rows(t):
    return pl.ds(t, 8, stride=C)


def row_of(b, f):
    if isinstance(b, int):
        return b // 2 * H + f * 2 + b % 2
    return lax.div(b, 2) * H + f * 2 + lax.rem(b, 2)


def beside(edge, side, b, f):
    return edge[side, pl.ds(pl.multiple_of(row_of(b, f) * 8, 8), 8), :]


def sweep(blocks, step, state, unroll=UNROLL):
    def steps(i, state):
        for n in range(unroll):
            state = step(blocks, i * unroll + n, state)
        return state
    return lax.fori_loop(0, C // unroll, steps, state)


def factor(k, kb, summ):
    sub = lax.broadcasted_iota(jnp.int32, (8, 128), 0)
    zero = jnp.zeros((8, 128), F32)

    def step(blocks, t, state):
        out = []
        fresh = sub == jnp.where(t == PAD, 0, 8)
        for b in blocks:
            nc, v, pr, a1 = state[4 * b:4 * b + 4]
            rows = chunk_rows(t)
            low = k[LOW, b, rows, :]
            den = (1.0 + k[DIAG, b, rows, :]) + low * nc
            inv = 1.0 / den
            na = -(low * inv)
            nc = -(k[UPP, b, rows, :] * inv)
            v = na * v
            pr = jnp.where(fresh, 1.0, pr)
            k[INV, b, rows, :] = inv
            k[NA, b, rows, :] = na
            k[PR, b, rows, :] = pr
            kb[NC, b, rows, :] = nc
            kb[V, b, rows, :] = v
            a1 = a1 + pr * v
            pr = pr * nc
            out += [nc, v, pr, a1]
        return tuple(out)

    state = (zero, zero + 1.0, jnp.where(sub == 0, 0.0, 1.0), zero) * NB
    state = sweep(range(NB), step, state)
    for b in range(NB):
        nc, v, pr, a1 = state[4 * b:4 * b + 4]
        for f in range(F):
            r = row_of(b, f)
            summ[A1 * R + r] = a1
            summ[A2 * R + r] = pr
            summ[B1 * R + r] = v
            summ[B2 * R + r] = nc


def of_chunk(summ, q, s, first=0, rows=R):
    return summ.reshape(6 * R * 8, 128)[pl.ds(q * R * 8 + first * 8 + s, rows, stride=8), :]


def join_coef(la1, la2, lb1, lb2, ra1, ra2, rb1, rb2):
    inv = 1.0 / (1.0 - ra1 * lb2)
    w = inv * ra1
    e1 = w * lb1
    e2 = inv * ra2
    m1 = lb1 + lb2 * e1
    m2 = lb2 * e2
    return (la1 + la2 * e1, la2 * e2, rb1 * m1, rb2 + rb1 * m2), (inv, w, lb2, la2, rb1), (e1, e2, m1, m2)


def join_rhs(part, la0, lb0, ra0, rb0):
    inv, w, lb2, la2, rb1 = part
    e0 = inv * ra0 + w * lb0
    m0 = lb0 + lb2 * e0
    return la0 + la2 * e0, rb0 + rb1 * m0, e0, m0


def reduce_coef(summ, co, send):
    def chunk(s):
        return tuple(of_chunk(summ, q, s) for q in (A1, A2, B1, B2))
    whole = chunk(0)
    for s in range(1, 8):
        whole, part, inner = join_coef(*whole, *chunk(s))
        for n, v in enumerate(part + inner):
            co[s - 1, n] = v
    for n, v in enumerate(whole):
        co[7, n] = v
        send[n * R:n * R + R, :] = v


def reduce_rhs(summ, co, first, rows, send):
    some = pl.ds(first, rows)
    a0, b0 = (of_chunk(summ, q, 0, first, rows) for q in (A0, B0))
    for s in range(1, 8):
        part = tuple(co[s - 1, n, some, :] for n in range(5))
        a0, b0, e0, m0 = join_rhs(part, a0, b0, *(of_chunk(summ, q, s, first, rows) for q in (A0, B0)))
        co[s - 1, 9, some, :] = e0
        co[s - 1, 10, some, :] = m0
    send[0:rows, :] = a0
    send[rows:2 * rows, :] = b0


def spread(co, first, rows, before, after, edge):
    def at(s):
        return pl.ds(first * 8 + s, rows, stride=8)
    some = pl.ds(first, rows)
    nxt = after
    edge[1, at(7), :] = after
    edge[0, at(0), :] = before
    for s in range(7, 0, -1):
        e1, e2, m1, m2, e0, m0 = (co[s - 1, n, some, :] for n in range(5, 11))
        edge[0, at(s), :] = (m0 + m1 * before) + m2 * nxt
        nxt = (e0 + e1 * before) + e2 * nxt
        edge[1, at(s - 1), :] = nxt


def forward(k, rhs_of, g, summ, blocks, unroll=UNROLL):
    zero = jnp.zeros((8, 128), F32)

    def step(blocks, t, state):
        out = []
        rows = chunk_rows(t)
        for j, b in enumerate(blocks):
            inv = k[INV, b, rows, :]
            na = k[NA, b, rows, :]
            pr = k[PR, b, rows, :]
            rhs = rhs_of(b, t)
            for f in range(F):
                last, first = state[2 * (j * F + f):2 * (j * F + f) + 2]
                last = inv * rhs[f] + na * last
                g[b, f, rows, :] = last
                out += [last, first + pr * last]
        return tuple(out)

    state = sweep(blocks, step, (zero,) * (2 * F * len(blocks)), unroll)
    for j, b in enumerate(blocks):
        for f in range(F):
            summ[B0 * R + row_of(b, f)] = state[2 * (j * F + f)]
            summ[A0 * R + row_of(b, f)] = state[2 * (j * F + f) + 1]


def backward(kb, g, edge, put, turn):
    def start(b):
        return tuple(beside(edge, 1, b, f) for f in range(F))

    def step(b, n, state):
        out = []
        rows = chunk_rows(C - 1 - n)
        v = kb[V, b, rows, :]
        nc = kb[NC, b, rows, :]
        for f in range(F):
            x = (g[b, f, rows, :] + v * beside(edge, 0, b, f)) + nc * state[f]
            put(b, f, rows, x)
            out.append(x)
        return tuple(out)

    def alone(b):
        sweep(b, step, start(b))

    def both(b, before):
        state = step(b, 0, start(b))
        for n in range(NB * F):
            turn(before, n)
            for m in range(4):
                state = step(b, 1 + 4 * n + m, state)

    def last(b):
        for n in range(NB * F):
            turn(b, n)

    return alone, both, last


def main_kernel(row_count, field, xl, xd, xu, yl, yd, yu, g, yb, edge,
                u, xk, xb, yn, yk, r1, y, sx, sy, cx, cy, pack, close,
                xcs, xcr, xrs, xrr, ycs, ycr, yrs, yrr,
                in_sem, ps, pr, xcss, xcrs, xrss, xrrs, yss, yrsem):
    row = lax.axis_index("row")
    col = lax.axis_index("col")
    other = 1 - col
    lane = lax.broadcasted_iota(jnp.int32, (8, 128), 1)
    zero = jnp.zeros((8, 128), F32)
    src_block = (NB - 1) * other
    src_lane = 127 * other
    dst_lane = 127 * col

    count = 0

    def fetch(src, dst):
        nonlocal count
        cp = pltpu.make_async_copy(src, dst, in_sem.at[count])
        cp.start()
        count += 1
        return cp

    def fetch_field(b):
        return fetch(field.at[:, b], u.at[b, pl.ds(PAD * F, T * F)].reshape(T, F, 128))

    def fetch_coef(refs, dst):
        return [fetch(ref.at[:, pl.ds(b * 128, 128)], dst.at[n, b, pl.ds(PAD, T)]) for n, ref in enumerate(refs) for b in range(NB)]

    in_x = fetch_coef((xd, xl, xu), xk)
    in_edge = fetch_field(src_block)
    in_u = [fetch_field(lax.rem(src_block + d, NB)) for d in range(1, NB)]
    in_y = fetch_coef((yd, yl, yu), yn)

    barrier = pltpu.get_barrier_semaphore()
    for d in range(1, row_count):
        pl.semaphore_signal(barrier, inc=1, device_id={"row": lax.rem(row + d, row_count)}, device_id_type=MESH)
    pl.semaphore_signal(barrier, inc=1, device_id={"col": other}, device_id_type=MESH)

    for b in range(NB):
        for n in range(3):
            yn[n, b, 0:PAD, :] = zero
            xk[n, b, 0:PAD, :] = zero - 1.0 if n == LOW else zero
            yk[n, b, 0:PAD, :] = zero - 1.0 if n == LOW else zero
        for f in range(F):
            y[b, f, 0:PAD, :] = zero
    for b in range(NB):
        u[b, 0:PAD * F, :] = jnp.zeros((PAD * F, 128), F32)
    u[NB] = jnp.zeros((ROWS * F, 128), F32)

    def to_line(send, recv, send_sem, recv_sem):
        copies = []
        for d in range(1, row_count):
            cp = pltpu.make_async_remote_copy(send, recv.at[d - 1], send_sem.at[d - 1], recv_sem.at[d - 1],
                                              device_id={"row": lax.rem(row + d, row_count)}, device_id_type=MESH)
            cp.start()
            copies.append(cp)
        return copies

    def to_pair(n, send, recv):
        cp = pltpu.make_async_remote_copy(send, recv, yss.at[n], yrsem.at[n], device_id={"col": other}, device_id_type=MESH)
        cp.start()
        return cp

    for cp in in_x:
        cp.wait()
    factor(xk, xb, sx)
    reduce_coef(sx, cx, xcs)

    in_edge.wait()
    from_src = jnp.bitwise_and(lane - src_lane, 127)
    for h in range(2):
        acc = zero
        for p in range(128):
            w = PAD * F + 8 * (h * 128 + p)
            acc = jnp.where(from_src == p, pltpu.roll(u[src_block, w:w + 8, :], p, 1), acc)
        pack[0, h * 8:h * 8 + 8, :] = acc
    pl.semaphore_wait(barrier, row_count)
    column = pltpu.make_async_remote_copy(pack.at[0], pack.at[1], ps, pr, device_id={"col": other}, device_id_type=MESH)
    column.start()

    coef_sends = to_line(xcs, xcr, xcss, xcrs)

    def stencil(b, t):
        rows = chunk_rows(t)
        cd = 1.0 - yn[DIAG, b, rows, :]
        cl = yn[LOW, b, rows, :]
        cu = yn[UPP, b, rows, :]
        left = lax.rem(b + NB, NB + 1)
        rhs = []
        for f in range(F):
            words = pl.ds(t * F + f, 8, stride=C * F)
            mid = u[b, words, :]
            prv = pltpu.roll(jnp.where(lane == 127, u[left, words, :], mid), 1, 1)
            nxt = pltpu.roll(jnp.where(lane == 0, u[b + 1, words, :], mid), 127, 1)
            v = (cd * mid - cl * prv) - cu * nxt
            r1[b, f, rows, :] = v
            rhs.append(v)
        return rhs

    for cp in in_u + in_y:
        cp.wait()

    halves = [col, other]

    def block(n):
        return n + col * (3 - 2 * n)

    def eliminate(n, carry):
        forward(xk, stencil, g, sx, [block(n)], X_UNROLL)
        return carry

    rhs_sends = []
    for h in range(2):
        if h == 0:
            lax.fori_loop(0, 2, eliminate, 0)
        else:
            eliminate(2, 0)
            column.wait()
            here = lane == dst_lane
            for i in range(2):
                got = pack[1, i * 8:i * 8 + 8, :]
                for p in range(128):
                    w = PAD * F + 8 * (i * 128 + p)
                    u[NB, w:w + 8, :] = jnp.where(here, pltpu.roll(got, (128 - p) % 128, 1), 0.0)
            eliminate(3, 0)
        reduce_rhs(sx, cx, pl.multiple_of(halves[h] * H, 8), H, xrs.at[h])
        rhs_sends.append(to_line(xrs.at[h], xrr.at[h], xrss.at[h], xrrs.at[h]))

    for b in range(NB):
        for c in range(NB):
            for n in range(3):
                yk[n, c, PAD + b * 128:PAD + b * 128 + 128, :] = yn[n, b, PAD + c * 128:PAD + c * 128 + 128, :].T
    factor(yk, yb, sy)
    reduce_coef(sy, cy, ycs)
    y_coef = to_pair(0, ycs, ycr)

    for cp in coef_sends:
        cp.wait()

    def coef_of(ref):
        return tuple(ref[q * R:q * R + R, :] for q in range(4))

    slots = range(row_count - 3, -1, -1)
    rest = coef_of(xcr.at[row_count - 2])
    known = []
    for n in slots:
        rest, part, _ = join_coef(*rest, *coef_of(xcr.at[n]))
        known += part
    p1, p2, q1, q2 = rest
    a1, a2, b1, b2 = (cx[7, n] for n in range(4))
    m12 = p1 * b1 + p2 * a1
    i11 = 1.0 / (1.0 - (p1 * b2 + p2 * a2))
    m21 = (q1 * b2 + q2 * a2) * i11
    i22 = 1.0 / ((1.0 - (q1 * b1 + q2 * a1)) - m21 * m12)
    for n, v in enumerate(known + [p1, p2, q1, q2, m12, m21, i11, i22]):
        close[n] = v

    def close_line(h):
        for cp in rhs_sends[h]:
            cp.wait()
        first = pl.multiple_of(halves[h] * H, 8)
        known = [close[n, pl.ds(first, H), :] for n in range(5 * (row_count - 2) + 8)]

        def received(n):
            return xrr[h, n, 0:H, :], xrr[h, n, H:2 * H, :]

        p0, q0 = received(row_count - 2)
        for i, n in enumerate(slots):
            p0, q0, _, _ = join_rhs(known[5 * i:5 * i + 5], p0, q0, *received(n))
        p1, p2, q1, q2, m12, m21, i11, i22 = known[5 * (row_count - 2):]
        a0, b0 = xrs[h, 0:H, :], xrs[h, H:2 * H, :]
        s1 = (p0 + p1 * b0) + p2 * a0
        s2 = (q0 + q1 * b0) + q2 * a0
        before = i22 * (s2 + m21 * s1)
        spread(cx, first, H, before, i11 * (s1 + m12 * before), edge)

    def put_x(b, f, rows, x):
        r1[b, f, rows, :] = (x + x) - r1[b, f, rows, :]

    def turn_in(b, n):
        c, f = n // F, n % F
        y[c, f, pl.ds(pl.multiple_of(PAD + b * 128, 8), 128), :] = r1[b, f, PAD + c * 128:PAD + c * 128 + 128, :].T

    alone, both, last = backward(xb, g, edge, put_x, turn_in)

    def solve(n, carry):
        both(block(n), block(n - 1))
        return carry

    close_line(0)
    alone(block(0))
    lax.fori_loop(1, 2, solve, 0)
    close_line(1)
    lax.fori_loop(2, 4, solve, 0)
    last(block(3))

    def rhs_y(b, t):
        return [y[b, f, chunk_rows(t), :] for f in range(F)]

    forward(yk, rhs_y, g, sy, [0, 1])
    forward(yk, rhs_y, g, sy, [2, 3])
    reduce_rhs(sy, cy, 0, R, yrs)
    a0, b0 = yrs[0:R, :], yrs[R:2 * R, :]
    y_rhs = to_pair(1, yrs, yrr)

    y_coef.wait()
    first = col == 0
    a1, a2, b1, b2 = (cy[7, n] for n in range(4))
    c1, c2, d1, d2 = coef_of(ycr)
    lb2 = jnp.where(first, b2, d2)
    ra1 = jnp.where(first, c1, a1)
    inv = 1.0 / (1.0 - lb2 * ra1)
    y_rhs.wait()
    c0, d0 = yrr[0:R, :], yrr[R:2 * R, :]
    lb0 = jnp.where(first, b0, d0)
    ra0 = jnp.where(first, c0, a0)
    last_left = inv * (lb0 + lb2 * ra0)
    first_right = ra0 + ra1 * last_left
    spread(cy, 0, R, jnp.where(first, 0.0, last_left), jnp.where(first, first_right, 0.0), edge)


def last_kernel(g, yb, edge, out, y, o, out_sem):
    def put_y(b, f, rows, x):
        y[b, f, rows, :] = x

    def turn_out(c, n):
        b, f = n // F, n % F
        o[b, pl.ds(c * 128 * F + f, 128, stride=F), :] = y[c, f, PAD + b * 128:PAD + b * 128 + 128, :].T
        if f == F - 1:
            cp = pltpu.make_async_copy(o.at[b, pl.ds(pl.multiple_of(c * 128 * F, 8), 128 * F)].reshape(128, F, 128),
                                       out.at[pl.ds(c * 128, 128), b], out_sem.at[c, b])
            cp.start()

    alone, both, last = backward(yb, g, edge, put_y, turn_out)
    alone(0)

    def pair(c, carry):
        both(c, c - 1)
        return carry

    lax.fori_loop(1, NB, pair, 0)
    last(NB - 1)
    for c in range(NB):
        for b in range(NB):
            pltpu.make_async_copy(o.at[b, c * 128 * F:(c + 1) * 128 * F].reshape(128, F, 128),
                                  out.at[c * 128:(c + 1) * 128, b], out_sem.at[c, b]).wait()


def solution(mesh):
    row_count = mesh.shape["row"]
    field_spec = P(("batch", "row"), "col", None)
    coef_spec = P(("batch", "row"), "col")

    def local_step(field, x_lower, x_diag, x_upper, y_lower, y_diag, y_upper):
        words = field.reshape(T, NB, 128, F).transpose(0, 1, 3, 2)
        plane = (NB, ROWS, 128)
        fields = (NB, F, ROWS, 128)
        peers = row_count - 1
        in_vmem = pl.BlockSpec(memory_space=pltpu.VMEM)
        in_hbm = pl.BlockSpec(memory_space=pl.ANY)
        dma = pltpu.SemaphoreType.DMA
        parts = pl.pallas_call(
            functools.partial(main_kernel, row_count),
            out_shape=[pltpu.VMEM(fields, F32), pltpu.VMEM((2,) + plane, F32), pltpu.VMEM((2, R * 8, 128), F32)],
            in_specs=[in_hbm] * 7,
            out_specs=[in_vmem] * 3,
            scratch_shapes=[
                pltpu.VMEM((NB + 1, ROWS * F, 128), F32),
                pltpu.VMEM((3,) + plane, F32),
                pltpu.VMEM((2,) + plane, F32),
                pltpu.VMEM((3,) + plane, F32),
                pltpu.VMEM((3,) + plane, F32),
                pltpu.VMEM(fields, F32),
                pltpu.VMEM(fields, F32),
                pltpu.VMEM((6 * R, 8, 128), F32),
                pltpu.VMEM((6 * R, 8, 128), F32),
                pltpu.VMEM((8, 11, R, 128), F32),
                pltpu.VMEM((8, 11, R, 128), F32),
                pltpu.VMEM((2, 16, 128), F32),
                pltpu.VMEM((5 * (row_count - 2) + 8, R, 128), F32),
                pltpu.VMEM((4 * R, 128), F32),
                pltpu.VMEM((peers, 4 * R, 128), F32),
                pltpu.VMEM((2, R, 128), F32),
                pltpu.VMEM((2, peers, R, 128), F32),
                pltpu.VMEM((4 * R, 128), F32),
                pltpu.VMEM((4 * R, 128), F32),
                pltpu.VMEM((2 * R, 128), F32),
                pltpu.VMEM((2 * R, 128), F32),
                dma((28,)), dma, dma, dma((peers,)), dma((peers,)), dma((2, peers)), dma((2, peers)), dma((2,)), dma((2,)),
            ],
            compiler_params=pltpu.CompilerParams(
                collective_id=0, has_side_effects=True, vmem_limit_bytes=57 << 20),
        )(words, x_lower, x_diag, x_upper, y_lower, y_diag, y_upper)
        solved = pl.pallas_call(
            last_kernel,
            out_shape=jax.ShapeDtypeStruct((T, NB, F, 128), F32),
            in_specs=[in_vmem] * 3,
            out_specs=in_hbm,
            scratch_shapes=[pltpu.VMEM(fields, F32), pltpu.VMEM((NB, T * F, 128), F32), dma((NB, NB))],
            compiler_params=pltpu.CompilerParams(vmem_limit_bytes=20 << 20),
        )(*parts)
        return solved.transpose(0, 1, 3, 2).reshape(T, T, F)

    return jax.shard_map(local_step, mesh=mesh, in_specs=(field_spec,) + (coef_spec,) * 6,
                         out_specs=field_spec, check_vma=False)
```

```python
import functools

import jax
import jax.numpy as jnp
from jax import lax
from jax.experimental import pallas as pl
from jax.experimental.pallas import tpu as pltpu
from jax.sharding import PartitionSpec as P

MESH = pl.DeviceIdType.MESH
F32 = jnp.float32

T = 512
F = 4
C = 65
PAD = 8
ROWS = T + PAD
NB = T // 128
R = F * NB
UNROLL = 5

DIAG, LOW, UPP = 0, 1, 2
INV, NA, PR = 0, 1, 2
V, NC = 0, 1
A0, A1, A2, B0, B1, B2 = range(6)


H = R // 2
X_UNROLL = C


def chunk_rows(t):
    return pl.ds(t, 8, stride=C)


def row_of(b, f):
    if isinstance(b, int):
        return b // 2 * H + f * 2 + b % 2
    return lax.div(b, 2) * H + f * 2 + lax.rem(b, 2)


def beside(edge, side, b, f):
    return edge[side, pl.ds(pl.multiple_of(row_of(b, f) * 8, 8), 8), :]


def sweep(blocks, step, state, unroll=UNROLL):
    def steps(i, state):
        for n in range(unroll):
            state = step(blocks, i * unroll + n, state)
        return state
    return lax.fori_loop(0, C // unroll, steps, state)


def factor(k, kb, summ):
    sub = lax.broadcasted_iota(jnp.int32, (8, 128), 0)
    zero = jnp.zeros((8, 128), F32)

    def step(blocks, t, state):
        out = []
        fresh = sub == jnp.where(t == PAD, 0, 8)
        for b in blocks:
            nc, v, pr, a1 = state[4 * b:4 * b + 4]
            rows = chunk_rows(t)
            low = k[LOW, b, rows, :]
            den = (1.0 + k[DIAG, b, rows, :]) + low * nc
            inv = 1.0 / den
            na = -(low * inv)
            nc = -(k[UPP, b, rows, :] * inv)
            v = na * v
            pr = jnp.where(fresh, 1.0, pr)
            k[INV, b, rows, :] = inv
            k[NA, b, rows, :] = na
            k[PR, b, rows, :] = pr
            kb[NC, b, rows, :] = nc
            kb[V, b, rows, :] = v
            a1 = a1 + pr * v
            pr = pr * nc
            out += [nc, v, pr, a1]
        return tuple(out)

    state = (zero, zero + 1.0, jnp.where(sub == 0, 0.0, 1.0), zero) * NB
    state = sweep(range(NB), step, state)
    for b in range(NB):
        nc, v, pr, a1 = state[4 * b:4 * b + 4]
        for f in range(F):
            r = row_of(b, f)
            summ[A1 * R + r] = a1
            summ[A2 * R + r] = pr
            summ[B1 * R + r] = v
            summ[B2 * R + r] = nc


def of_chunk(summ, q, s, first=0, rows=R):
    return summ.reshape(6 * R * 8, 128)[pl.ds(q * R * 8 + first * 8 + s, rows, stride=8), :]


def join_coef(la1, la2, lb1, lb2, ra1, ra2, rb1, rb2):
    inv = 1.0 / (1.0 - ra1 * lb2)
    w = inv * ra1
    e1 = w * lb1
    e2 = inv * ra2
    m1 = lb1 + lb2 * e1
    m2 = lb2 * e2
    return (la1 + la2 * e1, la2 * e2, rb1 * m1, rb2 + rb1 * m2), (inv, w, lb2, la2, rb1), (e1, e2, m1, m2)


def join_rhs(part, la0, lb0, ra0, rb0):
    inv, w, lb2, la2, rb1 = part
    e0 = inv * ra0 + w * lb0
    m0 = lb0 + lb2 * e0
    return la0 + la2 * e0, rb0 + rb1 * m0, e0, m0


def reduce_coef(summ, co, send):
    def chunk(s):
        return tuple(of_chunk(summ, q, s) for q in (A1, A2, B1, B2))
    whole = chunk(0)
    for s in range(1, 8):
        whole, part, inner = join_coef(*whole, *chunk(s))
        for n, v in enumerate(part + inner):
            co[s - 1, n] = v
    for n, v in enumerate(whole):
        co[7, n] = v
        send[n * R:n * R + R, :] = v


def reduce_rhs(summ, co, first, rows, send):
    some = pl.ds(first, rows)
    a0, b0 = (of_chunk(summ, q, 0, first, rows) for q in (A0, B0))
    for s in range(1, 8):
        part = tuple(co[s - 1, n, some, :] for n in range(5))
        a0, b0, e0, m0 = join_rhs(part, a0, b0, *(of_chunk(summ, q, s, first, rows) for q in (A0, B0)))
        co[s - 1, 9, some, :] = e0
        co[s - 1, 10, some, :] = m0
    send[0:rows, :] = a0
    send[rows:2 * rows, :] = b0


def spread(co, first, rows, before, after, edge):
    def at(s):
        return pl.ds(first * 8 + s, rows, stride=8)
    some = pl.ds(first, rows)
    nxt = after
    edge[1, at(7), :] = after
    edge[0, at(0), :] = before
    for s in range(7, 0, -1):
        e1, e2, m1, m2, e0, m0 = (co[s - 1, n, some, :] for n in range(5, 11))
        edge[0, at(s), :] = (m0 + m1 * before) + m2 * nxt
        nxt = (e0 + e1 * before) + e2 * nxt
        edge[1, at(s - 1), :] = nxt


def forward(k, rhs_of, g, summ, blocks, unroll=UNROLL):
    zero = jnp.zeros((8, 128), F32)

    def step(blocks, t, state):
        out = []
        rows = chunk_rows(t)
        for j, b in enumerate(blocks):
            inv = k[INV, b, rows, :]
            na = k[NA, b, rows, :]
            pr = k[PR, b, rows, :]
            rhs = rhs_of(b, t)
            for f in range(F):
                last, first = state[2 * (j * F + f):2 * (j * F + f) + 2]
                last = inv * rhs[f] + na * last
                g[b, f, rows, :] = last
                out += [last, first + pr * last]
        return tuple(out)

    state = (zero,) * (2 * F * len(blocks))
    if unroll == C:
        for t in range(C):
            state = step(blocks, t, state)
    else:
        state = sweep(blocks, step, state, unroll)
    for j, b in enumerate(blocks):
        for f in range(F):
            summ[B0 * R + row_of(b, f)] = state[2 * (j * F + f)]
            summ[A0 * R + row_of(b, f)] = state[2 * (j * F + f) + 1]


def backward(kb, g, edge, put, turn):
    def start(b):
        return tuple(beside(edge, 1, b, f) for f in range(F))

    def step(b, n, state):
        out = []
        rows = chunk_rows(C - 1 - n)
        v = kb[V, b, rows, :]
        nc = kb[NC, b, rows, :]
        for f in range(F):
            x = (g[b, f, rows, :] + v * beside(edge, 0, b, f)) + nc * state[f]
            put(b, f, rows, x)
            out.append(x)
        return tuple(out)

    def alone(b):
        sweep(b, step, start(b))

    def both(b, before):
        state = step(b, 0, start(b))
        for n in range(NB * F):
            turn(before, n)
            for m in range(4):
                state = step(b, 1 + 4 * n + m, state)

    def last(b):
        for n in range(NB * F):
            turn(b, n)

    return alone, both, last


def main_kernel(row_count, field, xl, xd, xu, yl, yd, yu, g, yb, edge,
                u, xk, xb, yn, yk, r1, y, sx, sy, cx, cy, pack, close,
                xcs, xcr, xrs, xrr, ycs, ycr, yrs, yrr,
                in_sem, field_sem, coef_sem, ps, pr, xcss, xcrs, xrss, xrrs, yss, yrsem):
    row = lax.axis_index("row")
    col = lax.axis_index("col")
    other = 1 - col
    lane = lax.broadcasted_iota(jnp.int32, (8, 128), 1)
    zero = jnp.zeros((8, 128), F32)
    src_block = (NB - 1) * other
    src_lane = 127 * other
    dst_lane = 127 * col

    count = 0

    def fetch(src, dst):
        nonlocal count
        cp = pltpu.make_async_copy(src, dst, in_sem.at[count])
        cp.start()
        count += 1
        return cp

    in_x = [fetch(ref.at[:, pl.ds(b * 128, 128)], xk.at[n, b, pl.ds(PAD, T)])
            for n, ref in enumerate((xd, xl, xu)) for b in range(NB)]

    def block(n):
        return n + col * (3 - 2 * n)

    def in_field(n):
        b = block(n)
        return pltpu.make_async_copy(field.at[:, b], u.at[b, pl.ds(PAD * F, T * F)].reshape(T, F, 128), field_sem.at[n])

    def in_coef(n):
        b = block(n)
        return [pltpu.make_async_copy(ref.at[:, pl.ds(pl.multiple_of(b * 128, 128), 128)], yn.at[i, b, pl.ds(PAD, T)], coef_sem.at[n, i])
                for i, ref in enumerate((yd, yl, yu))]

    for n in (3, 0, 1):
        in_field(n).start()
    for n in range(NB):
        for cp in in_coef(n):
            cp.start()
        if n == 0:
            in_field(2).start()

    barrier = pltpu.get_barrier_semaphore()
    for d in range(1, row_count):
        pl.semaphore_signal(barrier, inc=1, device_id={"row": lax.rem(row + d, row_count)}, device_id_type=MESH)
    pl.semaphore_signal(barrier, inc=1, device_id={"col": other}, device_id_type=MESH)

    for b in range(NB):
        for n in range(3):
            yn[n, b, 0:PAD, :] = zero
            xk[n, b, 0:PAD, :] = zero - 1.0 if n == LOW else zero
            yk[n, b, 0:PAD, :] = zero - 1.0 if n == LOW else zero
        for f in range(F):
            y[b, f, 0:PAD, :] = zero
    for b in range(NB):
        u[b, 0:PAD * F, :] = jnp.zeros((PAD * F, 128), F32)
    u[NB] = jnp.zeros((ROWS * F, 128), F32)

    def line_copies(send, recv, send_sem, recv_sem):
        return [pltpu.make_async_remote_copy(send, recv.at[d - 1], send_sem.at[d - 1], recv_sem.at[d - 1],
                                             device_id={"row": lax.rem(row + d, row_count)}, device_id_type=MESH)
                for d in range(1, row_count)]

    def to_line(*refs):
        copies = line_copies(*refs)
        for cp in copies:
            cp.start()
        return copies

    def to_pair(n, send, recv):
        cp = pltpu.make_async_remote_copy(send, recv, yss.at[n], yrsem.at[n], device_id={"col": other}, device_id_type=MESH)
        cp.start()
        return cp

    for cp in in_x:
        cp.wait()
    factor(xk, xb, sx)
    reduce_coef(sx, cx, xcs)

    in_field(3).wait()
    from_src = jnp.bitwise_and(lane - src_lane, 127)
    for h in range(2):
        acc = zero
        for p in range(128):
            w = PAD * F + 8 * (h * 128 + p)
            acc = jnp.where(from_src == p, pltpu.roll(u[src_block, w:w + 8, :], p, 1), acc)
        pack[0, h * 8:h * 8 + 8, :] = acc
    pl.semaphore_wait(barrier, row_count)
    column = pltpu.make_async_remote_copy(pack.at[0], pack.at[1], ps, pr, device_id={"col": other}, device_id_type=MESH)
    column.start()

    coef_sends = to_line(xcs, xcr, xcss, xcrs)

    def stencil(b, t):
        rows = chunk_rows(t)
        cd = 1.0 - yn[DIAG, b, rows, :]
        cl = yn[LOW, b, rows, :]
        cu = yn[UPP, b, rows, :]
        left = lax.rem(b + NB, NB + 1)
        rhs = []
        for f in range(F):
            words = pl.ds(t * F + f, 8, stride=C * F)
            mid = u[b, words, :]
            prv = pltpu.roll(jnp.where(lane == 127, u[left, words, :], mid), 1, 1)
            nxt = pltpu.roll(jnp.where(lane == 0, u[b + 1, words, :], mid), 127, 1)
            v = (cd * mid - cl * prv) - cu * nxt
            r1[b, f, rows, :] = v
            rhs.append(v)
        return rhs

    halves = [col, other]

    def send_half(h):
        reduce_rhs(sx, cx, pl.multiple_of(halves[h] * H, 8), H, xrs.at[h])
        return to_line(xrs.at[h], xrr.at[h], xrss.at[h], xrrs.at[h])

    def eliminate(n, carry):
        for cp in in_coef(n):
            cp.wait()

        @pl.when(n < 2)
        def _():
            in_field(n + 1).wait()

        @pl.when(n == 2)
        def _():
            send_half(0)

        @pl.when(n == 3)
        def _():
            column.wait()
            here = lane == dst_lane
            for i in range(2):
                got = pack[1, i * 8:i * 8 + 8, :]
                for p in range(128):
                    w = PAD * F + 8 * (i * 128 + p)
                    u[NB, w:w + 8, :] = jnp.where(here, pltpu.roll(got, (128 - p) % 128, 1), 0.0)

        forward(xk, stencil, g, sx, [block(n)], X_UNROLL)
        return carry

    in_field(0).wait()
    lax.fori_loop(0, NB, eliminate, 0)
    send_half(1)

    for b in range(NB):
        for c in range(NB):
            for n in range(3):
                yk[n, c, PAD + b * 128:PAD + b * 128 + 128, :] = yn[n, b, PAD + c * 128:PAD + c * 128 + 128, :].T
    factor(yk, yb, sy)
    reduce_coef(sy, cy, ycs)
    y_coef = to_pair(0, ycs, ycr)

    for cp in coef_sends:
        cp.wait()

    def coef_of(ref):
        return tuple(ref[q * R:q * R + R, :] for q in range(4))

    slots = range(row_count - 3, -1, -1)
    rest = coef_of(xcr.at[row_count - 2])
    known = []
    for n in slots:
        rest, part, _ = join_coef(*rest, *coef_of(xcr.at[n]))
        known += part
    p1, p2, q1, q2 = rest
    a1, a2, b1, b2 = (cx[7, n] for n in range(4))
    m12 = p1 * b1 + p2 * a1
    i11 = 1.0 / (1.0 - (p1 * b2 + p2 * a2))
    m21 = (q1 * b2 + q2 * a2) * i11
    i22 = 1.0 / ((1.0 - (q1 * b1 + q2 * a1)) - m21 * m12)
    for n, v in enumerate(known + [p1, p2, q1, q2, m12, m21, i11, i22]):
        close[n] = v

    def close_line(h):
        for cp in line_copies(xrs.at[h], xrr.at[h], xrss.at[h], xrrs.at[h]):
            cp.wait()
        first = pl.multiple_of(halves[h] * H, 8)
        known = [close[n, pl.ds(first, H), :] for n in range(5 * (row_count - 2) + 8)]

        def received(n):
            return xrr[h, n, 0:H, :], xrr[h, n, H:2 * H, :]

        p0, q0 = received(row_count - 2)
        for i, n in enumerate(slots):
            p0, q0, _, _ = join_rhs(known[5 * i:5 * i + 5], p0, q0, *received(n))
        p1, p2, q1, q2, m12, m21, i11, i22 = known[5 * (row_count - 2):]
        a0, b0 = xrs[h, 0:H, :], xrs[h, H:2 * H, :]
        s1 = (p0 + p1 * b0) + p2 * a0
        s2 = (q0 + q1 * b0) + q2 * a0
        before = i22 * (s2 + m21 * s1)
        spread(cx, first, H, before, i11 * (s1 + m12 * before), edge)

    def put_x(b, f, rows, x):
        r1[b, f, rows, :] = (x + x) - r1[b, f, rows, :]

    def turn_in(b, n):
        c, f = n // F, n % F
        y[c, f, pl.ds(pl.multiple_of(PAD + b * 128, 8), 128), :] = r1[b, f, PAD + c * 128:PAD + c * 128 + 128, :].T

    alone, both, last = backward(xb, g, edge, put_x, turn_in)

    def solve(n, carry):
        @pl.when(n == 2)
        def _():
            close_line(1)

        both(block(n), block(n - 1))
        return carry

    close_line(0)
    alone(block(0))
    lax.fori_loop(1, NB, solve, 0)
    last(block(3))

    def rhs_y(b, t):
        return [y[b, f, chunk_rows(t), :] for f in range(F)]

    forward(yk, rhs_y, g, sy, [0, 1])
    forward(yk, rhs_y, g, sy, [2, 3])
    reduce_rhs(sy, cy, 0, R, yrs)
    a0, b0 = yrs[0:R, :], yrs[R:2 * R, :]
    y_rhs = to_pair(1, yrs, yrr)

    y_coef.wait()
    first = col == 0
    a1, a2, b1, b2 = (cy[7, n] for n in range(4))
    c1, c2, d1, d2 = coef_of(ycr)
    lb2 = jnp.where(first, b2, d2)
    ra1 = jnp.where(first, c1, a1)
    inv = 1.0 / (1.0 - lb2 * ra1)
    y_rhs.wait()
    c0, d0 = yrr[0:R, :], yrr[R:2 * R, :]
    lb0 = jnp.where(first, b0, d0)
    ra0 = jnp.where(first, c0, a0)
    last_left = inv * (lb0 + lb2 * ra0)
    first_right = ra0 + ra1 * last_left
    spread(cy, 0, R, jnp.where(first, 0.0, last_left), jnp.where(first, first_right, 0.0), edge)


def last_kernel(g, yb, edge, out, y, o, out_sem):
    def put_y(b, f, rows, x):
        y[b, f, rows, :] = x

    def turn_out(c, n):
        b, f = n // F, n % F
        o[b, pl.ds(c * 128 * F + f, 128, stride=F), :] = y[c, f, PAD + b * 128:PAD + b * 128 + 128, :].T
        if f == F - 1:
            cp = pltpu.make_async_copy(o.at[b, pl.ds(pl.multiple_of(c * 128 * F, 8), 128 * F)].reshape(128, F, 128),
                                       out.at[pl.ds(c * 128, 128), b], out_sem.at[c, b])
            cp.start()

    alone, both, last = backward(yb, g, edge, put_y, turn_out)
    alone(0)

    def pair(c, carry):
        both(c, c - 1)
        return carry

    lax.fori_loop(1, NB, pair, 0)
    last(NB - 1)
    for c in range(NB):
        for b in range(NB):
            pltpu.make_async_copy(o.at[b, c * 128 * F:(c + 1) * 128 * F].reshape(128, F, 128),
                                  out.at[c * 128:(c + 1) * 128, b], out_sem.at[c, b]).wait()


def solution(mesh):
    row_count = mesh.shape["row"]
    field_spec = P(("batch", "row"), "col", None)
    coef_spec = P(("batch", "row"), "col")

    def local_step(field, x_lower, x_diag, x_upper, y_lower, y_diag, y_upper):
        words = field.reshape(T, NB, 128, F).transpose(0, 1, 3, 2)
        plane = (NB, ROWS, 128)
        fields = (NB, F, ROWS, 128)
        peers = row_count - 1
        in_vmem = pl.BlockSpec(memory_space=pltpu.VMEM)
        in_hbm = pl.BlockSpec(memory_space=pl.ANY)
        dma = pltpu.SemaphoreType.DMA
        parts = pl.pallas_call(
            functools.partial(main_kernel, row_count),
            out_shape=[pltpu.VMEM(fields, F32), pltpu.VMEM((2,) + plane, F32), pltpu.VMEM((2, R * 8, 128), F32)],
            in_specs=[in_hbm] * 7,
            out_specs=[in_vmem] * 3,
            scratch_shapes=[
                pltpu.VMEM((NB + 1, ROWS * F, 128), F32),
                pltpu.VMEM((3,) + plane, F32),
                pltpu.VMEM((2,) + plane, F32),
                pltpu.VMEM((3,) + plane, F32),
                pltpu.VMEM((3,) + plane, F32),
                pltpu.VMEM(fields, F32),
                pltpu.VMEM(fields, F32),
                pltpu.VMEM((6 * R, 8, 128), F32),
                pltpu.VMEM((6 * R, 8, 128), F32),
                pltpu.VMEM((8, 11, R, 128), F32),
                pltpu.VMEM((8, 11, R, 128), F32),
                pltpu.VMEM((2, 16, 128), F32),
                pltpu.VMEM((5 * (row_count - 2) + 8, R, 128), F32),
                pltpu.VMEM((4 * R, 128), F32),
                pltpu.VMEM((peers, 4 * R, 128), F32),
                pltpu.VMEM((2, R, 128), F32),
                pltpu.VMEM((2, peers, R, 128), F32),
                pltpu.VMEM((4 * R, 128), F32),
                pltpu.VMEM((4 * R, 128), F32),
                pltpu.VMEM((2 * R, 128), F32),
                pltpu.VMEM((2 * R, 128), F32),
                dma((3 * NB,)), dma((NB,)), dma((NB, 3)), dma, dma, dma((peers,)), dma((peers,)), dma((2, peers)), dma((2, peers)), dma((2,)), dma((2,)),
            ],
            compiler_params=pltpu.CompilerParams(
                collective_id=0, has_side_effects=True, vmem_limit_bytes=57 << 20),
        )(words, x_lower, x_diag, x_upper, y_lower, y_diag, y_upper)
        solved = pl.pallas_call(
            last_kernel,
            out_shape=jax.ShapeDtypeStruct((T, NB, F, 128), F32),
            in_specs=[in_vmem] * 3,
            out_specs=in_hbm,
            scratch_shapes=[pltpu.VMEM(fields, F32), pltpu.VMEM((NB, T * F, 128), F32), dma((NB, NB))],
            compiler_params=pltpu.CompilerParams(vmem_limit_bytes=20 << 20),
        )(*parts)
        return solved.transpose(0, 1, 3, 2).reshape(T, T, F)

    return jax.shard_map(local_step, mesh=mesh, in_specs=(field_spec,) + (coef_spec,) * 6,
                         out_specs=field_spec, check_vma=False)
```

```python
import functools

import jax
import jax.numpy as jnp
from jax import lax
from jax.experimental import pallas as pl
from jax.experimental.pallas import tpu as pltpu
from jax.sharding import PartitionSpec as P

MESH = pl.DeviceIdType.MESH
F32 = jnp.float32

T = 512
F = 4
C = 65
PAD = 8
ROWS = T + PAD
NB = T // 128
R = F * NB
UNROLL = 5

DIAG, LOW, UPP = 0, 1, 2
INV, NA, PR = 0, 1, 2
V, NC = 0, 1
A0, A1, A2, B0, B1, B2 = range(6)


H = R // 2
X_UNROLL = C


def chunk_rows(t):
    return pl.ds(t, 8, stride=C)


def row_of(b, f):
    if isinstance(b, int):
        return b // 2 * H + f * 2 + b % 2
    return lax.div(b, 2) * H + f * 2 + lax.rem(b, 2)


def beside(edge, side, b, f):
    return edge[side, pl.ds(pl.multiple_of(row_of(b, f) * 8, 8), 8), :]


def sweep(blocks, step, state, unroll=UNROLL):
    def steps(i, state):
        for n in range(unroll):
            state = step(blocks, i * unroll + n, state)
        return state
    return lax.fori_loop(0, C // unroll, steps, state)


def factor(k, kb, summ):
    sub = lax.broadcasted_iota(jnp.int32, (8, 128), 0)
    zero = jnp.zeros((8, 128), F32)

    def step(blocks, t, state):
        out = []
        fresh = sub == jnp.where(t == PAD, 0, 8)
        for b in blocks:
            nc, v, pr, a1 = state[4 * b:4 * b + 4]
            rows = chunk_rows(t)
            low = k[LOW, b, rows, :]
            den = (1.0 + k[DIAG, b, rows, :]) + low * nc
            inv = 1.0 / den
            na = -(low * inv)
            nc = -(k[UPP, b, rows, :] * inv)
            v = na * v
            pr = jnp.where(fresh, 1.0, pr)
            k[INV, b, rows, :] = inv
            k[NA, b, rows, :] = na
            k[PR, b, rows, :] = pr
            kb[NC, b, rows, :] = nc
            kb[V, b, rows, :] = v
            a1 = a1 + pr * v
            pr = pr * nc
            out += [nc, v, pr, a1]
        return tuple(out)

    state = (zero, zero + 1.0, jnp.where(sub == 0, 0.0, 1.0), zero) * NB
    state = sweep(range(NB), step, state)
    for b in range(NB):
        nc, v, pr, a1 = state[4 * b:4 * b + 4]
        for f in range(F):
            r = row_of(b, f)
            summ[A1 * R + r] = a1
            summ[A2 * R + r] = pr
            summ[B1 * R + r] = v
            summ[B2 * R + r] = nc


def of_chunk(summ, q, s, first=0, rows=R):
    return summ.reshape(6 * R * 8, 128)[pl.ds(q * R * 8 + first * 8 + s, rows, stride=8), :]


def join_coef(la1, la2, lb1, lb2, ra1, ra2, rb1, rb2):
    inv = 1.0 / (1.0 - ra1 * lb2)
    w = inv * ra1
    e1 = w * lb1
    e2 = inv * ra2
    m1 = lb1 + lb2 * e1
    m2 = lb2 * e2
    return (la1 + la2 * e1, la2 * e2, rb1 * m1, rb2 + rb1 * m2), (inv, w, lb2, la2, rb1), (e1, e2, m1, m2)


def join_rhs(part, la0, lb0, ra0, rb0):
    inv, w, lb2, la2, rb1 = part
    e0 = inv * ra0 + w * lb0
    m0 = lb0 + lb2 * e0
    return la0 + la2 * e0, rb0 + rb1 * m0, e0, m0


def reduce_coef(summ, co, send):
    def chunk(s):
        return tuple(of_chunk(summ, q, s) for q in (A1, A2, B1, B2))
    whole = chunk(0)
    for s in range(1, 8):
        whole, part, inner = join_coef(*whole, *chunk(s))
        for n, v in enumerate(part + inner):
            co[s - 1, n] = v
    for n, v in enumerate(whole):
        co[7, n] = v
        send[n * R:n * R + R, :] = v


def reduce_rhs(summ, co, first, rows, send):
    some = pl.ds(first, rows)
    a0, b0 = (of_chunk(summ, q, 0, first, rows) for q in (A0, B0))
    for s in range(1, 8):
        part = tuple(co[s - 1, n, some, :] for n in range(5))
        a0, b0, e0, m0 = join_rhs(part, a0, b0, *(of_chunk(summ, q, s, first, rows) for q in (A0, B0)))
        co[s - 1, 9, some, :] = e0
        co[s - 1, 10, some, :] = m0
    send[0:rows, :] = a0
    send[rows:2 * rows, :] = b0


def spread(co, first, rows, before, after, edge):
    def at(s):
        return pl.ds(first * 8 + s, rows, stride=8)
    some = pl.ds(first, rows)
    nxt = after
    edge[1, at(7), :] = after
    edge[0, at(0), :] = before
    for s in range(7, 0, -1):
        e1, e2, m1, m2, e0, m0 = (co[s - 1, n, some, :] for n in range(5, 11))
        edge[0, at(s), :] = (m0 + m1 * before) + m2 * nxt
        nxt = (e0 + e1 * before) + e2 * nxt
        edge[1, at(s - 1), :] = nxt


def forward(k, rhs_of, g, summ, blocks, unroll=UNROLL):
    zero = jnp.zeros((8, 128), F32)

    def step(blocks, t, state):
        out = []
        rows = chunk_rows(t)
        for j, b in enumerate(blocks):
            inv = k[INV, b, rows, :]
            na = k[NA, b, rows, :]
            pr = k[PR, b, rows, :]
            rhs = rhs_of(b, t)
            for f in range(F):
                last, first = state[2 * (j * F + f):2 * (j * F + f) + 2]
                last = inv * rhs[f] + na * last
                g[b, f, rows, :] = last
                out += [last, first + pr * last]
        return tuple(out)

    state = (zero,) * (2 * F * len(blocks))
    if unroll == C:
        for t in range(C):
            state = step(blocks, t, state)
    else:
        state = sweep(blocks, step, state, unroll)
    for j, b in enumerate(blocks):
        for f in range(F):
            summ[B0 * R + row_of(b, f)] = state[2 * (j * F + f)]
            summ[A0 * R + row_of(b, f)] = state[2 * (j * F + f) + 1]


def backward(kb, g, edge, put, turn):
    def start(b):
        return tuple(beside(edge, 1, b, f) for f in range(F))

    def step(b, n, state):
        out = []
        rows = chunk_rows(C - 1 - n)
        v = kb[V, b, rows, :]
        nc = kb[NC, b, rows, :]
        for f in range(F):
            x = (g[b, f, rows, :] + v * beside(edge, 0, b, f)) + nc * state[f]
            put(b, f, rows, x)
            out.append(x)
        return tuple(out)

    def alone(b):
        sweep(b, step, start(b))

    def both(b, before):
        state = step(b, 0, start(b))
        for n in range(NB * F):
            turn(before, n)
            for m in range(4):
                state = step(b, 1 + 4 * n + m, state)

    def last(b):
        for n in range(NB * F):
            turn(b, n)

    return alone, both, last


def main_kernel(row_count, field, xl, xd, xu, yl, yd, yu, g, yb, edge,
                u, xk, xb, yn, yk, r1, y, sx, sy, cx, cy, pack, close,
                xcs, xcr, xrs, xrr, ycs, ycr, yrs, yrr,
                in_sem, field_sem, coef_sem, ps, pr, xcss, xcrs, xrss, xrrs, yss, yrsem):
    row = lax.axis_index("row")
    col = lax.axis_index("col")
    other = 1 - col
    lane = lax.broadcasted_iota(jnp.int32, (8, 128), 1)
    zero = jnp.zeros((8, 128), F32)
    src_block = (NB - 1) * other
    src_lane = 127 * other
    dst_lane = 127 * col

    def block(n):
        return n + col * (3 - 2 * n)

    def in_field(n):
        b = block(n)
        return [pltpu.make_async_copy(field.at[pl.ds(i * 128, 128), b],
                                      u.at[b, pl.ds((PAD + i * 128) * F, 128 * F)].reshape(128, F, 128), field_sem.at[n, i])
                for i in range(NB)]

    def in_coef(n):
        b = block(n)
        return [pltpu.make_async_copy(ref.at[:, pl.ds(pl.multiple_of(b * 128, 128), 128)], yn.at[i, b, pl.ds(PAD, T)], coef_sem.at[n, i])
                for i, ref in enumerate((yd, yl, yu))]

    in_x = [pltpu.make_async_copy(ref.at[:, pl.ds(b * 128, 128)], xk.at[n, b, pl.ds(PAD, T)], in_sem.at[n, b])
            for n, ref in enumerate((xd, xl, xu)) for b in range(NB)]

    def start(copies):
        for cp in copies:
            cp.start()

    def wait(copies):
        for cp in copies:
            cp.wait()

    start(in_field(3))

    barrier = pltpu.get_barrier_semaphore()
    for d in range(1, row_count):
        pl.semaphore_signal(barrier, inc=1, device_id={"row": lax.rem(row + d, row_count)}, device_id_type=MESH)
    pl.semaphore_signal(barrier, inc=1, device_id={"col": other}, device_id_type=MESH)

    for b in range(NB):
        for n in range(3):
            yn[n, b, 0:PAD, :] = zero
            xk[n, b, 0:PAD, :] = zero - 1.0 if n == LOW else zero
            yk[n, b, 0:PAD, :] = zero - 1.0 if n == LOW else zero
        for f in range(F):
            y[b, f, 0:PAD, :] = zero
    for b in range(NB):
        u[b, 0:PAD * F, :] = jnp.zeros((PAD * F, 128), F32)
    u[NB] = jnp.zeros((ROWS * F, 128), F32)

    def line_copies(send, recv, send_sem, recv_sem):
        return [pltpu.make_async_remote_copy(send, recv.at[d - 1], send_sem.at[d - 1], recv_sem.at[d - 1],
                                             device_id={"row": lax.rem(row + d, row_count)}, device_id_type=MESH)
                for d in range(1, row_count)]

    def to_line(*refs):
        copies = line_copies(*refs)
        for cp in copies:
            cp.start()
        return copies

    def to_pair(n, send, recv):
        cp = pltpu.make_async_remote_copy(send, recv, yss.at[n], yrsem.at[n], device_id={"col": other}, device_id_type=MESH)
        cp.start()
        return cp

    start(in_x)

    wait(in_field(3))
    start(in_field(0) + in_field(1) + in_coef(0))
    from_src = jnp.bitwise_and(lane - src_lane, 127)
    for h in range(2):
        acc = zero
        for p in range(128):
            w = PAD * F + 8 * (h * 128 + p)
            acc = jnp.where(from_src == p, pltpu.roll(u[src_block, w:w + 8, :], p, 1), acc)
        pack[0, h * 8:h * 8 + 8, :] = acc
    pl.semaphore_wait(barrier, row_count)
    column = pltpu.make_async_remote_copy(pack.at[0], pack.at[1], ps, pr, device_id={"col": other}, device_id_type=MESH)
    column.start()


    wait(in_x)
    start(in_field(2) + in_coef(1) + in_coef(2) + in_coef(3))
    factor(xk, xb, sx)
    reduce_coef(sx, cx, xcs)
    coef_sends = to_line(xcs, xcr, xcss, xcrs)

    def stencil(b, t):
        rows = chunk_rows(t)
        cd = 1.0 - yn[DIAG, b, rows, :]
        cl = yn[LOW, b, rows, :]
        cu = yn[UPP, b, rows, :]
        left = lax.rem(b + NB, NB + 1)
        rhs = []
        for f in range(F):
            words = pl.ds(t * F + f, 8, stride=C * F)
            mid = u[b, words, :]
            prv = pltpu.roll(jnp.where(lane == 127, u[left, words, :], mid), 1, 1)
            nxt = pltpu.roll(jnp.where(lane == 0, u[b + 1, words, :], mid), 127, 1)
            v = (cd * mid - cl * prv) - cu * nxt
            r1[b, f, rows, :] = v
            rhs.append(v)
        return rhs

    halves = [col, other]

    def send_half(h):
        reduce_rhs(sx, cx, pl.multiple_of(halves[h] * H, 8), H, xrs.at[h])
        return to_line(xrs.at[h], xrr.at[h], xrss.at[h], xrrs.at[h])

    def eliminate(n, carry):
        wait(in_coef(n))

        @pl.when(n < 2)
        def _():
            wait(in_field(n + 1))

        @pl.when(n == 2)
        def _():
            send_half(0)

        @pl.when(n == 3)
        def _():
            column.wait()
            here = lane == dst_lane
            for i in range(2):
                got = pack[1, i * 8:i * 8 + 8, :]
                for p in range(128):
                    w = PAD * F + 8 * (i * 128 + p)
                    u[NB, w:w + 8, :] = jnp.where(here, pltpu.roll(got, (128 - p) % 128, 1), 0.0)

        forward(xk, stencil, g, sx, [block(n)], X_UNROLL)
        return carry

    wait(in_field(0))
    lax.fori_loop(0, NB, eliminate, 0)
    send_half(1)

    for b in range(NB):
        for c in range(NB):
            for n in range(3):
                yk[n, c, PAD + b * 128:PAD + b * 128 + 128, :] = yn[n, b, PAD + c * 128:PAD + c * 128 + 128, :].T
    factor(yk, yb, sy)
    reduce_coef(sy, cy, ycs)
    y_coef = to_pair(0, ycs, ycr)

    for cp in coef_sends:
        cp.wait()

    def coef_of(ref):
        return tuple(ref[q * R:q * R + R, :] for q in range(4))

    slots = range(row_count - 3, -1, -1)
    rest = coef_of(xcr.at[row_count - 2])
    known = []
    for n in slots:
        rest, part, _ = join_coef(*rest, *coef_of(xcr.at[n]))
        known += part
    p1, p2, q1, q2 = rest
    a1, a2, b1, b2 = (cx[7, n] for n in range(4))
    m12 = p1 * b1 + p2 * a1
    i11 = 1.0 / (1.0 - (p1 * b2 + p2 * a2))
    m21 = (q1 * b2 + q2 * a2) * i11
    i22 = 1.0 / ((1.0 - (q1 * b1 + q2 * a1)) - m21 * m12)
    for n, v in enumerate(known + [p1, p2, q1, q2, m12, m21, i11, i22]):
        close[n] = v

    def close_line(h):
        for cp in line_copies(xrs.at[h], xrr.at[h], xrss.at[h], xrrs.at[h]):
            cp.wait()
        first = pl.multiple_of(halves[h] * H, 8)
        known = [close[n, pl.ds(first, H), :] for n in range(5 * (row_count - 2) + 8)]

        def received(n):
            return xrr[h, n, 0:H, :], xrr[h, n, H:2 * H, :]

        p0, q0 = received(row_count - 2)
        for i, n in enumerate(slots):
            p0, q0, _, _ = join_rhs(known[5 * i:5 * i + 5], p0, q0, *received(n))
        p1, p2, q1, q2, m12, m21, i11, i22 = known[5 * (row_count - 2):]
        a0, b0 = xrs[h, 0:H, :], xrs[h, H:2 * H, :]
        s1 = (p0 + p1 * b0) + p2 * a0
        s2 = (q0 + q1 * b0) + q2 * a0
        before = i22 * (s2 + m21 * s1)
        spread(cx, first, H, before, i11 * (s1 + m12 * before), edge)

    def put_x(b, f, rows, x):
        r1[b, f, rows, :] = (x + x) - r1[b, f, rows, :]

    def turn_in(b, n):
        c, f = n // F, n % F
        y[c, f, pl.ds(pl.multiple_of(PAD + b * 128, 8), 128), :] = r1[b, f, PAD + c * 128:PAD + c * 128 + 128, :].T

    alone, both, last = backward(xb, g, edge, put_x, turn_in)

    def solve(n, carry):
        @pl.when(n == 2)
        def _():
            close_line(1)

        both(block(n), block(n - 1))
        return carry

    close_line(0)
    alone(block(0))
    lax.fori_loop(1, NB, solve, 0)
    last(block(3))

    def rhs_y(b, t):
        return [y[b, f, chunk_rows(t), :] for f in range(F)]

    forward(yk, rhs_y, g, sy, [0, 1])
    forward(yk, rhs_y, g, sy, [2, 3])
    reduce_rhs(sy, cy, 0, R, yrs)
    a0, b0 = yrs[0:R, :], yrs[R:2 * R, :]
    y_rhs = to_pair(1, yrs, yrr)

    y_coef.wait()
    first = col == 0
    a1, a2, b1, b2 = (cy[7, n] for n in range(4))
    c1, c2, d1, d2 = coef_of(ycr)
    lb2 = jnp.where(first, b2, d2)
    ra1 = jnp.where(first, c1, a1)
    inv = 1.0 / (1.0 - lb2 * ra1)
    y_rhs.wait()
    c0, d0 = yrr[0:R, :], yrr[R:2 * R, :]
    lb0 = jnp.where(first, b0, d0)
    ra0 = jnp.where(first, c0, a0)
    last_left = inv * (lb0 + lb2 * ra0)
    first_right = ra0 + ra1 * last_left
    spread(cy, 0, R, jnp.where(first, 0.0, last_left), jnp.where(first, first_right, 0.0), edge)


def last_kernel(g, yb, edge, out, y, o, out_sem):
    def put_y(b, f, rows, x):
        y[b, f, rows, :] = x

    def turn_out(c, n):
        b, f = n // F, n % F
        o[b, pl.ds(c * 128 * F + f, 128, stride=F), :] = y[c, f, PAD + b * 128:PAD + b * 128 + 128, :].T
        if f == F - 1:
            cp = pltpu.make_async_copy(o.at[b, pl.ds(pl.multiple_of(c * 128 * F, 8), 128 * F)].reshape(128, F, 128),
                                       out.at[pl.ds(c * 128, 128), b], out_sem.at[c, b])
            cp.start()

    alone, both, last = backward(yb, g, edge, put_y, turn_out)
    alone(0)

    def pair(c, carry):
        both(c, c - 1)
        return carry

    lax.fori_loop(1, NB, pair, 0)
    last(NB - 1)
    for c in range(NB):
        for b in range(NB):
            pltpu.make_async_copy(o.at[b, c * 128 * F:(c + 1) * 128 * F].reshape(128, F, 128),
                                  out.at[c * 128:(c + 1) * 128, b], out_sem.at[c, b]).wait()


def solution(mesh):
    row_count = mesh.shape["row"]
    field_spec = P(("batch", "row"), "col", None)
    coef_spec = P(("batch", "row"), "col")

    def local_step(field, x_lower, x_diag, x_upper, y_lower, y_diag, y_upper):
        words = field.reshape(T, NB, 128, F).transpose(0, 1, 3, 2)
        plane = (NB, ROWS, 128)
        fields = (NB, F, ROWS, 128)
        peers = row_count - 1
        in_vmem = pl.BlockSpec(memory_space=pltpu.VMEM)
        in_hbm = pl.BlockSpec(memory_space=pl.ANY)
        dma = pltpu.SemaphoreType.DMA
        parts = pl.pallas_call(
            functools.partial(main_kernel, row_count),
            out_shape=[pltpu.VMEM(fields, F32), pltpu.VMEM((2,) + plane, F32), pltpu.VMEM((2, R * 8, 128), F32)],
            in_specs=[in_hbm] * 7,
            out_specs=[in_vmem] * 3,
            scratch_shapes=[
                pltpu.VMEM((NB + 1, ROWS * F, 128), F32),
                pltpu.VMEM((3,) + plane, F32),
                pltpu.VMEM((2,) + plane, F32),
                pltpu.VMEM((3,) + plane, F32),
                pltpu.VMEM((3,) + plane, F32),
                pltpu.VMEM(fields, F32),
                pltpu.VMEM(fields, F32),
                pltpu.VMEM((6 * R, 8, 128), F32),
                pltpu.VMEM((6 * R, 8, 128), F32),
                pltpu.VMEM((8, 11, R, 128), F32),
                pltpu.VMEM((8, 11, R, 128), F32),
                pltpu.VMEM((2, 16, 128), F32),
                pltpu.VMEM((5 * (row_count - 2) + 8, R, 128), F32),
                pltpu.VMEM((4 * R, 128), F32),
                pltpu.VMEM((peers, 4 * R, 128), F32),
                pltpu.VMEM((2, R, 128), F32),
                pltpu.VMEM((2, peers, R, 128), F32),
                pltpu.VMEM((4 * R, 128), F32),
                pltpu.VMEM((4 * R, 128), F32),
                pltpu.VMEM((2 * R, 128), F32),
                pltpu.VMEM((2 * R, 128), F32),
                dma((3, NB)), dma((NB, NB)), dma((NB, 3)), dma, dma, dma((peers,)), dma((peers,)), dma((2, peers)), dma((2, peers)), dma((2,)), dma((2,)),
            ],
            compiler_params=pltpu.CompilerParams(
                collective_id=0, has_side_effects=True, vmem_limit_bytes=57 << 20),
        )(words, x_lower, x_diag, x_upper, y_lower, y_diag, y_upper)
        solved = pl.pallas_call(
            last_kernel,
            out_shape=jax.ShapeDtypeStruct((T, NB, F, 128), F32),
            in_specs=[in_vmem] * 3,
            out_specs=in_hbm,
            scratch_shapes=[pltpu.VMEM(fields, F32), pltpu.VMEM((NB, T * F, 128), F32), dma((NB, NB))],
            compiler_params=pltpu.CompilerParams(vmem_limit_bytes=20 << 20),
        )(*parts)
        return solved.transpose(0, 1, 3, 2).reshape(T, T, F)

    return jax.shard_map(local_step, mesh=mesh, in_specs=(field_spec,) + (coef_spec,) * 6,
                         out_specs=field_spec, check_vma=False)
```

```python
import functools

import jax
import jax.numpy as jnp
from jax import lax
from jax.experimental import pallas as pl
from jax.experimental.pallas import tpu as pltpu
from jax.sharding import PartitionSpec as P

MESH = pl.DeviceIdType.MESH
F32 = jnp.float32

T = 512
F = 4
C = 65
PAD = 8
ROWS = T + PAD
NB = T // 128
R = F * NB
UNROLL = 5

DIAG, LOW, UPP = 0, 1, 2
INV, NA, PR = 0, 1, 2
V, NC = 0, 1
A0, A1, A2, B0, B1, B2 = range(6)


H = R // 2
X_UNROLL = C


def chunk_rows(t):
    return pl.ds(t, 8, stride=C)


def row_of(b, f):
    if isinstance(b, int):
        return b // 2 * H + f * 2 + b % 2
    return lax.div(b, 2) * H + f * 2 + lax.rem(b, 2)


def beside(edge, side, b, f):
    return edge[side, pl.ds(pl.multiple_of(row_of(b, f) * 8, 8), 8), :]


def sweep(blocks, step, state, unroll=UNROLL):
    def steps(i, state):
        for n in range(unroll):
            state = step(blocks, i * unroll + n, state)
        return state
    return lax.fori_loop(0, C // unroll, steps, state)


def factor(k, kb, summ):
    sub = lax.broadcasted_iota(jnp.int32, (8, 128), 0)
    zero = jnp.zeros((8, 128), F32)

    def step(blocks, t, state):
        out = []
        fresh = sub == jnp.where(t == PAD, 0, 8)
        for b in blocks:
            nc, v, pr, a1 = state[4 * b:4 * b + 4]
            rows = chunk_rows(t)
            low = k[LOW, b, rows, :]
            den = (1.0 + k[DIAG, b, rows, :]) + low * nc
            inv = 1.0 / den
            na = -(low * inv)
            nc = -(k[UPP, b, rows, :] * inv)
            v = na * v
            pr = jnp.where(fresh, 1.0, pr)
            k[INV, b, rows, :] = inv
            k[NA, b, rows, :] = na
            k[PR, b, rows, :] = pr
            kb[NC, b, rows, :] = nc
            kb[V, b, rows, :] = v
            a1 = a1 + pr * v
            pr = pr * nc
            out += [nc, v, pr, a1]
        return tuple(out)

    state = (zero, zero + 1.0, jnp.where(sub == 0, 0.0, 1.0), zero) * NB
    state = sweep(range(NB), step, state)
    for b in range(NB):
        nc, v, pr, a1 = state[4 * b:4 * b + 4]
        for f in range(F):
            r = row_of(b, f)
            summ[A1 * R + r] = a1
            summ[A2 * R + r] = pr
            summ[B1 * R + r] = v
            summ[B2 * R + r] = nc


def of_chunk(summ, q, s, first=0, rows=R):
    return summ.reshape(6 * R * 8, 128)[pl.ds(q * R * 8 + first * 8 + s, rows, stride=8), :]


def join_coef(la1, la2, lb1, lb2, ra1, ra2, rb1, rb2):
    inv = 1.0 / (1.0 - ra1 * lb2)
    w = inv * ra1
    e1 = w * lb1
    e2 = inv * ra2
    m1 = lb1 + lb2 * e1
    m2 = lb2 * e2
    return (la1 + la2 * e1, la2 * e2, rb1 * m1, rb2 + rb1 * m2), (inv, w, lb2, la2, rb1), (e1, e2, m1, m2)


def join_rhs(part, la0, lb0, ra0, rb0):
    inv, w, lb2, la2, rb1 = part
    e0 = inv * ra0 + w * lb0
    m0 = lb0 + lb2 * e0
    return la0 + la2 * e0, rb0 + rb1 * m0, e0, m0


def reduce_coef(summ, co, send):
    def chunk(s):
        return tuple(of_chunk(summ, q, s) for q in (A1, A2, B1, B2))
    whole = chunk(0)
    for s in range(1, 8):
        whole, part, inner = join_coef(*whole, *chunk(s))
        for n, v in enumerate(part + inner):
            co[s - 1, n] = v
    for n, v in enumerate(whole):
        co[7, n] = v
        send[n * R:n * R + R, :] = v


def reduce_rhs(summ, co, first, rows, send):
    some = pl.ds(first, rows)
    a0, b0 = (of_chunk(summ, q, 0, first, rows) for q in (A0, B0))
    for s in range(1, 8):
        part = tuple(co[s - 1, n, some, :] for n in range(5))
        a0, b0, e0, m0 = join_rhs(part, a0, b0, *(of_chunk(summ, q, s, first, rows) for q in (A0, B0)))
        co[s - 1, 9, some, :] = e0
        co[s - 1, 10, some, :] = m0
    send[0:rows, :] = a0
    send[rows:2 * rows, :] = b0


def spread(co, first, rows, before, after, edge, rhs=True):
    def at(s):
        return pl.ds(first * 8 + s, rows, stride=8)
    some = pl.ds(first, rows)
    nxt = after
    edge[1, at(7), :] = after
    edge[0, at(0), :] = before
    for s in range(7, 0, -1):
        e1, e2, m1, m2, e0, m0 = (co[s - 1, n, some, :] for n in range(5, 11))
        last = m1 * before + m2 * nxt
        nxt = e1 * before + e2 * nxt
        if rhs:
            last, nxt = m0 + last, e0 + nxt
        edge[0, at(s), :] = last
        edge[1, at(s - 1), :] = nxt


def forward(k, rhs_of, g, summ, blocks, unroll=UNROLL):
    zero = jnp.zeros((8, 128), F32)

    def step(blocks, t, state):
        out = []
        rows = chunk_rows(t)
        for j, b in enumerate(blocks):
            inv = k[INV, b, rows, :]
            na = k[NA, b, rows, :]
            pr = k[PR, b, rows, :]
            rhs = rhs_of(b, t)
            for f in range(F):
                last, first = state[2 * (j * F + f):2 * (j * F + f) + 2]
                last = inv * rhs[f] + na * last
                g[b, f, rows, :] = last
                out += [last, first + pr * last]
        return tuple(out)

    state = (zero,) * (2 * F * len(blocks))
    if unroll == C:
        for t in range(C):
            state = step(blocks, t, state)
    else:
        state = sweep(blocks, step, state, unroll)
    for j, b in enumerate(blocks):
        for f in range(F):
            summ[B0 * R + row_of(b, f)] = state[2 * (j * F + f)]
            summ[A0 * R + row_of(b, f)] = state[2 * (j * F + f) + 1]


def backward(kb, g, edge, put, turn):
    def start(b):
        return tuple(beside(edge, 1, b, f) for f in range(F))

    def stepper(b):
        near = [beside(edge, 0, b, f) for f in range(F)]

        def step(_, n, state):
            out = []
            rows = chunk_rows(C - 1 - n)
            v = kb[V, b, rows, :]
            nc = kb[NC, b, rows, :]
            for f in range(F):
                x = (g[b, f, rows, :] + v * near[f]) + nc * state[f]
                put(b, f, rows, x)
                out.append(x)
            return tuple(out)
        return step

    def alone(b):
        sweep(b, stepper(b), start(b))

    def both(b, before):
        step = stepper(b)
        state = step(b, 0, start(b))
        for n in range(NB * F):
            turn(before, n)
            for m in range(4):
                state = step(b, 1 + 4 * n + m, state)

    def last(b):
        for n in range(NB * F):
            turn(b, n)

    return alone, both, last


def main_kernel(row_count, field, xl, xd, xu, yl, yd, yu, y, answer, ends,
                u, xk, xb, yn, yk, yb, r1, g, edge, sx, sy, cx, cy, pack, close,
                xcs, xcr, xrs, xrr, ycs, ycr, yrs, yrr,
                in_sem, field_sem, coef_sem, ps, pr, xcss, xcrs, xrss, xrrs, yss, yrsem):
    row = lax.axis_index("row")
    col = lax.axis_index("col")
    other = 1 - col
    lane = lax.broadcasted_iota(jnp.int32, (8, 128), 1)
    zero = jnp.zeros((8, 128), F32)
    src_block = (NB - 1) * other
    src_lane = 127 * other
    dst_lane = 127 * col

    def block(n):
        return n + col * (3 - 2 * n)

    def in_field(n):
        b = block(n)
        return [pltpu.make_async_copy(field.at[pl.ds(i * 128, 128), b],
                                      u.at[b, pl.ds((PAD + i * 128) * F, 128 * F)].reshape(128, F, 128), field_sem.at[n, i])
                for i in range(NB)]

    def in_coef(n):
        b = block(n)
        return [pltpu.make_async_copy(ref.at[:, pl.ds(pl.multiple_of(b * 128, 128), 128)], yn.at[i, b, pl.ds(PAD, T)], coef_sem.at[n, i])
                for i, ref in enumerate((yd, yl, yu))]

    in_x = [pltpu.make_async_copy(ref.at[:, pl.ds(b * 128, 128)], xk.at[n, b, pl.ds(PAD, T)], in_sem.at[n, b])
            for n, ref in enumerate((xd, xl, xu)) for b in range(NB)]

    def start(copies):
        for cp in copies:
            cp.start()

    def wait(copies):
        for cp in copies:
            cp.wait()

    start(in_field(3))

    barrier = pltpu.get_barrier_semaphore()
    for d in range(1, row_count):
        pl.semaphore_signal(barrier, inc=1, device_id={"row": lax.rem(row + d, row_count)}, device_id_type=MESH)
    pl.semaphore_signal(barrier, inc=1, device_id={"col": other}, device_id_type=MESH)

    for b in range(NB):
        for n in range(3):
            yn[n, b, 0:PAD, :] = zero
            xk[n, b, 0:PAD, :] = zero - 1.0 if n == LOW else zero
            yk[n, b, 0:PAD, :] = zero - 1.0 if n == LOW else zero
        for f in range(F):
            y[b, f, 0:PAD, :] = zero
    for b in range(NB):
        u[b, 0:PAD * F, :] = jnp.zeros((PAD * F, 128), F32)
    u[NB] = jnp.zeros((ROWS * F, 128), F32)

    def line_copies(send, recv, send_sem, recv_sem):
        return [pltpu.make_async_remote_copy(send, recv.at[d - 1], send_sem.at[d - 1], recv_sem.at[d - 1],
                                             device_id={"row": lax.rem(row + d, row_count)}, device_id_type=MESH)
                for d in range(1, row_count)]

    def to_line(*refs):
        copies = line_copies(*refs)
        for cp in copies:
            cp.start()
        return copies

    def to_pair(n, send, recv):
        cp = pltpu.make_async_remote_copy(send, recv, yss.at[n], yrsem.at[n], device_id={"col": other}, device_id_type=MESH)
        cp.start()
        return cp

    start(in_x)

    wait(in_field(3))
    start(in_field(0) + in_field(1) + in_coef(0))
    from_src = jnp.bitwise_and(lane - src_lane, 127)
    for h in range(2):
        acc = zero
        for p in range(128):
            w = PAD * F + 8 * (h * 128 + p)
            acc = jnp.where(from_src == p, pltpu.roll(u[src_block, w:w + 8, :], p, 1), acc)
        pack[0, h * 8:h * 8 + 8, :] = acc
    pl.semaphore_wait(barrier, row_count)
    column = pltpu.make_async_remote_copy(pack.at[0], pack.at[1], ps, pr, device_id={"col": other}, device_id_type=MESH)
    column.start()


    wait(in_x)
    start(in_field(2) + in_coef(1) + in_coef(2) + in_coef(3))
    factor(xk, xb, sx)
    reduce_coef(sx, cx, xcs)
    coef_sends = to_line(xcs, xcr, xcss, xcrs)

    def stencil(b, t):
        rows = chunk_rows(t)
        cd = 1.0 - yn[DIAG, b, rows, :]
        cl = yn[LOW, b, rows, :]
        cu = yn[UPP, b, rows, :]
        left = lax.rem(b + NB, NB + 1)
        rhs = []
        for f in range(F):
            words = pl.ds(t * F + f, 8, stride=C * F)
            mid = u[b, words, :]
            prv = pltpu.roll(jnp.where(lane == 127, u[left, words, :], mid), 1, 1)
            nxt = pltpu.roll(jnp.where(lane == 0, u[b + 1, words, :], mid), 127, 1)
            v = (cd * mid - cl * prv) - cu * nxt
            r1[b, f, rows, :] = v
            rhs.append(v)
        return rhs

    halves = [col, other]

    def send_half(h):
        reduce_rhs(sx, cx, pl.multiple_of(halves[h] * H, 8), H, xrs.at[h])
        return to_line(xrs.at[h], xrr.at[h], xrss.at[h], xrrs.at[h])

    def eliminate(n, carry):
        wait(in_coef(n))

        @pl.when(n < 2)
        def _():
            wait(in_field(n + 1))

        @pl.when(n == 2)
        def _():
            send_half(0)

        @pl.when(n == 3)
        def _():
            column.wait()
            here = lane == dst_lane
            for i in range(2):
                got = pack[1, i * 8:i * 8 + 8, :]
                for p in range(128):
                    w = PAD * F + 8 * (i * 128 + p)
                    u[NB, w:w + 8, :] = jnp.where(here, pltpu.roll(got, (128 - p) % 128, 1), 0.0)

        forward(xk, stencil, g, sx, [block(n)], X_UNROLL)
        return carry

    wait(in_field(0))
    lax.fori_loop(0, NB, eliminate, 0)
    send_half(1)

    for b in range(NB):
        for c in range(NB):
            for n in range(3):
                yk[n, c, PAD + b * 128:PAD + b * 128 + 128, :] = yn[n, b, PAD + c * 128:PAD + c * 128 + 128, :].T
    factor(yk, yb, sy)
    reduce_coef(sy, cy, ycs)
    y_coef = to_pair(0, ycs, ycr)

    for cp in coef_sends:
        cp.wait()

    def coef_of(ref):
        return tuple(ref[q * R:q * R + R, :] for q in range(4))

    slots = range(row_count - 3, -1, -1)
    rest = coef_of(xcr.at[row_count - 2])
    known = []
    for n in slots:
        rest, part, _ = join_coef(*rest, *coef_of(xcr.at[n]))
        known += part
    p1, p2, q1, q2 = rest
    a1, a2, b1, b2 = (cx[7, n] for n in range(4))
    m12 = p1 * b1 + p2 * a1
    i11 = 1.0 / (1.0 - (p1 * b2 + p2 * a2))
    m21 = (q1 * b2 + q2 * a2) * i11
    i22 = 1.0 / ((1.0 - (q1 * b1 + q2 * a1)) - m21 * m12)
    for n, v in enumerate(known + [p1, p2, q1, q2, m12, m21, i11, i22]):
        close[n] = v

    def close_line(h):
        for cp in line_copies(xrs.at[h], xrr.at[h], xrss.at[h], xrrs.at[h]):
            cp.wait()
        first = pl.multiple_of(halves[h] * H, 8)
        known = [close[n, pl.ds(first, H), :] for n in range(5 * (row_count - 2) + 8)]

        def received(n):
            return xrr[h, n, 0:H, :], xrr[h, n, H:2 * H, :]

        p0, q0 = received(row_count - 2)
        for i, n in enumerate(slots):
            p0, q0, _, _ = join_rhs(known[5 * i:5 * i + 5], p0, q0, *received(n))
        p1, p2, q1, q2, m12, m21, i11, i22 = known[5 * (row_count - 2):]
        a0, b0 = xrs[h, 0:H, :], xrs[h, H:2 * H, :]
        s1 = (p0 + p1 * b0) + p2 * a0
        s2 = (q0 + q1 * b0) + q2 * a0
        before = i22 * (s2 + m21 * s1)
        spread(cx, first, H, before, i11 * (s1 + m12 * before), edge)

    def put_x(b, f, rows, x):
        r1[b, f, rows, :] = (x + x) - r1[b, f, rows, :]

    def turn_in(b, n):
        c, f = n // F, n % F
        y[c, f, pl.ds(pl.multiple_of(PAD + b * 128, 8), 128), :] = r1[b, f, PAD + c * 128:PAD + c * 128 + 128, :].T

    alone, both, last = backward(xb, g, edge, put_x, turn_in)

    def solve(n, carry):
        @pl.when(n == 2)
        def _():
            close_line(1)

        both(block(n), block(n - 1))
        return carry

    close_line(0)
    alone(block(0))
    lax.fori_loop(1, NB, solve, 0)
    last(block(3))

    def rhs_y(b, t):
        return [y[b, f, chunk_rows(t), :] for f in range(F)]

    forward(yk, rhs_y, g, sy, [0, 1])
    forward(yk, rhs_y, g, sy, [2, 3])
    reduce_rhs(sy, cy, 0, R, yrs)
    first = col == 0
    give = pl.multiple_of(other * R, 8)
    take = pl.multiple_of(col * R, 8)
    y_rhs = to_pair(1, yrs.at[pl.ds(give, R)], yrr)

    nothing = jnp.zeros((R, 128), F32)
    spread(cy, 0, R, nothing, nothing, edge)

    def put_y(b, f, rows, x):
        y[b, f, rows, :] = x

    alone, _, _ = backward(yb, g, edge, put_y, None)

    def solve_y(b, carry):
        alone(b)
        return carry

    lax.fori_loop(0, NB, solve_y, 0)
    one_left = jnp.where(first, 0.0, 1.0) + nothing
    spread(cy, 0, R, one_left, 1.0 - one_left, edge, False)
    near = [beside(edge, 0, b, 0) for b in range(NB)]

    def step_h(blocks, n, state):
        rows = chunk_rows(C - 1 - n)
        out = []
        for b in blocks:
            out.append(yb[V, b, rows, :] * near[b] + yb[NC, b, rows, :] * state[b])
            answer[b, rows, :] = out[b]
        return tuple(out)

    sweep(range(NB), step_h, tuple(beside(edge, 1, b, 0) for b in range(NB)))

    y_coef.wait()
    a1, b2 = cy[7, 0], cy[7, 3]
    c1, d2 = ycr[0:R, :], ycr[3 * R:4 * R, :]
    lb2 = jnp.where(first, b2, d2)
    ra1 = jnp.where(first, c1, a1)
    inv = 1.0 / (1.0 - lb2 * ra1)
    y_rhs.wait()
    mine = yrs[pl.ds(give, R), :]
    theirs = yrr[...]
    lb0 = jnp.where(first, mine, theirs)
    ra0 = jnp.where(first, theirs, mine)
    last_left = inv * (lb0 + lb2 * ra0)
    ends[...] = jnp.where(first, ra0 + ra1 * last_left, last_left)


def last_kernel(y, h, ends, out, o, out_sem):
    def copy_out(c, b):
        return pltpu.make_async_copy(o.at[b, pl.ds(pl.multiple_of(c * 128 * F, 8), 128 * F)].reshape(128, F, 128),
                                     out.at[pl.ds(c * 128, 128), b], out_sem.at[c, b])

    def turn_out(c, carry):
        for b in range(NB):
            part = h[c, PAD + b * 128:PAD + b * 128 + 128, :]
            for f in range(F):
                end = jnp.broadcast_to(ends[pl.ds(row_of(c, f), 1), :], (128, 128))
                o[b, pl.ds(c * 128 * F + f, 128, stride=F), :] = (
                    y[c, f, PAD + b * 128:PAD + b * 128 + 128, :] + part * end).T
            copy_out(c, b).start()
        return carry

    lax.fori_loop(0, NB, turn_out, 0)
    for c in range(NB):
        for b in range(NB):
            copy_out(c, b).wait()


def solution(mesh):
    row_count = mesh.shape["row"]
    field_spec = P(("batch", "row"), "col", None)
    coef_spec = P(("batch", "row"), "col")

    def local_step(field, x_lower, x_diag, x_upper, y_lower, y_diag, y_upper):
        words = field.reshape(T, NB, 128, F).transpose(0, 1, 3, 2)
        plane = (NB, ROWS, 128)
        fields = (NB, F, ROWS, 128)
        peers = row_count - 1
        in_vmem = pl.BlockSpec(memory_space=pltpu.VMEM)
        in_hbm = pl.BlockSpec(memory_space=pl.ANY)
        dma = pltpu.SemaphoreType.DMA
        parts = pl.pallas_call(
            functools.partial(main_kernel, row_count),
            out_shape=[pltpu.VMEM(fields, F32), pltpu.VMEM(plane, F32), pltpu.VMEM((R, 128), F32)],
            in_specs=[in_hbm] * 7,
            out_specs=[in_vmem] * 3,
            scratch_shapes=[
                pltpu.VMEM((NB + 1, ROWS * F, 128), F32),
                pltpu.VMEM((3,) + plane, F32),
                pltpu.VMEM((2,) + plane, F32),
                pltpu.VMEM((3,) + plane, F32),
                pltpu.VMEM((3,) + plane, F32),
                pltpu.VMEM((2,) + plane, F32),
                pltpu.VMEM(fields, F32),
                pltpu.VMEM(fields, F32),
                pltpu.VMEM((2, R * 8, 128), F32),
                pltpu.VMEM((6 * R, 8, 128), F32),
                pltpu.VMEM((6 * R, 8, 128), F32),
                pltpu.VMEM((8, 11, R, 128), F32),
                pltpu.VMEM((8, 11, R, 128), F32),
                pltpu.VMEM((2, 16, 128), F32),
                pltpu.VMEM((5 * (row_count - 2) + 8, R, 128), F32),
                pltpu.VMEM((4 * R, 128), F32),
                pltpu.VMEM((peers, 4 * R, 128), F32),
                pltpu.VMEM((2, R, 128), F32),
                pltpu.VMEM((2, peers, R, 128), F32),
                pltpu.VMEM((4 * R, 128), F32),
                pltpu.VMEM((4 * R, 128), F32),
                pltpu.VMEM((2 * R, 128), F32),
                pltpu.VMEM((R, 128), F32),
                dma((3, NB)), dma((NB, NB)), dma((NB, 3)), dma, dma, dma((peers,)), dma((peers,)), dma((2, peers)), dma((2, peers)), dma((2,)), dma((2,)),
            ],
            compiler_params=pltpu.CompilerParams(
                collective_id=0, has_side_effects=True, vmem_limit_bytes=58 << 20),
        )(words, x_lower, x_diag, x_upper, y_lower, y_diag, y_upper)
        solved = pl.pallas_call(
            last_kernel,
            out_shape=jax.ShapeDtypeStruct((T, NB, F, 128), F32),
            in_specs=[in_vmem] * 3,
            out_specs=in_hbm,
            scratch_shapes=[pltpu.VMEM((NB, T * F, 128), F32), dma((NB, NB))],
            compiler_params=pltpu.CompilerParams(vmem_limit_bytes=16 << 20),
        )(*parts)
        return solved.transpose(0, 1, 3, 2).reshape(T, T, F)

    return jax.shard_map(local_step, mesh=mesh, in_specs=(field_spec,) + (coef_spec,) * 6,
                         out_specs=field_spec, check_vma=False)
```

```python
import functools

import jax
import jax.numpy as jnp
from jax import lax
from jax.experimental import pallas as pl
from jax.experimental.pallas import tpu as pltpu
from jax.sharding import PartitionSpec as P

MESH = pl.DeviceIdType.MESH
F32 = jnp.float32

T = 512
F = 4
C = 65
PAD = 8
ROWS = T + PAD
NB = T // 128
R = F * NB
UNROLL = 5

DIAG, LOW, UPP = 0, 1, 2
INV, NA, PR = 0, 1, 2
V, NC = 0, 1
A0, A1, A2, B0, B1, B2 = range(6)


H = R // 2
X_UNROLL = C


def chunk_rows(t):
    return pl.ds(t, 8, stride=C)


def row_of(b, f):
    if isinstance(b, int):
        return b // 2 * H + f * 2 + b % 2
    return lax.div(b, 2) * H + f * 2 + lax.rem(b, 2)


def beside(edge, side, b, f):
    return edge[side, pl.ds(pl.multiple_of(row_of(b, f) * 8, 8), 8), :]


def sweep(blocks, step, state, unroll=UNROLL, side=None):
    ahead = C % unroll
    for n in range(ahead):
        state = step(blocks, n, state)

    def steps(i, state):
        if side is not None:
            side(i)
        for n in range(unroll):
            state = step(blocks, ahead + i * unroll + n, state)
        return state
    return lax.fori_loop(0, C // unroll, steps, state)


def factor(k, kb, summ):
    sub = lax.broadcasted_iota(jnp.int32, (8, 128), 0)
    zero = jnp.zeros((8, 128), F32)

    def step(blocks, t, state):
        out = []
        fresh = sub == jnp.where(t == PAD, 0, 8)
        for b in blocks:
            nc, v, pr, a1 = state[4 * b:4 * b + 4]
            rows = chunk_rows(t)
            low = k[LOW, b, rows, :]
            den = (1.0 + k[DIAG, b, rows, :]) + low * nc
            inv = 1.0 / den
            na = (0.0 - low) * inv
            nc = (0.0 - k[UPP, b, rows, :]) * inv
            v = na * v
            pr = jnp.where(fresh, 1.0, pr)
            k[INV, b, rows, :] = inv
            k[NA, b, rows, :] = na
            k[PR, b, rows, :] = pr
            kb[NC, b, rows, :] = nc
            kb[V, b, rows, :] = v
            a1 = a1 + pr * v
            pr = pr * nc
            out += [nc, v, pr, a1]
        return tuple(out)

    state = (zero, zero + 1.0, jnp.where(sub == 0, 0.0, 1.0), zero) * NB
    state = sweep(range(NB), step, state)
    for b in range(NB):
        nc, v, pr, a1 = state[4 * b:4 * b + 4]
        for f in range(F):
            r = row_of(b, f)
            summ[A1 * R + r] = a1
            summ[A2 * R + r] = pr
            summ[B1 * R + r] = v
            summ[B2 * R + r] = nc


def of_chunk(summ, q, s, first=0, rows=R):
    return summ.reshape(6 * R * 8, 128)[pl.ds(q * R * 8 + first * 8 + s, rows, stride=8), :]


def join_coef(la1, la2, lb1, lb2, ra1, ra2, rb1, rb2):
    inv = 1.0 / (1.0 - ra1 * lb2)
    w = inv * ra1
    e1 = w * lb1
    e2 = inv * ra2
    m1 = lb1 + lb2 * e1
    m2 = lb2 * e2
    return (la1 + la2 * e1, la2 * e2, rb1 * m1, rb2 + rb1 * m2), (inv, w, lb2, la2, rb1), (e1, e2, m1, m2)


def join_rhs(part, la0, lb0, ra0, rb0):
    inv, w, lb2, la2, rb1 = part
    e0 = inv * ra0 + w * lb0
    m0 = lb0 + lb2 * e0
    return la0 + la2 * e0, rb0 + rb1 * m0, e0, m0


def reduce_coef(summ, co, send):
    def chunk(s):
        return tuple(of_chunk(summ, q, s) for q in (A1, A2, B1, B2))
    whole = chunk(0)
    for s in range(1, 8):
        whole, part, inner = join_coef(*whole, *chunk(s))
        for n, v in enumerate(part + inner):
            co[s - 1, n] = v
    for n, v in enumerate(whole):
        co[7, n] = v
        send[n * R:n * R + R, :] = v


def reduce_rhs(summ, co, first, rows, send):
    some = pl.ds(first, rows)
    a0, b0 = (of_chunk(summ, q, 0, first, rows) for q in (A0, B0))
    for s in range(1, 8):
        part = tuple(co[s - 1, n, some, :] for n in range(5))
        a0, b0, e0, m0 = join_rhs(part, a0, b0, *(of_chunk(summ, q, s, first, rows) for q in (A0, B0)))
        co[s - 1, 9, some, :] = e0
        co[s - 1, 10, some, :] = m0
    send[0:rows, :] = a0
    send[rows:2 * rows, :] = b0


def spread(co, first, rows, before, after, edge, rhs=True):
    def at(s):
        return pl.ds(first * 8 + s, rows, stride=8)
    some = pl.ds(first, rows)
    nxt = after
    edge[1, at(7), :] = after
    edge[0, at(0), :] = before
    for s in range(7, 0, -1):
        e1, e2, m1, m2, e0, m0 = (co[s - 1, n, some, :] for n in range(5, 11))
        last = m1 * before + m2 * nxt
        nxt = e1 * before + e2 * nxt
        if rhs:
            last, nxt = m0 + last, e0 + nxt
        edge[0, at(s), :] = last
        edge[1, at(s - 1), :] = nxt


def forward(k, rhs_of, g, summ, blocks, unroll=UNROLL, side=None):
    zero = jnp.zeros((8, 128), F32)

    def step(blocks, t, state):
        out = []
        rows = chunk_rows(t)
        for j, b in enumerate(blocks):
            inv = k[INV, b, rows, :]
            na = k[NA, b, rows, :]
            pr = k[PR, b, rows, :]
            rhs = rhs_of(b, t)
            for f in range(F):
                last, first = state[2 * (j * F + f):2 * (j * F + f) + 2]
                last = inv * rhs[f] + na * last
                g[b, f, rows, :] = last
                out += [last, first + pr * last]
        return tuple(out)

    state = (zero,) * (2 * F * len(blocks))
    if unroll == C:
        for t in range(C):
            state = step(blocks, t, state)
    else:
        state = sweep(blocks, step, state, unroll, side)
    for j, b in enumerate(blocks):
        for f in range(F):
            summ[B0 * R + row_of(b, f)] = state[2 * (j * F + f)]
            summ[A0 * R + row_of(b, f)] = state[2 * (j * F + f) + 1]


def backward(kb, g, edge, put, turn):
    def start(b):
        return tuple(beside(edge, 1, b, f) for f in range(F))

    def stepper(b):
        near = [beside(edge, 0, b, f) for f in range(F)]

        def step(_, n, state):
            out = []
            rows = chunk_rows(C - 1 - n)
            v = kb[V, b, rows, :]
            nc = kb[NC, b, rows, :]
            for f in range(F):
                x = (g[b, f, rows, :] + v * near[f]) + nc * state[f]
                put(b, f, rows, x)
                out.append(x)
            return tuple(out)
        return step

    def alone(b):
        sweep(b, stepper(b), start(b), 13)

    def both(b, before):
        step = stepper(b)
        state = step(b, 0, start(b))
        for n in range(NB * F):
            turn(before, n)
            for m in range(4):
                state = step(b, 1 + 4 * n + m, state)

    return alone, both


def main_kernel(row_count, field, xl, xd, xu, yl, yd, yu, y, answer, ends,
                u, xk, xb, yn, yk, yb, r1, g, edge, sx, sy, cx, cy, pack, close,
                xcs, xcr, xrs, xrr, ycs, ycr, yrs, yrr,
                in_sem, field_sem, coef_sem, ps, pr, xcss, xcrs, xrss, xrrs, yss, yrsem):
    row = lax.axis_index("row")
    col = lax.axis_index("col")
    other = 1 - col
    lane = lax.broadcasted_iota(jnp.int32, (8, 128), 1)
    zero = jnp.zeros((8, 128), F32)
    src_block = (NB - 1) * other
    src_lane = 127 * other
    dst_lane = 127 * col

    def block(n):
        return n + col * (3 - 2 * n)

    def in_field(n):
        b = block(n)
        return [pltpu.make_async_copy(field.at[pl.ds(i * 128, 128), b],
                                      u.at[b, pl.ds((PAD + i * 128) * F, 128 * F)].reshape(128, F, 128), field_sem.at[n, i])
                for i in range(NB)]

    def in_coef(n):
        b = block(n)
        return [pltpu.make_async_copy(ref.at[:, pl.ds(pl.multiple_of(b * 128, 128), 128)], yn.at[i, b, pl.ds(PAD, T)], coef_sem.at[n, i])
                for i, ref in enumerate((yd, yl, yu))]

    in_x = [pltpu.make_async_copy(ref.at[:, pl.ds(b * 128, 128)], xk.at[n, b, pl.ds(PAD, T)], in_sem.at[n, b])
            for n, ref in enumerate((xd, xl, xu)) for b in range(NB)]

    def start(copies):
        for cp in copies:
            cp.start()

    def wait(copies):
        for cp in copies:
            cp.wait()

    start(in_field(3))

    barrier = pltpu.get_barrier_semaphore()
    for d in range(1, row_count):
        pl.semaphore_signal(barrier, inc=1, device_id={"row": lax.rem(row + d, row_count)}, device_id_type=MESH)
    pl.semaphore_signal(barrier, inc=1, device_id={"col": other}, device_id_type=MESH)

    for b in range(NB):
        for n in range(3):
            yn[n, b, 0:PAD, :] = zero
            xk[n, b, 0:PAD, :] = zero - 1.0 if n == LOW else zero
            yk[n, b, 0:PAD, :] = zero - 1.0 if n == LOW else zero
        for f in range(F):
            y[b, f, 0:PAD, :] = zero
    for b in range(NB):
        u[b, 0:PAD * F, :] = jnp.zeros((PAD * F, 128), F32)
    u[NB] = jnp.zeros((ROWS * F, 128), F32)

    def line_copies(send, recv, send_sem, recv_sem):
        return [pltpu.make_async_remote_copy(send, recv.at[d - 1], send_sem.at[d - 1], recv_sem.at[d - 1],
                                             device_id={"row": lax.rem(row + d, row_count)}, device_id_type=MESH)
                for d in range(1, row_count)]

    def to_line(*refs):
        copies = line_copies(*refs)
        for cp in copies:
            cp.start()
        return copies

    def to_pair(n, send, recv):
        cp = pltpu.make_async_remote_copy(send, recv, yss.at[n], yrsem.at[n], device_id={"col": other}, device_id_type=MESH)
        cp.start()
        return cp

    start(in_x)

    wait(in_field(3))
    start(in_field(0) + in_field(1) + in_coef(0))
    from_src = jnp.bitwise_and(lane - src_lane, 127)
    for h in range(2):
        acc = zero
        for p in range(128):
            w = PAD * F + 8 * (h * 128 + p)
            acc = jnp.where(from_src == p, pltpu.roll(u[src_block, w:w + 8, :], p, 1), acc)
        pack[0, h * 8:h * 8 + 8, :] = acc
    pl.semaphore_wait(barrier, row_count)
    column = pltpu.make_async_remote_copy(pack.at[0], pack.at[1], ps, pr, device_id={"col": other}, device_id_type=MESH)
    column.start()


    wait(in_x)
    start(in_field(2) + in_coef(1) + in_coef(2) + in_coef(3))
    factor(xk, xb, sx)
    reduce_coef(sx, cx, xcs)
    coef_sends = to_line(xcs, xcr, xcss, xcrs)

    def stencil(b, t):
        rows = chunk_rows(t)
        cd = 1.0 - yn[DIAG, b, rows, :]
        cl = yn[LOW, b, rows, :]
        cu = yn[UPP, b, rows, :]
        left = lax.rem(b + NB, NB + 1)
        rhs = []
        for f in range(F):
            words = pl.ds(t * F + f, 8, stride=C * F)
            mid = u[b, words, :]
            prv = pltpu.roll(jnp.where(lane == 127, u[left, words, :], mid), 1, 1)
            nxt = pltpu.roll(jnp.where(lane == 0, u[b + 1, words, :], mid), 127, 1)
            v = (cd * mid - cl * prv) - cu * nxt
            r1[b, f, rows, :] = v
            rhs.append(v)
        return rhs

    halves = [col, other]

    def send_half(h):
        reduce_rhs(sx, cx, pl.multiple_of(halves[h] * H, 8), H, xrs.at[h])
        return to_line(xrs.at[h], xrr.at[h], xrss.at[h], xrrs.at[h])

    def eliminate(n, carry):
        wait(in_coef(n))

        @pl.when(n < 2)
        def _():
            wait(in_field(n + 1))

        @pl.when(n == 2)
        def _():
            send_half(0)

        @pl.when(n == 3)
        def _():
            column.wait()
            here = lane == dst_lane
            for i in range(2):
                got = pack[1, i * 8:i * 8 + 8, :]
                for p in range(128):
                    w = PAD * F + 8 * (i * 128 + p)
                    u[NB, w:w + 8, :] = jnp.where(here, pltpu.roll(got, (128 - p) % 128, 1), 0.0)

        forward(xk, stencil, g, sx, [block(n)], X_UNROLL)
        return carry

    wait(in_field(0))
    lax.fori_loop(0, NB, eliminate, 0)
    send_half(1)

    for b in range(NB):
        for c in range(NB):
            for n in range(3):
                yk[n, c, PAD + b * 128:PAD + b * 128 + 128, :] = yn[n, b, PAD + c * 128:PAD + c * 128 + 128, :].T
    factor(yk, yb, sy)
    reduce_coef(sy, cy, ycs)
    y_coef = to_pair(0, ycs, ycr)

    for cp in coef_sends:
        cp.wait()

    def coef_of(ref):
        return tuple(ref[q * R:q * R + R, :] for q in range(4))

    slots = range(row_count - 3, -1, -1)
    rest = coef_of(xcr.at[row_count - 2])
    known = []
    for n in slots:
        rest, part, _ = join_coef(*rest, *coef_of(xcr.at[n]))
        known += part
    p1, p2, q1, q2 = rest
    a1, a2, b1, b2 = (cx[7, n] for n in range(4))
    m12 = p1 * b1 + p2 * a1
    i11 = 1.0 / (1.0 - (p1 * b2 + p2 * a2))
    m21 = (q1 * b2 + q2 * a2) * i11
    i22 = 1.0 / ((1.0 - (q1 * b1 + q2 * a1)) - m21 * m12)
    for n, v in enumerate(known + [p1, p2, q1, q2, m12, m21, i11, i22]):
        close[n] = v

    def close_line(h):
        for cp in line_copies(xrs.at[h], xrr.at[h], xrss.at[h], xrrs.at[h]):
            cp.wait()
        first = pl.multiple_of(halves[h] * H, 8)
        known = [close[n, pl.ds(first, H), :] for n in range(5 * (row_count - 2) + 8)]

        def received(n):
            return xrr[h, n, 0:H, :], xrr[h, n, H:2 * H, :]

        p0, q0 = received(row_count - 2)
        for i, n in enumerate(slots):
            p0, q0, _, _ = join_rhs(known[5 * i:5 * i + 5], p0, q0, *received(n))
        p1, p2, q1, q2, m12, m21, i11, i22 = known[5 * (row_count - 2):]
        a0, b0 = xrs[h, 0:H, :], xrs[h, H:2 * H, :]
        s1 = (p0 + p1 * b0) + p2 * a0
        s2 = (q0 + q1 * b0) + q2 * a0
        before = i22 * (s2 + m21 * s1)
        spread(cx, first, H, before, i11 * (s1 + m12 * before), edge)

    def put_x(b, f, rows, x):
        r1[b, f, rows, :] = (x + x) - r1[b, f, rows, :]

    def turn_in(b, n):
        c, f = (n // F, n % F) if isinstance(n, int) else (lax.div(n, F), lax.rem(n, F))
        y[c, f, pl.ds(pl.multiple_of(PAD + b * 128, 8), 128), :] = r1[b, f, pl.ds(pl.multiple_of(PAD + c * 128, 8), 128), :].T

    alone, both = backward(xb, g, edge, put_x, turn_in)

    def solve(n, carry):
        @pl.when(n == 2)
        def _():
            close_line(1)

        both(block(n), block(n - 1))
        return carry

    close_line(0)
    alone(block(0))
    lax.fori_loop(1, NB, solve, 0)
    for n in range(NB * F // 2):
        turn_in(block(3), n)

    def rhs_y(b, t):
        return [y[b, f, chunk_rows(t), :] for f in range(F)]

    def turn_rest(i):
        for n in range(2):
            turn_in(block(3), NB * F // 2 + 2 * i + n)

    forward(yk, rhs_y, g, sy, [0, 1], 16, turn_rest)
    forward(yk, rhs_y, g, sy, [2, 3], 13)
    reduce_rhs(sy, cy, 0, R, yrs)
    first = col == 0
    give = pl.multiple_of(other * R, 8)
    take = pl.multiple_of(col * R, 8)
    y_rhs = to_pair(1, yrs.at[pl.ds(give, R)], yrr)

    nothing = jnp.zeros((R, 128), F32)
    spread(cy, 0, R, nothing, nothing, edge)

    def put_y(b, f, rows, x):
        y[b, f, rows, :] = x

    alone, _ = backward(yb, g, edge, put_y, None)

    def solve_y(b, carry):
        alone(b)
        return carry

    lax.fori_loop(0, NB, solve_y, 0)
    one_left = jnp.where(first, 0.0, 1.0) + nothing
    spread(cy, 0, R, one_left, 1.0 - one_left, edge, False)
    near = [beside(edge, 0, b, 0) for b in range(NB)]

    def step_h(blocks, n, state):
        rows = chunk_rows(C - 1 - n)
        out = []
        for b in blocks:
            out.append(yb[V, b, rows, :] * near[b] + yb[NC, b, rows, :] * state[b])
            answer[b, rows, :] = out[b]
        return tuple(out)

    sweep(range(NB), step_h, tuple(beside(edge, 1, b, 0) for b in range(NB)))

    y_coef.wait()
    a1, b2 = cy[7, 0], cy[7, 3]
    c1, d2 = ycr[0:R, :], ycr[3 * R:4 * R, :]
    lb2 = jnp.where(first, b2, d2)
    ra1 = jnp.where(first, c1, a1)
    inv = 1.0 / (1.0 - lb2 * ra1)
    y_rhs.wait()
    mine = yrs[pl.ds(give, R), :]
    theirs = yrr[...]
    lb0 = jnp.where(first, mine, theirs)
    ra0 = jnp.where(first, theirs, mine)
    last_left = inv * (lb0 + lb2 * ra0)
    ends[...] = jnp.where(first, ra0 + ra1 * last_left, last_left)


def last_kernel(y, h, ends, out, o, out_sem):
    def copy_out(c, b):
        return pltpu.make_async_copy(o.at[b, pl.ds(pl.multiple_of(c * 128 * F, 8), 128 * F)].reshape(128, F, 128),
                                     out.at[pl.ds(c * 128, 128), b], out_sem.at[c, b])

    def turn_out(c, carry):
        for b in range(NB):
            part = h[c, PAD + b * 128:PAD + b * 128 + 128, :]
            for f in range(F):
                end = jnp.broadcast_to(ends[pl.ds(row_of(c, f), 1), :], (128, 128))
                o[b, pl.ds(c * 128 * F + f, 128, stride=F), :] = (
                    y[c, f, PAD + b * 128:PAD + b * 128 + 128, :] + part * end).T
            copy_out(c, b).start()
        return carry

    for c in range(NB):
        turn_out(c, 0)
    for c in range(NB):
        for b in range(NB):
            copy_out(c, b).wait()


def solution(mesh):
    row_count = mesh.shape["row"]
    field_spec = P(("batch", "row"), "col", None)
    coef_spec = P(("batch", "row"), "col")

    def local_step(field, x_lower, x_diag, x_upper, y_lower, y_diag, y_upper):
        words = field.reshape(T, NB, 128, F).transpose(0, 1, 3, 2)
        plane = (NB, ROWS, 128)
        fields = (NB, F, ROWS, 128)
        peers = row_count - 1
        in_vmem = pl.BlockSpec(memory_space=pltpu.VMEM)
        in_hbm = pl.BlockSpec(memory_space=pl.ANY)
        dma = pltpu.SemaphoreType.DMA
        parts = pl.pallas_call(
            functools.partial(main_kernel, row_count),
            out_shape=[pltpu.VMEM(fields, F32), pltpu.VMEM(plane, F32), pltpu.VMEM((R, 128), F32)],
            in_specs=[in_hbm] * 7,
            out_specs=[in_vmem] * 3,
            scratch_shapes=[
                pltpu.VMEM((NB + 1, ROWS * F, 128), F32),
                pltpu.VMEM((3,) + plane, F32),
                pltpu.VMEM((2,) + plane, F32),
                pltpu.VMEM((3,) + plane, F32),
                pltpu.VMEM((3,) + plane, F32),
                pltpu.VMEM((2,) + plane, F32),
                pltpu.VMEM(fields, F32),
                pltpu.VMEM(fields, F32),
                pltpu.VMEM((2, R * 8, 128), F32),
                pltpu.VMEM((6 * R, 8, 128), F32),
                pltpu.VMEM((6 * R, 8, 128), F32),
                pltpu.VMEM((8, 11, R, 128), F32),
                pltpu.VMEM((8, 11, R, 128), F32),
                pltpu.VMEM((2, 16, 128), F32),
                pltpu.VMEM((5 * (row_count - 2) + 8, R, 128), F32),
                pltpu.VMEM((4 * R, 128), F32),
                pltpu.VMEM((peers, 4 * R, 128), F32),
                pltpu.VMEM((2, R, 128), F32),
                pltpu.VMEM((2, peers, R, 128), F32),
                pltpu.VMEM((4 * R, 128), F32),
                pltpu.VMEM((4 * R, 128), F32),
                pltpu.VMEM((2 * R, 128), F32),
                pltpu.VMEM((R, 128), F32),
                dma((3, NB)), dma((NB, NB)), dma((NB, 3)), dma, dma, dma((peers,)), dma((peers,)), dma((2, peers)), dma((2, peers)), dma((2,)), dma((2,)),
            ],
            compiler_params=pltpu.CompilerParams(
                collective_id=0, has_side_effects=True, vmem_limit_bytes=58 << 20),
        )(words, x_lower, x_diag, x_upper, y_lower, y_diag, y_upper)
        solved = pl.pallas_call(
            last_kernel,
            out_shape=jax.ShapeDtypeStruct((T, NB, F, 128), F32),
            in_specs=[in_vmem] * 3,
            out_specs=in_hbm,
            scratch_shapes=[pltpu.VMEM((NB, T * F, 128), F32), dma((NB, NB))],
            compiler_params=pltpu.CompilerParams(vmem_limit_bytes=16 << 20),
        )(*parts)
        return solved.transpose(0, 1, 3, 2).reshape(T, T, F)

    return jax.shard_map(local_step, mesh=mesh, in_specs=(field_spec,) + (coef_spec,) * 6,
                         out_specs=field_spec, check_vma=False)
```

```python
import functools

import jax
import jax.numpy as jnp
from jax import lax
from jax.experimental import pallas as pl
from jax.experimental.pallas import tpu as pltpu
from jax.sharding import PartitionSpec as P

MESH = pl.DeviceIdType.MESH
F32 = jnp.float32

T = 512
F = 4
C = 65
PAD = 8
ROWS = T + PAD
NB = T // 128
R = F * NB
UNROLL = 5

DIAG, LOW, UPP = 0, 1, 2
INV, NA, PR = 0, 1, 2
V, NC = 0, 1
A0, A1, A2, B0, B1, B2 = range(6)


H = R // 2
X_UNROLL = C


def chunk_rows(t):
    return pl.ds(t, 8, stride=C)


def row_of(b, f):
    if isinstance(b, int):
        return b // 2 * H + f * 2 + b % 2
    return lax.div(b, 2) * H + f * 2 + lax.rem(b, 2)


def beside(edge, side, b, f):
    return edge[side, pl.ds(pl.multiple_of(row_of(b, f) * 8, 8), 8), :]


def sweep(blocks, step, state, unroll=UNROLL):
    def steps(i, state):
        for n in range(unroll):
            state = step(blocks, i * unroll + n, state)
        return state
    return lax.fori_loop(0, C // unroll, steps, state)


def factor(k, kb, summ):
    sub = lax.broadcasted_iota(jnp.int32, (8, 128), 0)
    zero = jnp.zeros((8, 128), F32)

    def step(blocks, t, state):
        out = []
        fresh = sub == jnp.where(t == PAD, 0, 8)
        for b in blocks:
            nc, v, pr, a1 = state[4 * b:4 * b + 4]
            rows = chunk_rows(t)
            low = k[LOW, b, rows, :]
            den = (1.0 + k[DIAG, b, rows, :]) + low * nc
            inv = 1.0 / den
            na = -(low * inv)
            nc = -(k[UPP, b, rows, :] * inv)
            v = na * v
            pr = jnp.where(fresh, 1.0, pr)
            k[INV, b, rows, :] = inv
            k[NA, b, rows, :] = na
            k[PR, b, rows, :] = pr
            kb[NC, b, rows, :] = nc
            kb[V, b, rows, :] = v
            a1 = a1 + pr * v
            pr = pr * nc
            out += [nc, v, pr, a1]
        return tuple(out)

    state = (zero, zero + 1.0, jnp.where(sub == 0, 0.0, 1.0), zero) * NB
    state = sweep(range(NB), step, state)
    for b in range(NB):
        nc, v, pr, a1 = state[4 * b:4 * b + 4]
        for f in range(F):
            r = row_of(b, f)
            summ[A1 * R + r] = a1
            summ[A2 * R + r] = pr
            summ[B1 * R + r] = v
            summ[B2 * R + r] = nc


def of_chunk(summ, q, s, first=0, rows=R):
    return summ.reshape(6 * R * 8, 128)[pl.ds(q * R * 8 + first * 8 + s, rows, stride=8), :]


def join_coef(la1, la2, lb1, lb2, ra1, ra2, rb1, rb2):
    inv = 1.0 / (1.0 - ra1 * lb2)
    w = inv * ra1
    e1 = w * lb1
    e2 = inv * ra2
    m1 = lb1 + lb2 * e1
    m2 = lb2 * e2
    return (la1 + la2 * e1, la2 * e2, rb1 * m1, rb2 + rb1 * m2), (inv, w, lb2, la2, rb1), (e1, e2, m1, m2)


def join_rhs(part, la0, lb0, ra0, rb0):
    inv, w, lb2, la2, rb1 = part
    e0 = inv * ra0 + w * lb0
    m0 = lb0 + lb2 * e0
    return la0 + la2 * e0, rb0 + rb1 * m0, e0, m0


def reduce_coef(summ, co, send):
    def chunk(s):
        return tuple(of_chunk(summ, q, s) for q in (A1, A2, B1, B2))
    whole = chunk(0)
    for s in range(1, 8):
        whole, part, inner = join_coef(*whole, *chunk(s))
        for n, v in enumerate(part + inner):
            co[s - 1, n] = v
    for n, v in enumerate(whole):
        co[7, n] = v
        send[n * R:n * R + R, :] = v


def reduce_rhs(summ, co, first, rows, send):
    some = pl.ds(first, rows)
    a0, b0 = (of_chunk(summ, q, 0, first, rows) for q in (A0, B0))
    for s in range(1, 8):
        part = tuple(co[s - 1, n, some, :] for n in range(5))
        a0, b0, e0, m0 = join_rhs(part, a0, b0, *(of_chunk(summ, q, s, first, rows) for q in (A0, B0)))
        co[s - 1, 9, some, :] = e0
        co[s - 1, 10, some, :] = m0
    send[0:rows, :] = a0
    send[rows:2 * rows, :] = b0


def weigh(k, co, want_first, edge, weights):
    lam = (1.0 - want_first) + jnp.zeros((R, 128), F32)

    def at(s):
        return pl.ds(s, R, stride=8)

    for s in range(7, 0, -1):
        inv, w, lb2, la2, rb1 = (co[s - 1, n] for n in range(5))
        la2 = want_first * la2
        edge[1, at(s), :] = lam
        edge[0, at(s), :] = inv * (la2 + lam * (rb1 * lb2))
        lam = lam * (rb1 * (1.0 + lb2 * w)) + la2 * w
    edge[1, at(0), :] = lam
    edge[0, at(0), :] = want_first + jnp.zeros((R, 128), F32)
    parts = [(beside(edge, 0, b, 0), beside(edge, 1, b, 0)) for b in range(NB)]

    def step(blocks, n, state):
        rows = chunk_rows(C - 1 - n)
        out = []
        for b in blocks:
            first = k[PR, b, rows, :] + state[2 * b]
            last = state[2 * b + 1]
            na = k[NA, b, rows, :]
            weights[b, rows, :] = k[INV, b, rows, :] * (parts[b][0] * first + parts[b][1] * last)
            out += [na * first, na * last]
        return tuple(out)

    zero = jnp.zeros((8, 128), F32)
    sweep(range(NB), step, (zero, zero + 1.0) * NB)


def spread(co, first, rows, before, after, edge, rhs=True):
    def at(s):
        return pl.ds(first * 8 + s, rows, stride=8)
    some = pl.ds(first, rows)
    nxt = after
    edge[1, at(7), :] = after
    edge[0, at(0), :] = before
    for s in range(7, 0, -1):
        e1, e2, m1, m2, e0, m0 = (co[s - 1, n, some, :] for n in range(5, 11))
        last = m1 * before + m2 * nxt
        nxt = e1 * before + e2 * nxt
        if rhs:
            last, nxt = m0 + last, e0 + nxt
        edge[0, at(s), :] = last
        edge[1, at(s - 1), :] = nxt


def forward(k, rhs_of, g, summ, blocks, unroll=UNROLL):
    zero = jnp.zeros((8, 128), F32)

    def step(blocks, t, state):
        out = []
        rows = chunk_rows(t)
        for j, b in enumerate(blocks):
            inv = k[INV, b, rows, :]
            na = k[NA, b, rows, :]
            pr = k[PR, b, rows, :]
            rhs = rhs_of(b, t)
            for f in range(F):
                last, first = state[2 * (j * F + f):2 * (j * F + f) + 2]
                last = inv * rhs[f] + na * last
                g[b, f, rows, :] = last
                out += [last, first + pr * last]
        return tuple(out)

    state = (zero,) * (2 * F * len(blocks))
    if unroll == C:
        for t in range(C):
            state = step(blocks, t, state)
    else:
        state = sweep(blocks, step, state, unroll)
    for j, b in enumerate(blocks):
        for f in range(F):
            summ[B0 * R + row_of(b, f)] = state[2 * (j * F + f)]
            summ[A0 * R + row_of(b, f)] = state[2 * (j * F + f) + 1]


def backward(kb, g, edge, put, turn):
    def start(b):
        return tuple(beside(edge, 1, b, f) for f in range(F))

    def stepper(b):
        near = [beside(edge, 0, b, f) for f in range(F)]

        def step(_, n, state):
            out = []
            rows = chunk_rows(C - 1 - n)
            v = kb[V, b, rows, :]
            nc = kb[NC, b, rows, :]
            for f in range(F):
                x = (g[b, f, rows, :] + v * near[f]) + nc * state[f]
                put(b, f, rows, x)
                out.append(x)
            return tuple(out)
        return step

    def alone(b):
        sweep(b, stepper(b), start(b))

    def both(b, before):
        step = stepper(b)
        state = step(b, 0, start(b))
        for n in range(NB * F):
            turn(before, n)
            for m in range(4):
                state = step(b, 1 + 4 * n + m, state)

    def last(b):
        for n in range(NB * F):
            turn(b, n)

    return alone, both, last


def main_kernel(row_count, field, xl, xd, xu, yl, yd, yu, y, answer, ends,
                u, xk, xb, yn, yk, yb, r1, g, edge, sx, sy, cx, cy, pack, close, weights, dots, ends2,
                xcs, xcr, xrs, xrr, ycs, ycr, yrs, yrr,
                in_sem, field_sem, coef_sem, ps, pr, xcss, xcrs, xrss, xrrs, yss, yrsem):
    row = lax.axis_index("row")
    col = lax.axis_index("col")
    other = 1 - col
    lane = lax.broadcasted_iota(jnp.int32, (8, 128), 1)
    zero = jnp.zeros((8, 128), F32)
    src_block = (NB - 1) * other
    src_lane = 127 * other
    dst_lane = 127 * col

    def block(n):
        return n + col * (3 - 2 * n)

    def in_field(n):
        b = block(n)
        return [pltpu.make_async_copy(field.at[pl.ds(i * 128, 128), b],
                                      u.at[b, pl.ds((PAD + i * 128) * F, 128 * F)].reshape(128, F, 128), field_sem.at[n, i])
                for i in range(NB)]

    def in_coef(n):
        b = block(n)
        return [pltpu.make_async_copy(ref.at[:, pl.ds(pl.multiple_of(b * 128, 128), 128)], yn.at[i, b, pl.ds(PAD, T)], coef_sem.at[n, i])
                for i, ref in enumerate((yd, yl, yu))]

    in_x = [pltpu.make_async_copy(ref.at[:, pl.ds(b * 128, 128)], xk.at[n, b, pl.ds(PAD, T)], in_sem.at[n, b])
            for n, ref in enumerate((xd, xl, xu)) for b in range(NB)]

    def start(copies):
        for cp in copies:
            cp.start()

    def wait(copies):
        for cp in copies:
            cp.wait()

    start(in_field(3))

    barrier = pltpu.get_barrier_semaphore()
    for d in range(1, row_count):
        pl.semaphore_signal(barrier, inc=1, device_id={"row": lax.rem(row + d, row_count)}, device_id_type=MESH)
    pl.semaphore_signal(barrier, inc=1, device_id={"col": other}, device_id_type=MESH)

    for b in range(NB):
        for n in range(3):
            yn[n, b, 0:PAD, :] = zero
            xk[n, b, 0:PAD, :] = zero - 1.0 if n == LOW else zero
            yk[n, b, 0:PAD, :] = zero - 1.0 if n == LOW else zero
        for f in range(F):
            y[b, f, 0:PAD, :] = zero
    for b in range(NB):
        u[b, 0:PAD * F, :] = jnp.zeros((PAD * F, 128), F32)
    u[NB] = jnp.zeros((ROWS * F, 128), F32)

    def line_copies(send, recv, send_sem, recv_sem):
        return [pltpu.make_async_remote_copy(send, recv.at[d - 1], send_sem.at[d - 1], recv_sem.at[d - 1],
                                             device_id={"row": lax.rem(row + d, row_count)}, device_id_type=MESH)
                for d in range(1, row_count)]

    def to_line(*refs):
        copies = line_copies(*refs)
        for cp in copies:
            cp.start()
        return copies

    def to_pair(n, send, recv):
        cp = pltpu.make_async_remote_copy(send, recv, yss.at[n], yrsem.at[n], device_id={"col": other}, device_id_type=MESH)
        cp.start()
        return cp

    start(in_x)

    wait(in_field(3))
    start(in_field(0) + in_field(1) + in_coef(0))
    from_src = jnp.bitwise_and(lane - src_lane, 127)
    for h in range(2):
        acc = zero
        for p in range(128):
            w = PAD * F + 8 * (h * 128 + p)
            acc = jnp.where(from_src == p, pltpu.roll(u[src_block, w:w + 8, :], p, 1), acc)
        pack[0, h * 8:h * 8 + 8, :] = acc
    pl.semaphore_wait(barrier, row_count)
    column = pltpu.make_async_remote_copy(pack.at[0], pack.at[1], ps, pr, device_id={"col": other}, device_id_type=MESH)
    column.start()


    wait(in_x)
    start(in_field(2) + in_coef(1) + in_coef(2) + in_coef(3))
    factor(xk, xb, sx)
    reduce_coef(sx, cx, xcs)
    coef_sends = to_line(xcs, xcr, xcss, xcrs)

    def stencil(b, t):
        rows = chunk_rows(t)
        cd = 1.0 - yn[DIAG, b, rows, :]
        cl = yn[LOW, b, rows, :]
        cu = yn[UPP, b, rows, :]
        left = lax.rem(b + NB, NB + 1)
        rhs = []
        for f in range(F):
            words = pl.ds(t * F + f, 8, stride=C * F)
            mid = u[b, words, :]
            prv = pltpu.roll(jnp.where(lane == 127, u[left, words, :], mid), 1, 1)
            nxt = pltpu.roll(jnp.where(lane == 0, u[b + 1, words, :], mid), 127, 1)
            v = (cd * mid - cl * prv) - cu * nxt
            r1[b, f, rows, :] = v
            rhs.append(v)
        return rhs

    halves = [col, other]

    def send_half(h):
        reduce_rhs(sx, cx, pl.multiple_of(halves[h] * H, 8), H, xrs.at[h])
        return to_line(xrs.at[h], xrr.at[h], xrss.at[h], xrrs.at[h])

    def eliminate(n, carry):
        wait(in_coef(n))

        @pl.when(n < 2)
        def _():
            wait(in_field(n + 1))

        @pl.when(n == 2)
        def _():
            send_half(0)

        @pl.when(n == 3)
        def _():
            column.wait()
            here = lane == dst_lane
            for i in range(2):
                got = pack[1, i * 8:i * 8 + 8, :]
                for p in range(128):
                    w = PAD * F + 8 * (i * 128 + p)
                    u[NB, w:w + 8, :] = jnp.where(here, pltpu.roll(got, (128 - p) % 128, 1), 0.0)

        forward(xk, stencil, g, sx, [block(n)], X_UNROLL)
        return carry

    wait(in_field(0))
    lax.fori_loop(0, NB, eliminate, 0)
    send_half(1)

    for b in range(NB):
        for c in range(NB):
            for n in range(3):
                yk[n, c, PAD + b * 128:PAD + b * 128 + 128, :] = yn[n, b, PAD + c * 128:PAD + c * 128 + 128, :].T
    factor(yk, yb, sy)
    reduce_coef(sy, cy, ycs)
    y_coef = to_pair(0, ycs, ycr)
    weigh(yk, cy, jnp.where(col == 0, 0.0, 1.0), edge, weights)
    dots[...] = jnp.zeros((R, 8, 128), F32)

    for cp in coef_sends:
        cp.wait()

    def coef_of(ref):
        return tuple(ref[q * R:q * R + R, :] for q in range(4))

    slots = range(row_count - 3, -1, -1)
    rest = coef_of(xcr.at[row_count - 2])
    known = []
    for n in slots:
        rest, part, _ = join_coef(*rest, *coef_of(xcr.at[n]))
        known += part
    p1, p2, q1, q2 = rest
    a1, a2, b1, b2 = (cx[7, n] for n in range(4))
    m12 = p1 * b1 + p2 * a1
    i11 = 1.0 / (1.0 - (p1 * b2 + p2 * a2))
    m21 = (q1 * b2 + q2 * a2) * i11
    i22 = 1.0 / ((1.0 - (q1 * b1 + q2 * a1)) - m21 * m12)
    for n, v in enumerate(known + [p1, p2, q1, q2, m12, m21, i11, i22]):
        close[n] = v

    def close_line(h):
        for cp in line_copies(xrs.at[h], xrr.at[h], xrss.at[h], xrrs.at[h]):
            cp.wait()
        first = pl.multiple_of(halves[h] * H, 8)
        known = [close[n, pl.ds(first, H), :] for n in range(5 * (row_count - 2) + 8)]

        def received(n):
            return xrr[h, n, 0:H, :], xrr[h, n, H:2 * H, :]

        p0, q0 = received(row_count - 2)
        for i, n in enumerate(slots):
            p0, q0, _, _ = join_rhs(known[5 * i:5 * i + 5], p0, q0, *received(n))
        p1, p2, q1, q2, m12, m21, i11, i22 = known[5 * (row_count - 2):]
        a0, b0 = xrs[h, 0:H, :], xrs[h, H:2 * H, :]
        s1 = (p0 + p1 * b0) + p2 * a0
        s2 = (q0 + q1 * b0) + q2 * a0
        before = i22 * (s2 + m21 * s1)
        spread(cx, first, H, before, i11 * (s1 + m12 * before), edge)

    def put_x(b, f, rows, x):
        r1[b, f, rows, :] = (x + x) - r1[b, f, rows, :]

    def turn_in(b, n):
        c, f = n // F, n % F
        rows = pl.ds(pl.multiple_of(PAD + b * 128, 8), 128)
        square = r1[b, f, PAD + c * 128:PAD + c * 128 + 128, :].T
        y[c, f, rows, :] = square
        r = row_of(c, f)
        dots[r] = dots[r] + jnp.sum((square * weights[c, rows, :]).reshape(16, 8, 128), axis=0)

    alone, both, last = backward(xb, g, edge, put_x, turn_in)

    def solve(n, carry):
        @pl.when(n == 2)
        def _():
            close_line(1)

        both(block(n), block(n - 1))
        return carry

    close_line(0)
    alone(block(0))
    lax.fori_loop(1, NB, solve, 0)
    last(block(3))

    flat = dots.reshape(R * 8, 128)
    mine = flat[pl.ds(0, R, stride=8), :]
    for i in range(1, 8):
        mine = mine + flat[pl.ds(i, R, stride=8), :]
    yrs[...] = mine
    y_rhs = to_pair(1, yrs, yrr)

    def rhs_y(b, t):
        return [y[b, f, chunk_rows(t), :] for f in range(F)]

    forward(yk, rhs_y, g, sy, [0, 1])
    forward(yk, rhs_y, g, sy, [2, 3])
    reduce_rhs(sy, cy, 0, R, ends2)
    first = col == 0

    nothing = jnp.zeros((R, 128), F32)
    spread(cy, 0, R, nothing, nothing, edge)

    def put_y(b, f, rows, x):
        y[b, f, rows, :] = x

    alone, _, _ = backward(yb, g, edge, put_y, None)

    def solve_y(b, carry):
        alone(b)
        return carry

    lax.fori_loop(0, NB, solve_y, 0)
    one_left = jnp.where(first, 0.0, 1.0) + nothing
    spread(cy, 0, R, one_left, 1.0 - one_left, edge, False)
    near = [beside(edge, 0, b, 0) for b in range(NB)]

    def step_h(blocks, n, state):
        rows = chunk_rows(C - 1 - n)
        out = []
        for b in blocks:
            out.append(yb[V, b, rows, :] * near[b] + yb[NC, b, rows, :] * state[b])
            answer[b, rows, :] = out[b]
        return tuple(out)

    sweep(range(NB), step_h, tuple(beside(edge, 1, b, 0) for b in range(NB)))

    y_coef.wait()
    a1, b2 = cy[7, 0], cy[7, 3]
    c1, d2 = ycr[0:R, :], ycr[3 * R:4 * R, :]
    lb2 = jnp.where(first, b2, d2)
    ra1 = jnp.where(first, c1, a1)
    inv = 1.0 / (1.0 - lb2 * ra1)
    y_rhs.wait()
    mine = yrs[...]
    theirs = yrr[...]
    lb0 = jnp.where(first, mine, theirs)
    ra0 = jnp.where(first, theirs, mine)
    last_left = inv * (lb0 + lb2 * ra0)
    ends[...] = jnp.where(first, ra0 + ra1 * last_left, last_left)


def last_kernel(y, h, ends, out, o, out_sem):
    def copy_out(c, b):
        return pltpu.make_async_copy(o.at[b, pl.ds(pl.multiple_of(c * 128 * F, 8), 128 * F)].reshape(128, F, 128),
                                     out.at[pl.ds(c * 128, 128), b], out_sem.at[c, b])

    def turn_out(c, carry):
        for b in range(NB):
            part = h[c, PAD + b * 128:PAD + b * 128 + 128, :]
            for f in range(F):
                end = jnp.broadcast_to(ends[pl.ds(row_of(c, f), 1), :], (128, 128))
                o[b, pl.ds(c * 128 * F + f, 128, stride=F), :] = (
                    y[c, f, PAD + b * 128:PAD + b * 128 + 128, :] + part * end).T
            copy_out(c, b).start()
        return carry

    lax.fori_loop(0, NB, turn_out, 0)
    for c in range(NB):
        for b in range(NB):
            copy_out(c, b).wait()


def solution(mesh):
    row_count = mesh.shape["row"]
    field_spec = P(("batch", "row"), "col", None)
    coef_spec = P(("batch", "row"), "col")

    def local_step(field, x_lower, x_diag, x_upper, y_lower, y_diag, y_upper):
        words = field.reshape(T, NB, 128, F).transpose(0, 1, 3, 2)
        plane = (NB, ROWS, 128)
        fields = (NB, F, ROWS, 128)
        peers = row_count - 1
        in_vmem = pl.BlockSpec(memory_space=pltpu.VMEM)
        in_hbm = pl.BlockSpec(memory_space=pl.ANY)
        dma = pltpu.SemaphoreType.DMA
        parts = pl.pallas_call(
            functools.partial(main_kernel, row_count),
            out_shape=[pltpu.VMEM(fields, F32), pltpu.VMEM(plane, F32), pltpu.VMEM((R, 128), F32)],
            in_specs=[in_hbm] * 7,
            out_specs=[in_vmem] * 3,
            scratch_shapes=[
                pltpu.VMEM((NB + 1, ROWS * F, 128), F32),
                pltpu.VMEM((3,) + plane, F32),
                pltpu.VMEM((2,) + plane, F32),
                pltpu.VMEM((3,) + plane, F32),
                pltpu.VMEM((3,) + plane, F32),
                pltpu.VMEM((2,) + plane, F32),
                pltpu.VMEM(fields, F32),
                pltpu.VMEM(fields, F32),
                pltpu.VMEM((2, R * 8, 128), F32),
                pltpu.VMEM((6 * R, 8, 128), F32),
                pltpu.VMEM((6 * R, 8, 128), F32),
                pltpu.VMEM((8, 11, R, 128), F32),
                pltpu.VMEM((8, 11, R, 128), F32),
                pltpu.VMEM((2, 16, 128), F32),
                pltpu.VMEM((5 * (row_count - 2) + 8, R, 128), F32),
                pltpu.VMEM(plane, F32),
                pltpu.VMEM((R, 8, 128), F32),
                pltpu.VMEM((2 * R, 128), F32),
                pltpu.VMEM((4 * R, 128), F32),
                pltpu.VMEM((peers, 4 * R, 128), F32),
                pltpu.VMEM((2, R, 128), F32),
                pltpu.VMEM((2, peers, R, 128), F32),
                pltpu.VMEM((4 * R, 128), F32),
                pltpu.VMEM((4 * R, 128), F32),
                pltpu.VMEM((R, 128), F32),
                pltpu.VMEM((R, 128), F32),
                dma((3, NB)), dma((NB, NB)), dma((NB, 3)), dma, dma, dma((peers,)), dma((peers,)), dma((2, peers)), dma((2, peers)), dma((2,)), dma((2,)),
            ],
            compiler_params=pltpu.CompilerParams(
                collective_id=0, has_side_effects=True, vmem_limit_bytes=58 << 20),
        )(words, x_lower, x_diag, x_upper, y_lower, y_diag, y_upper)
        solved = pl.pallas_call(
            last_kernel,
            out_shape=jax.ShapeDtypeStruct((T, NB, F, 128), F32),
            in_specs=[in_vmem] * 3,
            out_specs=in_hbm,
            scratch_shapes=[pltpu.VMEM((NB, T * F, 128), F32), dma((NB, NB))],
            compiler_params=pltpu.CompilerParams(vmem_limit_bytes=16 << 20),
        )(*parts)
        return solved.transpose(0, 1, 3, 2).reshape(T, T, F)

    return jax.shard_map(local_step, mesh=mesh, in_specs=(field_spec,) + (coef_spec,) * 6,
                         out_specs=field_spec, check_vma=False)
```

```python
import functools

import jax
import jax.numpy as jnp
from jax import lax
from jax.experimental import pallas as pl
from jax.experimental.pallas import tpu as pltpu
from jax.sharding import PartitionSpec as P

MESH = pl.DeviceIdType.MESH
F32 = jnp.float32

T = 512
F = 4
C = 65
PAD = 8
ROWS = T + PAD
NB = T // 128
R = F * NB
UNROLL = 5

DIAG, LOW, UPP = 0, 1, 2
INV, NA, PR = 0, 1, 2
V, NC = 0, 1
A0, A1, A2, B0, B1, B2 = range(6)


H = R // 2
X_UNROLL = C


def chunk_rows(t):
    return pl.ds(t, 8, stride=C)


def row_of(b, f):
    if isinstance(b, int):
        return b // 2 * H + f * 2 + b % 2
    return lax.div(b, 2) * H + f * 2 + lax.rem(b, 2)


def beside(edge, side, b, f):
    return edge[side, pl.ds(pl.multiple_of(row_of(b, f) * 8, 8), 8), :]


def sweep(blocks, step, state, unroll=UNROLL):
    def steps(i, state):
        for n in range(unroll):
            state = step(blocks, i * unroll + n, state)
        return state
    return lax.fori_loop(0, C // unroll, steps, state)


def factor(k, kb, summ, scale):
    sub = lax.broadcasted_iota(jnp.int32, (8, 128), 0)
    zero = jnp.zeros((8, 128), F32)

    def step(blocks, t, state):
        out = []
        fresh = sub == jnp.where(t == PAD, 0, 8)
        for b in blocks:
            nc, v, pr, a1 = state[4 * b:4 * b + 4]
            rows = chunk_rows(t)
            low = k[LOW, b, rows, :]
            den = (1.0 + k[DIAG, b, rows, :]) + low * nc
            inv = 1.0 / den
            na = -(low * inv)
            nc = -(k[UPP, b, rows, :] * inv)
            v = na * v
            pr = jnp.where(fresh, 1.0, pr)
            k[INV, b, rows, :] = inv if scale == 1 else inv * scale
            k[NA, b, rows, :] = na
            k[PR, b, rows, :] = pr
            kb[NC, b, rows, :] = nc
            kb[V, b, rows, :] = v
            a1 = a1 + pr * v
            pr = pr * nc
            out += [nc, v, pr, a1]
        return tuple(out)

    state = (zero, zero + 1.0, jnp.where(sub == 0, 0.0, 1.0), zero) * NB
    state = sweep(range(NB), step, state)
    for b in range(NB):
        nc, v, pr, a1 = state[4 * b:4 * b + 4]
        for f in range(F):
            r = row_of(b, f)
            summ[A1 * R + r] = a1
            summ[A2 * R + r] = pr
            summ[B1 * R + r] = v
            summ[B2 * R + r] = nc


def of_chunk(summ, q, s, first=0, rows=R):
    return summ.reshape(6 * R * 8, 128)[pl.ds(q * R * 8 + first * 8 + s, rows, stride=8), :]


def join_coef(la1, la2, lb1, lb2, ra1, ra2, rb1, rb2):
    inv = 1.0 / (1.0 - ra1 * lb2)
    w = inv * ra1
    e1 = w * lb1
    e2 = inv * ra2
    m1 = lb1 + lb2 * e1
    m2 = lb2 * e2
    return (la1 + la2 * e1, la2 * e2, rb1 * m1, rb2 + rb1 * m2), (inv, w, lb2, la2, rb1), (e1, e2, m1, m2)


def join_rhs(part, la0, lb0, ra0, rb0):
    inv, w, lb2, la2, rb1 = part
    e0 = inv * ra0 + w * lb0
    m0 = lb0 + lb2 * e0
    return la0 + la2 * e0, rb0 + rb1 * m0, e0, m0


def reduce_coef(summ, co, send):
    def chunk(s):
        return tuple(of_chunk(summ, q, s) for q in (A1, A2, B1, B2))
    whole = chunk(0)
    for s in range(1, 8):
        whole, part, inner = join_coef(*whole, *chunk(s))
        for n, v in enumerate(part + inner):
            co[s - 1, n] = v
    for n, v in enumerate(whole):
        co[7, n] = v
        send[n * R:n * R + R, :] = v


def reduce_rhs(summ, co, first, rows, send):
    some = pl.ds(first, rows)
    a0, b0 = (of_chunk(summ, q, 0, first, rows) for q in (A0, B0))
    for s in range(1, 8):
        part = tuple(co[s - 1, n, some, :] for n in range(5))
        a0, b0, e0, m0 = join_rhs(part, a0, b0, *(of_chunk(summ, q, s, first, rows) for q in (A0, B0)))
        co[s - 1, 9, some, :] = e0
        co[s - 1, 10, some, :] = m0
    send[0:rows, :] = a0
    send[rows:2 * rows, :] = b0


def weigh(k, co, want_first, edge, weights):
    lam = (1.0 - want_first) + jnp.zeros((R, 128), F32)

    def at(s):
        return pl.ds(s, R, stride=8)

    for s in range(7, 0, -1):
        inv, w, lb2, la2, rb1 = (co[s - 1, n] for n in range(5))
        la2 = want_first * la2
        edge[1, at(s), :] = lam
        edge[0, at(s), :] = inv * (la2 + lam * (rb1 * lb2))
        lam = lam * (rb1 * (1.0 + lb2 * w)) + la2 * w
    edge[1, at(0), :] = lam
    edge[0, at(0), :] = want_first + jnp.zeros((R, 128), F32)
    parts = [(beside(edge, 0, b, 0), beside(edge, 1, b, 0)) for b in range(NB)]

    def step(blocks, n, state):
        rows = chunk_rows(C - 1 - n)
        out = []
        for b in blocks:
            first = k[PR, b, rows, :] + state[2 * b]
            last = state[2 * b + 1]
            na = k[NA, b, rows, :]
            weights[b, rows, :] = k[INV, b, rows, :] * (parts[b][0] * first + parts[b][1] * last)
            out += [na * first, na * last]
        return tuple(out)

    zero = jnp.zeros((8, 128), F32)
    sweep(range(NB), step, (zero, zero + 1.0) * NB)


def spread(co, first, rows, before, after, edge, rhs=True):
    def at(s):
        return pl.ds(first * 8 + s, rows, stride=8)
    some = pl.ds(first, rows)
    nxt = after
    edge[1, at(7), :] = after
    edge[0, at(0), :] = before
    for s in range(7, 0, -1):
        e1, e2, m1, m2, e0, m0 = (co[s - 1, n, some, :] for n in range(5, 11))
        last = m1 * before + m2 * nxt
        nxt = e1 * before + e2 * nxt
        if rhs:
            last, nxt = m0 + last, e0 + nxt
        edge[0, at(s), :] = last
        edge[1, at(s - 1), :] = nxt


def forward(k, rhs_of, g, summ, blocks, unroll=UNROLL):
    zero = jnp.zeros((8, 128), F32)

    def step(blocks, t, state):
        out = []
        rows = chunk_rows(t)
        for j, b in enumerate(blocks):
            inv = k[INV, b, rows, :]
            na = k[NA, b, rows, :]
            pr = k[PR, b, rows, :]
            rhs = rhs_of(b, t)
            for f in range(F):
                last, first = state[2 * (j * F + f):2 * (j * F + f) + 2]
                last = inv * rhs[f] + na * last
                g[b, f, rows, :] = last
                out += [last, first + pr * last]
        return tuple(out)

    state = (zero,) * (2 * F * len(blocks))
    if unroll == C:
        for t in range(C):
            state = step(blocks, t, state)
    else:
        state = sweep(blocks, step, state, unroll)
    for j, b in enumerate(blocks):
        for f in range(F):
            summ[B0 * R + row_of(b, f)] = state[2 * (j * F + f)]
            summ[A0 * R + row_of(b, f)] = state[2 * (j * F + f) + 1]


def backward(kb, g, edge, put, turn):
    def start(b):
        return tuple(beside(edge, 1, b, f) for f in range(F))

    def stepper(b):
        near = [beside(edge, 0, b, f) for f in range(F)]

        def step(_, n, state):
            out = []
            rows = chunk_rows(C - 1 - n)
            v = kb[V, b, rows, :]
            nc = kb[NC, b, rows, :]
            for f in range(F):
                x = (g[b, f, rows, :] + v * near[f]) + nc * state[f]
                put(b, f, rows, x)
                out.append(x)
            return tuple(out)
        return step

    def alone(b):
        sweep(b, stepper(b), start(b))

    def both(b, before):
        step = stepper(b)
        state = step(b, 0, start(b))
        for n in range(NB * F):
            for m in range(4):
                state = step(b, 1 + 4 * n + m, state)
            turn(before, n)

    def last(b):
        for n in range(NB * F):
            turn(b, n)

    return alone, both, last


def main_kernel(row_count, field, xl, xd, xu, yl, yd, yu, y, answer, ends,
                u, xk, xb, yn, yk, yb, r1, g, edge, sx, sy, cx, cy, pack, close, weights, dots, ends2,
                xcs, xcr, xrs, xrr, ycs, ycr, yrs, yrr,
                in_sem, field_sem, coef_sem, ps, pr, xcss, xcrs, xrss, xrrs, yss, yrsem):
    row = lax.axis_index("row")
    col = lax.axis_index("col")
    other = 1 - col
    lane = lax.broadcasted_iota(jnp.int32, (8, 128), 1)
    zero = jnp.zeros((8, 128), F32)
    src_block = (NB - 1) * other
    src_lane = 127 * other
    dst_lane = 127 * col

    def block(n):
        return n + col * (3 - 2 * n)

    def in_field(n):
        b = block(n)
        return [pltpu.make_async_copy(field.at[pl.ds(i * 128, 128), b],
                                      u.at[b, pl.ds((PAD + i * 128) * F, 128 * F)].reshape(128, F, 128), field_sem.at[n, i])
                for i in range(NB)]

    def in_coef(n):
        b = block(n)
        return [pltpu.make_async_copy(ref.at[:, pl.ds(pl.multiple_of(b * 128, 128), 128)], yn.at[i, b, pl.ds(PAD, T)], coef_sem.at[n, i])
                for i, ref in enumerate((yd, yl, yu))]

    in_x = [pltpu.make_async_copy(ref.at[:, pl.ds(b * 128, 128)], xk.at[n, b, pl.ds(PAD, T)], in_sem.at[n, b])
            for n, ref in enumerate((xd, xl, xu)) for b in range(NB)]

    def start(copies):
        for cp in copies:
            cp.start()

    def wait(copies):
        for cp in copies:
            cp.wait()

    start(in_field(3))

    barrier = pltpu.get_barrier_semaphore()
    for d in range(1, row_count):
        pl.semaphore_signal(barrier, inc=1, device_id={"row": lax.rem(row + d, row_count)}, device_id_type=MESH)
    pl.semaphore_signal(barrier, inc=1, device_id={"col": other}, device_id_type=MESH)

    for b in range(NB):
        for n in range(3):
            yn[n, b, 0:PAD, :] = zero
            xk[n, b, 0:PAD, :] = zero - 1.0 if n == LOW else zero
            yk[n, b, 0:PAD, :] = zero - 1.0 if n == LOW else zero
        for f in range(F):
            y[b, f, 0:PAD, :] = zero
    for b in range(NB):
        u[b, 0:PAD * F, :] = jnp.zeros((PAD * F, 128), F32)
    u[NB] = jnp.zeros((ROWS * F, 128), F32)

    def line_copies(send, recv, send_sem, recv_sem):
        return [pltpu.make_async_remote_copy(send, recv.at[d - 1], send_sem.at[d - 1], recv_sem.at[d - 1],
                                             device_id={"row": lax.rem(row + d, row_count)}, device_id_type=MESH)
                for d in range(1, row_count)]

    def to_line(*refs):
        copies = line_copies(*refs)
        for cp in copies:
            cp.start()
        return copies

    def to_pair(n, send, recv):
        cp = pltpu.make_async_remote_copy(send, recv, yss.at[n], yrsem.at[n], device_id={"col": other}, device_id_type=MESH)
        cp.start()
        return cp

    start(in_x)

    wait(in_field(3))
    from_src = jnp.bitwise_and(lane - src_lane, 127)
    for h in range(2):
        acc = zero
        for p in range(128):
            w = PAD * F + 8 * (h * 128 + p)
            acc = jnp.where(from_src == p, pltpu.roll(u[src_block, w:w + 8, :], p, 1), acc)
        pack[0, h * 8:h * 8 + 8, :] = acc
    start(in_field(0) + in_field(1) + in_coef(0))
    pl.semaphore_wait(barrier, row_count)
    column = pltpu.make_async_remote_copy(pack.at[0], pack.at[1], ps, pr, device_id={"col": other}, device_id_type=MESH)
    column.start()


    wait(in_x)
    start(in_field(2) + in_coef(1) + in_coef(2) + in_coef(3))
    factor(xk, xb, sx, 2.0)
    reduce_coef(sx, cx, xcs)
    coef_sends = to_line(xcs, xcr, xcss, xcrs)

    def stencil(b, t):
        rows = chunk_rows(t)
        cd = 1.0 - yn[DIAG, b, rows, :]
        cl = yn[LOW, b, rows, :]
        cu = yn[UPP, b, rows, :]
        left = lax.rem(b + NB, NB + 1)
        rhs = []
        for f in range(F):
            words = pl.ds(t * F + f, 8, stride=C * F)
            mid = u[b, words, :]
            prv = pltpu.roll(jnp.where(lane == 127, u[left, words, :], mid), 1, 1)
            nxt = pltpu.roll(jnp.where(lane == 0, u[b + 1, words, :], mid), 127, 1)
            v = (cd * mid - cl * prv) - cu * nxt
            r1[b, f, rows, :] = v
            rhs.append(v)
        return rhs

    halves = [col, other]

    def send_half(h):
        reduce_rhs(sx, cx, pl.multiple_of(halves[h] * H, 8), H, xrs.at[h])
        return to_line(xrs.at[h], xrr.at[h], xrss.at[h], xrrs.at[h])

    def eliminate(n, carry):
        wait(in_coef(n))

        @pl.when(n < 2)
        def _():
            wait(in_field(n + 1))

        @pl.when(n == 2)
        def _():
            send_half(0)

        @pl.when(n == 3)
        def _():
            column.wait()
            here = lane == dst_lane
            for i in range(2):
                got = pack[1, i * 8:i * 8 + 8, :]
                for p in range(128):
                    w = PAD * F + 8 * (i * 128 + p)
                    u[NB, w:w + 8, :] = jnp.where(here, pltpu.roll(got, (128 - p) % 128, 1), 0.0)

        forward(xk, stencil, g, sx, [block(n)], X_UNROLL)
        return carry

    wait(in_field(0))
    lax.fori_loop(0, NB, eliminate, 0)
    send_half(1)

    for b in range(NB):
        for c in range(NB):
            for n in range(3):
                yk[n, c, PAD + b * 128:PAD + b * 128 + 128, :] = yn[n, b, PAD + c * 128:PAD + c * 128 + 128, :].T
    factor(yk, yb, sy, 1)
    reduce_coef(sy, cy, ycs)
    y_coef = to_pair(0, ycs, ycr)
    weigh(yk, cy, jnp.where(col == 0, 0.0, 1.0), edge, weights)
    dots[...] = jnp.zeros((R, 8, 128), F32)

    for cp in coef_sends:
        cp.wait()

    def coef_of(ref):
        return tuple(ref[q * R:q * R + R, :] for q in range(4))

    slots = range(row_count - 3, -1, -1)
    rest = coef_of(xcr.at[row_count - 2])
    known = []
    for n in slots:
        rest, part, _ = join_coef(*rest, *coef_of(xcr.at[n]))
        known += part
    p1, p2, q1, q2 = rest
    a1, a2, b1, b2 = (cx[7, n] for n in range(4))
    m12 = p1 * b1 + p2 * a1
    i11 = 1.0 / (1.0 - (p1 * b2 + p2 * a2))
    m21 = (q1 * b2 + q2 * a2) * i11
    i22 = 1.0 / ((1.0 - (q1 * b1 + q2 * a1)) - m21 * m12)
    for n, v in enumerate(known + [p1, p2, q1, q2, m12, m21, i11, i22]):
        close[n] = v

    def close_line(h):
        for cp in line_copies(xrs.at[h], xrr.at[h], xrss.at[h], xrrs.at[h]):
            cp.wait()
        first = pl.multiple_of(halves[h] * H, 8)
        known = [close[n, pl.ds(first, H), :] for n in range(5 * (row_count - 2) + 8)]

        def received(n):
            return xrr[h, n, 0:H, :], xrr[h, n, H:2 * H, :]

        p0, q0 = received(row_count - 2)
        for i, n in enumerate(slots):
            p0, q0, _, _ = join_rhs(known[5 * i:5 * i + 5], p0, q0, *received(n))
        p1, p2, q1, q2, m12, m21, i11, i22 = known[5 * (row_count - 2):]
        a0, b0 = xrs[h, 0:H, :], xrs[h, H:2 * H, :]
        s1 = (p0 + p1 * b0) + p2 * a0
        s2 = (q0 + q1 * b0) + q2 * a0
        before = i22 * (s2 + m21 * s1)
        spread(cx, first, H, before, i11 * (s1 + m12 * before), edge)

    def put_x(b, f, rows, x):
        r1[b, f, rows, :] = x - r1[b, f, rows, :]

    def turn_in(b, n):
        c, f = n // F, n % F
        rows = pl.ds(pl.multiple_of(PAD + b * 128, 8), 128)
        square = r1[b, f, PAD + c * 128:PAD + c * 128 + 128, :].T
        y[c, f, rows, :] = square
        r = row_of(c, f)
        dots[r] = dots[r] + jnp.sum((square * weights[c, rows, :]).reshape(16, 8, 128), axis=0)

    alone, both, last = backward(xb, g, edge, put_x, turn_in)

    def solve(n, carry):
        @pl.when(n == 2)
        def _():
            close_line(1)

        both(block(n), block(n - 1))
        return carry

    close_line(0)
    alone(block(0))
    lax.fori_loop(1, NB, solve, 0)
    last(block(3))

    flat = dots.reshape(R * 8, 128)
    mine = flat[pl.ds(0, R, stride=8), :]
    for i in range(1, 8):
        mine = mine + flat[pl.ds(i, R, stride=8), :]
    yrs[...] = mine
    y_rhs = to_pair(1, yrs, yrr)

    def rhs_y(b, t):
        return [y[b, f, chunk_rows(t), :] for f in range(F)]

    forward(yk, rhs_y, g, sy, [0, 1])
    forward(yk, rhs_y, g, sy, [2, 3])
    reduce_rhs(sy, cy, 0, R, ends2)
    first = col == 0

    nothing = jnp.zeros((R, 128), F32)
    spread(cy, 0, R, nothing, nothing, edge)

    def put_y(b, f, rows, x):
        y[b, f, rows, :] = x

    alone, _, _ = backward(yb, g, edge, put_y, None)

    def solve_y(b, carry):
        alone(b)
        return carry

    lax.fori_loop(0, NB, solve_y, 0)
    one_left = jnp.where(first, 0.0, 1.0) + nothing
    spread(cy, 0, R, one_left, 1.0 - one_left, edge, False)
    near = [beside(edge, 0, b, 0) for b in range(NB)]

    def step_h(blocks, n, state):
        rows = chunk_rows(C - 1 - n)
        out = []
        for b in blocks:
            out.append(yb[V, b, rows, :] * near[b] + yb[NC, b, rows, :] * state[b])
            answer[b, rows, :] = out[b]
        return tuple(out)

    sweep(range(NB), step_h, tuple(beside(edge, 1, b, 0) for b in range(NB)))

    y_coef.wait()
    a1, b2 = cy[7, 0], cy[7, 3]
    c1, d2 = ycr[0:R, :], ycr[3 * R:4 * R, :]
    lb2 = jnp.where(first, b2, d2)
    ra1 = jnp.where(first, c1, a1)
    inv = 1.0 / (1.0 - lb2 * ra1)
    y_rhs.wait()
    mine = yrs[...]
    theirs = yrr[...]
    lb0 = jnp.where(first, mine, theirs)
    ra0 = jnp.where(first, theirs, mine)
    last_left = inv * (lb0 + lb2 * ra0)
    ends[...] = jnp.where(first, ra0 + ra1 * last_left, last_left)


def last_kernel(y, h, ends, out, o, out_sem):
    def copy_out(c, b):
        return pltpu.make_async_copy(o.at[b, pl.ds(pl.multiple_of(c * 128 * F, 8), 128 * F)].reshape(128, F, 128),
                                     out.at[pl.ds(c * 128, 128), b], out_sem.at[c, b])

    def turn_out(c, carry):
        for b in range(NB):
            part = h[c, PAD + b * 128:PAD + b * 128 + 128, :]
            for f in range(F):
                end = jnp.broadcast_to(ends[pl.ds(row_of(c, f), 1), :], (128, 128))
                o[b, pl.ds(c * 128 * F + f, 128, stride=F), :] = (
                    y[c, f, PAD + b * 128:PAD + b * 128 + 128, :] + part * end).T
            copy_out(c, b).start()
        return carry

    lax.fori_loop(0, NB, turn_out, 0)
    for c in range(NB):
        for b in range(NB):
            copy_out(c, b).wait()


def solution(mesh):
    row_count = mesh.shape["row"]
    field_spec = P(("batch", "row"), "col", None)
    coef_spec = P(("batch", "row"), "col")

    def local_step(field, x_lower, x_diag, x_upper, y_lower, y_diag, y_upper):
        words = field.reshape(T, NB, 128, F).transpose(0, 1, 3, 2)
        plane = (NB, ROWS, 128)
        fields = (NB, F, ROWS, 128)
        peers = row_count - 1
        in_vmem = pl.BlockSpec(memory_space=pltpu.VMEM)
        in_hbm = pl.BlockSpec(memory_space=pl.ANY)
        dma = pltpu.SemaphoreType.DMA
        parts = pl.pallas_call(
            functools.partial(main_kernel, row_count),
            out_shape=[pltpu.VMEM(fields, F32), pltpu.VMEM(plane, F32), pltpu.VMEM((R, 128), F32)],
            in_specs=[in_hbm] * 7,
            out_specs=[in_vmem] * 3,
            scratch_shapes=[
                pltpu.VMEM((NB + 1, ROWS * F, 128), F32),
                pltpu.VMEM((3,) + plane, F32),
                pltpu.VMEM((2,) + plane, F32),
                pltpu.VMEM((3,) + plane, F32),
                pltpu.VMEM((3,) + plane, F32),
                pltpu.VMEM((2,) + plane, F32),
                pltpu.VMEM(fields, F32),
                pltpu.VMEM(fields, F32),
                pltpu.VMEM((2, R * 8, 128), F32),
                pltpu.VMEM((6 * R, 8, 128), F32),
                pltpu.VMEM((6 * R, 8, 128), F32),
                pltpu.VMEM((8, 11, R, 128), F32),
                pltpu.VMEM((8, 11, R, 128), F32),
                pltpu.VMEM((2, 16, 128), F32),
                pltpu.VMEM((5 * (row_count - 2) + 8, R, 128), F32),
                pltpu.VMEM(plane, F32),
                pltpu.VMEM((R, 8, 128), F32),
                pltpu.VMEM((2 * R, 128), F32),
                pltpu.VMEM((4 * R, 128), F32),
                pltpu.VMEM((peers, 4 * R, 128), F32),
                pltpu.VMEM((2, R, 128), F32),
                pltpu.VMEM((2, peers, R, 128), F32),
                pltpu.VMEM((4 * R, 128), F32),
                pltpu.VMEM((4 * R, 128), F32),
                pltpu.VMEM((R, 128), F32),
                pltpu.VMEM((R, 128), F32),
                dma((3, NB)), dma((NB, NB)), dma((NB, 3)), dma, dma, dma((peers,)), dma((peers,)), dma((2, peers)), dma((2, peers)), dma((2,)), dma((2,)),
            ],
            compiler_params=pltpu.CompilerParams(
                collective_id=0, has_side_effects=True, vmem_limit_bytes=58 << 20),
        )(words, x_lower, x_diag, x_upper, y_lower, y_diag, y_upper)
        solved = pl.pallas_call(
            last_kernel,
            out_shape=jax.ShapeDtypeStruct((T, NB, F, 128), F32),
            in_specs=[in_vmem] * 3,
            out_specs=in_hbm,
            scratch_shapes=[pltpu.VMEM((NB, T * F, 128), F32), dma((NB, NB))],
            compiler_params=pltpu.CompilerParams(vmem_limit_bytes=16 << 20),
        )(*parts)
        return solved.transpose(0, 1, 3, 2).reshape(T, T, F)

    return jax.shard_map(local_step, mesh=mesh, in_specs=(field_spec,) + (coef_spec,) * 6,
                         out_specs=field_spec, check_vma=False)
```

```python
import functools

import jax
import jax.numpy as jnp
from jax import lax
from jax.experimental import pallas as pl
from jax.experimental.pallas import tpu as pltpu
from jax.sharding import PartitionSpec as P

MESH = pl.DeviceIdType.MESH
F32 = jnp.float32

T = 512
F = 4
C = 65
PAD = 8
ROWS = T + PAD
NB = T // 128
R = F * NB
UNROLL = 5

DIAG, LOW, UPP = 0, 1, 2
INV, NA, PR = 0, 1, 2
V, NC = 0, 1
A0, A1, A2, B0, B1, B2 = range(6)


H = R // 2
X_UNROLL = C


def chunk_rows(t):
    return pl.ds(t, 8, stride=C)


def row_of(b, f):
    if isinstance(b, int):
        return b // 2 * H + f * 2 + b % 2
    return lax.div(b, 2) * H + f * 2 + lax.rem(b, 2)


def beside(edge, side, b, f):
    return edge[side, pl.ds(pl.multiple_of(row_of(b, f) * 8, 8), 8), :]


def sweep(blocks, step, state, unroll=UNROLL):
    def steps(i, state):
        for n in range(unroll):
            state = step(blocks, i * unroll + n, state)
        return state
    return lax.fori_loop(0, C // unroll, steps, state)


def factor(k, kb, summ, scale):
    sub = lax.broadcasted_iota(jnp.int32, (8, 128), 0)
    zero = jnp.zeros((8, 128), F32)

    def step(blocks, t, state):
        out = []
        fresh = sub == jnp.where(t == PAD, 0, 8)
        for b in blocks:
            nc, v, pr, a1 = state[4 * b:4 * b + 4]
            rows = chunk_rows(t)
            low = k[LOW, b, rows, :]
            den = (1.0 + k[DIAG, b, rows, :]) + low * nc
            inv = 1.0 / den
            na = -(low * inv)
            nc = -(k[UPP, b, rows, :] * inv)
            v = na * v
            pr = jnp.where(fresh, 1.0, pr)
            k[INV, b, rows, :] = inv if scale == 1 else inv * scale
            k[NA, b, rows, :] = na
            k[PR, b, rows, :] = pr
            kb[NC, b, rows, :] = nc
            kb[V, b, rows, :] = v
            a1 = a1 + pr * v
            pr = pr * nc
            out += [nc, v, pr, a1]
        return tuple(out)

    state = (zero, zero + 1.0, jnp.where(sub == 0, 0.0, 1.0), zero) * NB
    state = sweep(range(NB), step, state)
    for b in range(NB):
        nc, v, pr, a1 = state[4 * b:4 * b + 4]
        for f in range(F):
            r = row_of(b, f)
            summ[A1 * R + r] = a1
            summ[A2 * R + r] = pr
            summ[B1 * R + r] = v
            summ[B2 * R + r] = nc


def of_chunk(summ, q, s, first=0, rows=R):
    return summ.reshape(6 * R * 8, 128)[pl.ds(q * R * 8 + first * 8 + s, rows, stride=8), :]


def join_coef(la1, la2, lb1, lb2, ra1, ra2, rb1, rb2):
    inv = 1.0 / (1.0 - ra1 * lb2)
    w = inv * ra1
    e1 = w * lb1
    e2 = inv * ra2
    m1 = lb1 + lb2 * e1
    m2 = lb2 * e2
    return (la1 + la2 * e1, la2 * e2, rb1 * m1, rb2 + rb1 * m2), (inv, w, lb2, la2, rb1), (e1, e2, m1, m2)


def join_rhs(part, la0, lb0, ra0, rb0):
    inv, w, lb2, la2, rb1 = part
    e0 = inv * ra0 + w * lb0
    m0 = lb0 + lb2 * e0
    return la0 + la2 * e0, rb0 + rb1 * m0, e0, m0


def reduce_coef(summ, co, send):
    def chunk(s):
        return tuple(of_chunk(summ, q, s) for q in (A1, A2, B1, B2))
    whole = chunk(0)
    for s in range(1, 8):
        whole, part, inner = join_coef(*whole, *chunk(s))
        for n, v in enumerate(part + inner):
            co[s - 1, n] = v
    for n, v in enumerate(whole):
        co[7, n] = v
        send[n * R:n * R + R, :] = v


def reduce_rhs(summ, co, first, rows, send):
    some = pl.ds(first, rows)
    a0, b0 = (of_chunk(summ, q, 0, first, rows) for q in (A0, B0))
    for s in range(1, 8):
        part = tuple(co[s - 1, n, some, :] for n in range(5))
        a0, b0, e0, m0 = join_rhs(part, a0, b0, *(of_chunk(summ, q, s, first, rows) for q in (A0, B0)))
        co[s - 1, 9, some, :] = e0
        co[s - 1, 10, some, :] = m0
    send[0:rows, :] = a0
    send[rows:2 * rows, :] = b0


def weigh(k, co, want_first, edge, weights):
    lam = (1.0 - want_first) + jnp.zeros((R, 128), F32)

    def at(s):
        return pl.ds(s, R, stride=8)

    for s in range(7, 0, -1):
        inv, w, lb2, la2, rb1 = (co[s - 1, n] for n in range(5))
        la2 = want_first * la2
        edge[1, at(s), :] = lam
        edge[0, at(s), :] = inv * (la2 + lam * (rb1 * lb2))
        lam = lam * (rb1 * (1.0 + lb2 * w)) + la2 * w
    edge[1, at(0), :] = lam
    edge[0, at(0), :] = want_first + jnp.zeros((R, 128), F32)
    parts = [(beside(edge, 0, b, 0), beside(edge, 1, b, 0)) for b in range(NB)]

    def step(blocks, n, state):
        rows = chunk_rows(C - 1 - n)
        out = []
        for b in blocks:
            first = k[PR, b, rows, :] + state[2 * b]
            last = state[2 * b + 1]
            na = k[NA, b, rows, :]
            weights[b, rows, :] = k[INV, b, rows, :] * (parts[b][0] * first + parts[b][1] * last)
            out += [na * first, na * last]
        return tuple(out)

    zero = jnp.zeros((8, 128), F32)
    sweep(range(NB), step, (zero, zero + 1.0) * NB)


def spread(co, first, rows, before, after, edge, rhs=True):
    def at(s):
        return pl.ds(first * 8 + s, rows, stride=8)
    some = pl.ds(first, rows)
    nxt = after
    edge[1, at(7), :] = after
    edge[0, at(0), :] = before
    for s in range(7, 0, -1):
        e1, e2, m1, m2, e0, m0 = (co[s - 1, n, some, :] for n in range(5, 11))
        last = m1 * before + m2 * nxt
        nxt = e1 * before + e2 * nxt
        if rhs:
            last, nxt = m0 + last, e0 + nxt
        edge[0, at(s), :] = last
        edge[1, at(s - 1), :] = nxt


def forward(k, rhs_of, g, summ, blocks, unroll=UNROLL):
    zero = jnp.zeros((8, 128), F32)

    def step(blocks, t, state):
        out = []
        rows = chunk_rows(t)
        for j, b in enumerate(blocks):
            inv = k[INV, b, rows, :]
            na = k[NA, b, rows, :]
            pr = k[PR, b, rows, :]
            rhs = rhs_of(b, t)
            for f in range(F):
                last, first = state[2 * (j * F + f):2 * (j * F + f) + 2]
                last = inv * rhs[f] + na * last
                g[b, f, rows, :] = last
                out += [last, first + pr * last]
        return tuple(out)

    state = (zero,) * (2 * F * len(blocks))
    if unroll == C:
        for t in range(C):
            state = step(blocks, t, state)
    else:
        state = sweep(blocks, step, state, unroll)
    for j, b in enumerate(blocks):
        for f in range(F):
            summ[B0 * R + row_of(b, f)] = state[2 * (j * F + f)]
            summ[A0 * R + row_of(b, f)] = state[2 * (j * F + f) + 1]


def backward(kb, g, edge, put, turn):
    def start(b):
        return tuple(beside(edge, 1, b, f) for f in range(F))

    def stepper(b):
        near = [beside(edge, 0, b, f) for f in range(F)]

        def step(_, n, state):
            out = []
            rows = chunk_rows(C - 1 - n)
            v = kb[V, b, rows, :]
            nc = kb[NC, b, rows, :]
            for f in range(F):
                x = (g[b, f, rows, :] + v * near[f]) + nc * state[f]
                put(b, f, rows, x)
                out.append(x)
            return tuple(out)
        return step

    def alone(b):
        sweep(b, stepper(b), start(b))

    def both(b, before):
        step = stepper(b)
        state = step(b, 0, start(b))
        for n in range(NB * F):
            for m in range(4):
                state = step(b, 1 + 4 * n + m, state)
            turn(before, n)

    def last(b):
        for n in range(NB * F):
            turn(b, n)

    return alone, both, last


def main_kernel(row_count, field, xl, xd, xu, yl, yd, yu, y, answer, ends,
                u, xk, xb, yn, yk, yb, r1, g, edge, sx, sy, cx, cy, pack, close, weights, dots, ends2,
                xcs, xcr, xrs, xrr, ycs, ycr, yrs, yrr,
                in_sem, field_sem, coef_sem, ps, pr, xcss, xcrs, xrss, xrrs, yss, yrsem):
    row = lax.axis_index("row")
    col = lax.axis_index("col")
    other = 1 - col
    lane = lax.broadcasted_iota(jnp.int32, (8, 128), 1)
    zero = jnp.zeros((8, 128), F32)
    src_block = (NB - 1) * other
    src_lane = 127 * other
    dst_lane = 127 * col

    def block(n):
        return n + col * (3 - 2 * n)

    def in_field(n):
        b = block(n)
        return [pltpu.make_async_copy(field.at[pl.ds(i * 128, 128), b],
                                      u.at[b, pl.ds((PAD + i * 128) * F, 128 * F)].reshape(128, F, 128), field_sem.at[n, i])
                for i in range(NB)]

    def in_coef(n):
        b = block(n)
        return [pltpu.make_async_copy(ref.at[:, pl.ds(pl.multiple_of(b * 128, 128), 128)], yn.at[i, b, pl.ds(PAD, T)], coef_sem.at[n, i])
                for i, ref in enumerate((yd, yl, yu))]

    in_x = [pltpu.make_async_copy(ref.at[:, pl.ds(b * 128, 128)], xk.at[n, b, pl.ds(PAD, T)], in_sem.at[n, b])
            for n, ref in enumerate((xd, xl, xu)) for b in range(NB)]

    def start(copies):
        for cp in copies:
            cp.start()

    def wait(copies):
        for cp in copies:
            cp.wait()

    start(in_field(3))

    barrier = pltpu.get_barrier_semaphore()
    for d in range(1, row_count):
        pl.semaphore_signal(barrier, inc=1, device_id={"row": lax.rem(row + d, row_count)}, device_id_type=MESH)
    pl.semaphore_signal(barrier, inc=1, device_id={"col": other}, device_id_type=MESH)

    for b in range(NB):
        for n in range(3):
            yn[n, b, 0:PAD, :] = zero
            xk[n, b, 0:PAD, :] = zero - 1.0 if n == LOW else zero
            yk[n, b, 0:PAD, :] = zero - 1.0 if n == LOW else zero
        for f in range(F):
            y[b, f, 0:PAD, :] = zero
    for b in range(NB):
        u[b, 0:PAD * F, :] = jnp.zeros((PAD * F, 128), F32)
    u[NB] = jnp.zeros((ROWS * F, 128), F32)

    def line_copies(send, recv, send_sem, recv_sem):
        return [pltpu.make_async_remote_copy(send, recv.at[d - 1], send_sem.at[d - 1], recv_sem.at[d - 1],
                                             device_id={"row": lax.rem(row + d, row_count)}, device_id_type=MESH)
                for d in range(1, row_count)]

    def to_line(*refs):
        copies = line_copies(*refs)
        for cp in copies:
            cp.start()
        return copies

    def to_pair(n, send, recv):
        cp = pltpu.make_async_remote_copy(send, recv, yss.at[n], yrsem.at[n], device_id={"col": other}, device_id_type=MESH)
        cp.start()
        return cp

    start(in_x)

    wait(in_field(3))
    start(in_field(0) + in_field(1) + in_coef(0))
    from_src = jnp.bitwise_and(lane - src_lane, 127)
    for h in range(2):
        acc = zero
        for p in range(128):
            w = PAD * F + 8 * (h * 128 + p)
            acc = jnp.where(from_src == p, pltpu.roll(u[src_block, w:w + 8, :], p, 1), acc)
        pack[0, h * 8:h * 8 + 8, :] = acc
    pl.semaphore_wait(barrier, row_count)
    column = pltpu.make_async_remote_copy(pack.at[0], pack.at[1], ps, pr, device_id={"col": other}, device_id_type=MESH)
    column.start()


    wait(in_x)
    start(in_field(2) + in_coef(1) + in_coef(2) + in_coef(3))
    factor(xk, xb, sx, 2.0)
    reduce_coef(sx, cx, xcs)
    coef_sends = to_line(xcs, xcr, xcss, xcrs)

    def stencil(b, t):
        rows = chunk_rows(t)
        cd = 1.0 - yn[DIAG, b, rows, :]
        cl = yn[LOW, b, rows, :]
        cu = yn[UPP, b, rows, :]
        left = lax.rem(b + NB, NB + 1)
        rhs = []
        for f in range(F):
            words = pl.ds(t * F + f, 8, stride=C * F)
            mid = u[b, words, :]
            prv = pltpu.roll(jnp.where(lane == 127, u[left, words, :], mid), 1, 1)
            nxt = pltpu.roll(jnp.where(lane == 0, u[b + 1, words, :], mid), 127, 1)
            v = (cd * mid - cl * prv) - cu * nxt
            r1[b, f, rows, :] = v
            rhs.append(v)
        return rhs

    halves = [col, other]

    def send_half(h):
        reduce_rhs(sx, cx, pl.multiple_of(halves[h] * H, 8), H, xrs.at[h])
        return to_line(xrs.at[h], xrr.at[h], xrss.at[h], xrrs.at[h])

    def eliminate(n, carry):
        wait(in_coef(n))

        @pl.when(n < 2)
        def _():
            wait(in_field(n + 1))

        @pl.when(n == 2)
        def _():
            send_half(0)

        @pl.when(n == 3)
        def _():
            column.wait()
            here = lane == dst_lane
            for i in range(2):
                got = pack[1, i * 8:i * 8 + 8, :]
                for p in range(128):
                    w = PAD * F + 8 * (i * 128 + p)
                    u[NB, w:w + 8, :] = jnp.where(here, pltpu.roll(got, (128 - p) % 128, 1), 0.0)

        forward(xk, stencil, g, sx, [block(n)], X_UNROLL)
        return carry

    wait(in_field(0))
    lax.fori_loop(0, NB, eliminate, 0)
    send_half(1)

    for b in range(NB):
        for c in range(NB):
            for n in range(3):
                yk[n, c, PAD + b * 128:PAD + b * 128 + 128, :] = yn[n, b, PAD + c * 128:PAD + c * 128 + 128, :].T
    factor(yk, yb, sy, 1)
    reduce_coef(sy, cy, ycs)
    y_coef = to_pair(0, ycs, ycr)
    weigh(yk, cy, jnp.where(col == 0, 0.0, 1.0), edge, weights)
    dots[...] = jnp.zeros((R, 8, 128), F32)

    for cp in coef_sends:
        cp.wait()

    def coef_of(ref):
        return tuple(ref[q * R:q * R + R, :] for q in range(4))

    slots = range(row_count - 3, -1, -1)
    rest = coef_of(xcr.at[row_count - 2])
    known = []
    for n in slots:
        rest, part, _ = join_coef(*rest, *coef_of(xcr.at[n]))
        known += part
    p1, p2, q1, q2 = rest
    a1, a2, b1, b2 = (cx[7, n] for n in range(4))
    m12 = p1 * b1 + p2 * a1
    i11 = 1.0 / (1.0 - (p1 * b2 + p2 * a2))
    m21 = (q1 * b2 + q2 * a2) * i11
    i22 = 1.0 / ((1.0 - (q1 * b1 + q2 * a1)) - m21 * m12)
    for n, v in enumerate(known + [p1, p2, q1, q2, m12, m21, i11, i22]):
        close[n] = v

    def close_line(h):
        for cp in line_copies(xrs.at[h], xrr.at[h], xrss.at[h], xrrs.at[h]):
            cp.wait()
        first = pl.multiple_of(halves[h] * H, 8)
        known = [close[n, pl.ds(first, H), :] for n in range(5 * (row_count - 2) + 8)]

        def received(n):
            return xrr[h, n, 0:H, :], xrr[h, n, H:2 * H, :]

        p0, q0 = received(row_count - 2)
        for i, n in enumerate(slots):
            p0, q0, _, _ = join_rhs(known[5 * i:5 * i + 5], p0, q0, *received(n))
        p1, p2, q1, q2, m12, m21, i11, i22 = known[5 * (row_count - 2):]
        a0, b0 = xrs[h, 0:H, :], xrs[h, H:2 * H, :]
        s1 = (p0 + p1 * b0) + p2 * a0
        s2 = (q0 + q1 * b0) + q2 * a0
        before = i22 * (s2 + m21 * s1)
        spread(cx, first, H, before, i11 * (s1 + m12 * before), edge)

    def put_x(b, f, rows, x):
        r1[b, f, rows, :] = x - r1[b, f, rows, :]

    def turn_in(b, n):
        c, f = n // F, n % F
        rows = pl.ds(pl.multiple_of(PAD + b * 128, 8), 128)
        square = r1[b, f, PAD + c * 128:PAD + c * 128 + 128, :].T
        y[c, f, rows, :] = square
        r = row_of(c, f)
        dots[r] = dots[r] + jnp.sum((square * weights[c, rows, :]).reshape(16, 8, 128), axis=0)

    alone, both, last = backward(xb, g, edge, put_x, turn_in)

    def solve(n, carry):
        @pl.when(n == 2)
        def _():
            close_line(1)

        both(block(n), block(n - 1))
        return carry

    close_line(0)
    alone(block(0))
    lax.fori_loop(1, NB, solve, 0)
    last(block(3))

    flat = dots.reshape(R * 8, 128)
    mine = flat[pl.ds(0, R, stride=8), :]
    for i in range(1, 8):
        mine = mine + flat[pl.ds(i, R, stride=8), :]
    yrs[...] = mine
    y_rhs = to_pair(1, yrs, yrr)

    def rhs_y(b, t):
        return [y[b, f, chunk_rows(t), :] for f in range(F)]

    forward(yk, rhs_y, g, sy, [0, 1])
    forward(yk, rhs_y, g, sy, [2, 3])
    reduce_rhs(sy, cy, 0, R, ends2)
    first = col == 0

    nothing = jnp.zeros((R, 128), F32)
    spread(cy, 0, R, nothing, nothing, edge)

    def put_y(b, f, rows, x):
        y[b, f, rows, :] = x

    alone, _, _ = backward(yb, g, edge, put_y, None)

    def solve_y(b, carry):
        alone(b)
        return carry

    lax.fori_loop(0, NB, solve_y, 0)
    one_left = jnp.where(first, 0.0, 1.0) + nothing
    spread(cy, 0, R, one_left, 1.0 - one_left, edge, False)
    near = [beside(edge, 0, b, 0) for b in range(NB)]

    def step_h(blocks, n, state):
        rows = chunk_rows(C - 1 - n)
        out = []
        for b in blocks:
            out.append(yb[V, b, rows, :] * near[b] + yb[NC, b, rows, :] * state[b])
            answer[b, rows, :] = out[b]
        return tuple(out)

    sweep(range(NB), step_h, tuple(beside(edge, 1, b, 0) for b in range(NB)))

    y_coef.wait()
    a1, b2 = cy[7, 0], cy[7, 3]
    c1, d2 = ycr[0:R, :], ycr[3 * R:4 * R, :]
    lb2 = jnp.where(first, b2, d2)
    ra1 = jnp.where(first, c1, a1)
    inv = 1.0 / (1.0 - lb2 * ra1)
    y_rhs.wait()
    mine = yrs[...]
    theirs = yrr[...]
    lb0 = jnp.where(first, mine, theirs)
    ra0 = jnp.where(first, theirs, mine)
    last_left = inv * (lb0 + lb2 * ra0)
    ends[...] = jnp.where(first, ra0 + ra1 * last_left, last_left)


def last_kernel(y, h, ends, out, o, out_sem):
    def copy_out(c, b):
        return pltpu.make_async_copy(o.at[b, pl.ds(pl.multiple_of(c * 128 * F, 8), 128 * F)].reshape(128, F, 128),
                                     out.at[pl.ds(c * 128, 128), b], out_sem.at[c, b])

    def turn_out(c, carry):
        for b in range(NB):
            part = h[c, PAD + b * 128:PAD + b * 128 + 128, :]
            for f in range(F):
                end = jnp.broadcast_to(ends[pl.ds(row_of(c, f), 1), :], (128, 128))
                o[b, pl.ds(c * 128 * F + f, 128, stride=F), :] = (
                    y[c, f, PAD + b * 128:PAD + b * 128 + 128, :] + part * end).T
            copy_out(c, b).start()
        return carry

    lax.fori_loop(0, NB, turn_out, 0)
    for c in range(NB):
        for b in range(NB):
            copy_out(c, b).wait()


def solution(mesh):
    row_count = mesh.shape["row"]
    field_spec = P(("batch", "row"), "col", None)
    coef_spec = P(("batch", "row"), "col")

    def local_step(field, x_lower, x_diag, x_upper, y_lower, y_diag, y_upper):
        words = field.reshape(T, NB, 128, F).transpose(0, 1, 3, 2)
        plane = (NB, ROWS, 128)
        fields = (NB, F, ROWS, 128)
        peers = row_count - 1
        in_vmem = pl.BlockSpec(memory_space=pltpu.VMEM)
        in_hbm = pl.BlockSpec(memory_space=pl.ANY)
        dma = pltpu.SemaphoreType.DMA
        parts = pl.pallas_call(
            functools.partial(main_kernel, row_count),
            out_shape=[pltpu.VMEM(fields, F32), pltpu.VMEM(plane, F32), pltpu.VMEM((R, 128), F32)],
            in_specs=[in_hbm] * 7,
            out_specs=[in_vmem] * 3,
            scratch_shapes=[
                pltpu.VMEM((NB + 1, ROWS * F, 128), F32),
                pltpu.VMEM((3,) + plane, F32),
                pltpu.VMEM((2,) + plane, F32),
                pltpu.VMEM((3,) + plane, F32),
                pltpu.VMEM((3,) + plane, F32),
                pltpu.VMEM((2,) + plane, F32),
                pltpu.VMEM(fields, F32),
                pltpu.VMEM(fields, F32),
                pltpu.VMEM((2, R * 8, 128), F32),
                pltpu.VMEM((6 * R, 8, 128), F32),
                pltpu.VMEM((6 * R, 8, 128), F32),
                pltpu.VMEM((8, 11, R, 128), F32),
                pltpu.VMEM((8, 11, R, 128), F32),
                pltpu.VMEM((2, 16, 128), F32),
                pltpu.VMEM((5 * (row_count - 2) + 8, R, 128), F32),
                pltpu.VMEM(plane, F32),
                pltpu.VMEM((R, 8, 128), F32),
                pltpu.VMEM((2 * R, 128), F32),
                pltpu.VMEM((4 * R, 128), F32),
                pltpu.VMEM((peers, 4 * R, 128), F32),
                pltpu.VMEM((2, R, 128), F32),
                pltpu.VMEM((2, peers, R, 128), F32),
                pltpu.VMEM((4 * R, 128), F32),
                pltpu.VMEM((4 * R, 128), F32),
                pltpu.VMEM((R, 128), F32),
                pltpu.VMEM((R, 128), F32),
                dma((3, NB)), dma((NB, NB)), dma((NB, 3)), dma, dma, dma((peers,)), dma((peers,)), dma((2, peers)), dma((2, peers)), dma((2,)), dma((2,)),
            ],
            compiler_params=pltpu.CompilerParams(
                collective_id=0, has_side_effects=True, vmem_limit_bytes=58 << 20),
        )(words, x_lower, x_diag, x_upper, y_lower, y_diag, y_upper)
        solved = pl.pallas_call(
            last_kernel,
            out_shape=jax.ShapeDtypeStruct((T, NB, F, 128), F32),
            in_specs=[in_vmem] * 3,
            out_specs=in_hbm,
            scratch_shapes=[pltpu.VMEM((NB, T * F, 128), F32), dma((NB, NB))],
            compiler_params=pltpu.CompilerParams(vmem_limit_bytes=16 << 20),
        )(*parts)
        return solved.transpose(0, 1, 3, 2).reshape(T, T, F)

    return jax.shard_map(local_step, mesh=mesh, in_specs=(field_spec,) + (coef_spec,) * 6,
                         out_specs=field_spec, check_vma=False)
```

```python
import functools

import jax
import jax.numpy as jnp
from jax import lax
from jax.experimental import pallas as pl
from jax.experimental.pallas import tpu as pltpu
from jax.sharding import PartitionSpec as P

MESH = pl.DeviceIdType.MESH
F32 = jnp.float32

T = 512
F = 4
C = 65
PAD = 8
ROWS = T + PAD
NB = T // 128
R = F * NB
UNROLL = 5

DIAG, LOW, UPP = 0, 1, 2
INV, NA, PR = 0, 1, 2
V, NC = 0, 1
A0, A1, A2, B0, B1, B2 = range(6)


H = R // 2
X_UNROLL = C


def chunk_rows(t):
    return pl.ds(t, 8, stride=C)


def row_of(b, f):
    if isinstance(b, int):
        return b // 2 * H + f * 2 + b % 2
    return lax.div(b, 2) * H + f * 2 + lax.rem(b, 2)


def beside(edge, side, b, f):
    return edge[side, pl.ds(pl.multiple_of(row_of(b, f) * 8, 8), 8), :]


def sweep(blocks, step, state, unroll=UNROLL):
    def steps(i, state):
        for n in range(unroll):
            state = step(blocks, i * unroll + n, state)
        return state
    return lax.fori_loop(0, C // unroll, steps, state)


def factor(k, kb, summ, scale):
    sub = lax.broadcasted_iota(jnp.int32, (8, 128), 0)
    zero = jnp.zeros((8, 128), F32)

    def step(blocks, t, state):
        out = []
        fresh = sub == jnp.where(t == PAD, 0, 8)
        for b in blocks:
            nc, v, pr, a1 = state[4 * b:4 * b + 4]
            rows = chunk_rows(t)
            low = k[LOW, b, rows, :]
            den = (1.0 + k[DIAG, b, rows, :]) + low * nc
            inv = 1.0 / den
            na = -(low * inv)
            nc = -(k[UPP, b, rows, :] * inv)
            v = na * v
            pr = jnp.where(fresh, 1.0, pr)
            k[INV, b, rows, :] = inv if scale == 1 else inv * scale
            k[NA, b, rows, :] = na
            k[PR, b, rows, :] = pr
            kb[NC, b, rows, :] = nc
            kb[V, b, rows, :] = v
            a1 = a1 + pr * v
            pr = pr * nc
            out += [nc, v, pr, a1]
        return tuple(out)

    state = (zero, zero + 1.0, jnp.where(sub == 0, 0.0, 1.0), zero) * NB
    state = sweep(range(NB), step, state)
    for b in range(NB):
        nc, v, pr, a1 = state[4 * b:4 * b + 4]
        for f in range(F):
            r = row_of(b, f)
            summ[A1 * R + r] = a1
            summ[A2 * R + r] = pr
            summ[B1 * R + r] = v
            summ[B2 * R + r] = nc


def of_chunk(summ, q, s, first=0, rows=R):
    return summ.reshape(6 * R * 8, 128)[pl.ds(q * R * 8 + first * 8 + s, rows, stride=8), :]


def join_coef(la1, la2, lb1, lb2, ra1, ra2, rb1, rb2):
    inv = 1.0 / (1.0 - ra1 * lb2)
    w = inv * ra1
    e1 = w * lb1
    e2 = inv * ra2
    m1 = lb1 + lb2 * e1
    m2 = lb2 * e2
    return (la1 + la2 * e1, la2 * e2, rb1 * m1, rb2 + rb1 * m2), (inv, w, lb2, la2, rb1), (e1, e2, m1, m2)


def join_rhs(part, la0, lb0, ra0, rb0):
    inv, w, lb2, la2, rb1 = part
    e0 = inv * ra0 + w * lb0
    m0 = lb0 + lb2 * e0
    return la0 + la2 * e0, rb0 + rb1 * m0, e0, m0


def reduce_coef(summ, co, send):
    def chunk(s):
        return tuple(of_chunk(summ, q, s) for q in (A1, A2, B1, B2))
    whole = chunk(0)
    for s in range(1, 8):
        whole, part, inner = join_coef(*whole, *chunk(s))
        for n, v in enumerate(part + inner):
            co[s - 1, n] = v
    for n, v in enumerate(whole):
        co[7, n] = v
        send[n * R:n * R + R, :] = v


def reduce_rhs(summ, co, first, rows, send):
    some = pl.ds(first, rows)
    a0, b0 = (of_chunk(summ, q, 0, first, rows) for q in (A0, B0))
    for s in range(1, 8):
        part = tuple(co[s - 1, n, some, :] for n in range(5))
        a0, b0, e0, m0 = join_rhs(part, a0, b0, *(of_chunk(summ, q, s, first, rows) for q in (A0, B0)))
        co[s - 1, 9, some, :] = e0
        co[s - 1, 10, some, :] = m0
    send[0:rows, :] = a0
    send[rows:2 * rows, :] = b0


def weigh(k, co, want_first, edge, weights):
    lam = (1.0 - want_first) + jnp.zeros((R, 128), F32)

    def at(s):
        return pl.ds(s, R, stride=8)

    for s in range(7, 0, -1):
        inv, w, lb2, la2, rb1 = (co[s - 1, n] for n in range(5))
        la2 = want_first * la2
        edge[1, at(s), :] = lam
        edge[0, at(s), :] = inv * (la2 + lam * (rb1 * lb2))
        lam = lam * (rb1 * (1.0 + lb2 * w)) + la2 * w
    edge[1, at(0), :] = lam
    edge[0, at(0), :] = want_first + jnp.zeros((R, 128), F32)
    parts = [(beside(edge, 0, b, 0), beside(edge, 1, b, 0)) for b in range(NB)]

    def step(blocks, n, state):
        rows = chunk_rows(C - 1 - n)
        out = []
        for b in blocks:
            first = k[PR, b, rows, :] + state[2 * b]
            last = state[2 * b + 1]
            na = k[NA, b, rows, :]
            weights[b, rows, :] = k[INV, b, rows, :] * (parts[b][0] * first + parts[b][1] * last)
            out += [na * first, na * last]
        return tuple(out)

    zero = jnp.zeros((8, 128), F32)
    sweep(range(NB), step, (zero, zero + 1.0) * NB)


def spread(co, first, rows, before, after, edge, rhs=True):
    def at(s):
        return pl.ds(first * 8 + s, rows, stride=8)
    some = pl.ds(first, rows)
    nxt = after
    edge[1, at(7), :] = after
    edge[0, at(0), :] = before
    for s in range(7, 0, -1):
        e1, e2, m1, m2, e0, m0 = (co[s - 1, n, some, :] for n in range(5, 11))
        last = m1 * before + m2 * nxt
        nxt = e1 * before + e2 * nxt
        if rhs:
            last, nxt = m0 + last, e0 + nxt
        edge[0, at(s), :] = last
        edge[1, at(s - 1), :] = nxt


def forward(k, rhs_of, g, summ, blocks, unroll=UNROLL):
    zero = jnp.zeros((8, 128), F32)

    def step(blocks, t, state):
        out = []
        rows = chunk_rows(t)
        for j, b in enumerate(blocks):
            inv = k[INV, b, rows, :]
            na = k[NA, b, rows, :]
            pr = k[PR, b, rows, :]
            rhs = rhs_of(b, t)
            for f in range(F):
                last, first = state[2 * (j * F + f):2 * (j * F + f) + 2]
                last = inv * rhs[f] + na * last
                g[b, f, rows, :] = last
                out += [last, first + pr * last]
        return tuple(out)

    state = (zero,) * (2 * F * len(blocks))
    if unroll == C:
        for t in range(C):
            state = step(blocks, t, state)
    else:
        state = sweep(blocks, step, state, unroll)
    for j, b in enumerate(blocks):
        for f in range(F):
            summ[B0 * R + row_of(b, f)] = state[2 * (j * F + f)]
            summ[A0 * R + row_of(b, f)] = state[2 * (j * F + f) + 1]


def backward(kb, g, edge, put, turn):
    def start(b):
        return tuple(beside(edge, 1, b, f) for f in range(F))

    def stepper(b):
        near = [beside(edge, 0, b, f) for f in range(F)]

        def step(_, n, state):
            out = []
            rows = chunk_rows(C - 1 - n)
            v = kb[V, b, rows, :]
            nc = kb[NC, b, rows, :]
            for f in range(F):
                x = (g[b, f, rows, :] + v * near[f]) + nc * state[f]
                put(b, f, rows, x)
                out.append(x)
            return tuple(out)
        return step

    def alone(b):
        sweep(b, stepper(b), start(b))

    def both(b, before):
        step = stepper(b)
        state = step(b, 0, start(b))
        for n in range(NB * F):
            turn(before, n)
            for m in range(4):
                state = step(b, 1 + 4 * n + m, state)

    def last(b):
        for n in range(NB * F):
            turn(b, n)

    return alone, both, last


def main_kernel(row_count, field, xl, xd, xu, yl, yd, yu, y, answer, ends,
                u, xk, xb, yn, yk, yb, r1, g, edge, sx, sy, cx, cy, pack, close, weights, dots, ends2,
                xcs, xcr, xrs, xrr, ycs, ycr, yrs, yrr,
                in_sem, field_sem, coef_sem, ps, pr, xcss, xcrs, xrss, xrrs, yss, yrsem):
    row = lax.axis_index("row")
    col = lax.axis_index("col")
    other = 1 - col
    lane = lax.broadcasted_iota(jnp.int32, (8, 128), 1)
    zero = jnp.zeros((8, 128), F32)
    src_block = (NB - 1) * other
    src_lane = 127 * other
    dst_lane = 127 * col

    def block(n):
        return n + col * (3 - 2 * n)

    def in_field(n):
        b = block(n)
        return [pltpu.make_async_copy(field.at[pl.ds(i * 128, 128), b],
                                      u.at[b, pl.ds((PAD + i * 128) * F, 128 * F)].reshape(128, F, 128), field_sem.at[n, i])
                for i in range(NB)]

    def in_coef(n):
        b = block(n)
        return [pltpu.make_async_copy(ref.at[:, pl.ds(pl.multiple_of(b * 128, 128), 128)], yn.at[i, b, pl.ds(PAD, T)], coef_sem.at[n, i])
                for i, ref in enumerate((yd, yl, yu))]

    in_x = [pltpu.make_async_copy(ref.at[:, pl.ds(b * 128, 128)], xk.at[n, b, pl.ds(PAD, T)], in_sem.at[n, b])
            for n, ref in enumerate((xd, xl, xu)) for b in range(NB)]

    def start(copies):
        for cp in copies:
            cp.start()

    def wait(copies):
        for cp in copies:
            cp.wait()

    start(in_field(3))

    barrier = pltpu.get_barrier_semaphore()
    for d in range(1, row_count):
        pl.semaphore_signal(barrier, inc=1, device_id={"row": lax.rem(row + d, row_count)}, device_id_type=MESH)
    pl.semaphore_signal(barrier, inc=1, device_id={"col": other}, device_id_type=MESH)

    for b in range(NB):
        for n in range(3):
            yn[n, b, 0:PAD, :] = zero
            xk[n, b, 0:PAD, :] = zero - 1.0 if n == LOW else zero
            yk[n, b, 0:PAD, :] = zero - 1.0 if n == LOW else zero
        for f in range(F):
            y[b, f, 0:PAD, :] = zero
    for b in range(NB):
        u[b, 0:PAD * F, :] = jnp.zeros((PAD * F, 128), F32)
    u[NB] = jnp.zeros((ROWS * F, 128), F32)

    def line_copies(send, recv, send_sem, recv_sem):
        return [pltpu.make_async_remote_copy(send, recv.at[d - 1], send_sem.at[d - 1], recv_sem.at[d - 1],
                                             device_id={"row": lax.rem(row + d, row_count)}, device_id_type=MESH)
                for d in range(1, row_count)]

    def to_line(*refs):
        copies = line_copies(*refs)
        for cp in copies:
            cp.start()
        return copies

    def to_pair(n, send, recv):
        cp = pltpu.make_async_remote_copy(send, recv, yss.at[n], yrsem.at[n], device_id={"col": other}, device_id_type=MESH)
        cp.start()
        return cp

    start(in_x)

    wait(in_field(3))
    start(in_field(0) + in_field(1) + in_coef(0))
    from_src = jnp.bitwise_and(lane - src_lane, 127)
    for h in range(2):
        acc = zero
        for p in range(128):
            w = PAD * F + 8 * (h * 128 + p)
            acc = jnp.where(from_src == p, pltpu.roll(u[src_block, w:w + 8, :], p, 1), acc)
        pack[0, h * 8:h * 8 + 8, :] = acc
    pl.semaphore_wait(barrier, row_count)
    column = pltpu.make_async_remote_copy(pack.at[0], pack.at[1], ps, pr, device_id={"col": other}, device_id_type=MESH)
    column.start()


    wait(in_x)
    start(in_field(2) + in_coef(1) + in_coef(2) + in_coef(3))
    factor(xk, xb, sx, 2.0)
    reduce_coef(sx, cx, xcs)
    coef_sends = to_line(xcs, xcr, xcss, xcrs)

    def stencil(b, t):
        rows = chunk_rows(t)
        cd = 1.0 - yn[DIAG, b, rows, :]
        cl = yn[LOW, b, rows, :]
        cu = yn[UPP, b, rows, :]
        left = lax.rem(b + NB, NB + 1)
        rhs = []
        for f in range(F):
            words = pl.ds(t * F + f, 8, stride=C * F)
            mid = u[b, words, :]
            prv = pltpu.roll(jnp.where(lane == 127, u[left, words, :], mid), 1, 1)
            nxt = pltpu.roll(jnp.where(lane == 0, u[b + 1, words, :], mid), 127, 1)
            v = (cd * mid - cl * prv) - cu * nxt
            r1[b, f, rows, :] = v
            rhs.append(v)
        return rhs

    halves = [col, other]

    def send_half(h):
        reduce_rhs(sx, cx, pl.multiple_of(halves[h] * H, 8), H, xrs.at[h])
        return to_line(xrs.at[h], xrr.at[h], xrss.at[h], xrrs.at[h])

    def eliminate(n, carry):
        wait(in_coef(n))

        @pl.when(n < 2)
        def _():
            wait(in_field(n + 1))

        @pl.when(n == 2)
        def _():
            send_half(0)

        @pl.when(n == 3)
        def _():
            column.wait()
            here = lane == dst_lane
            for i in range(2):
                got = pack[1, i * 8:i * 8 + 8, :]
                for p in range(128):
                    w = PAD * F + 8 * (i * 128 + p)
                    u[NB, w:w + 8, :] = jnp.where(here, pltpu.roll(got, (128 - p) % 128, 1), 0.0)

        forward(xk, stencil, g, sx, [block(n)], X_UNROLL)
        return carry

    wait(in_field(0))
    lax.fori_loop(0, NB, eliminate, 0)
    send_half(1)

    for b in range(NB):
        for c in range(NB):
            for n in range(3):
                yk[n, c, PAD + b * 128:PAD + b * 128 + 128, :] = yn[n, b, PAD + c * 128:PAD + c * 128 + 128, :].T
    factor(yk, yb, sy, 1)
    reduce_coef(sy, cy, ycs)
    y_coef = to_pair(0, ycs, ycr)
    weigh(yk, cy, jnp.where(col == 0, 0.0, 1.0), edge, weights)
    dots[...] = jnp.zeros((R, 8, 128), F32)

    for cp in coef_sends:
        cp.wait()

    def coef_of(ref):
        return tuple(ref[q * R:q * R + R, :] for q in range(4))

    slots = range(row_count - 3, -1, -1)
    rest = coef_of(xcr.at[row_count - 2])
    known = []
    for n in slots:
        rest, part, _ = join_coef(*rest, *coef_of(xcr.at[n]))
        known += part
    p1, p2, q1, q2 = rest
    a1, a2, b1, b2 = (cx[7, n] for n in range(4))
    m12 = p1 * b1 + p2 * a1
    i11 = 1.0 / (1.0 - (p1 * b2 + p2 * a2))
    m21 = (q1 * b2 + q2 * a2) * i11
    i22 = 1.0 / ((1.0 - (q1 * b1 + q2 * a1)) - m21 * m12)
    for n, v in enumerate(known + [p1, p2, q1, q2, m12, m21, i11, i22]):
        close[n] = v

    def close_line(h):
        for cp in line_copies(xrs.at[h], xrr.at[h], xrss.at[h], xrrs.at[h]):
            cp.wait()
        first = pl.multiple_of(halves[h] * H, 8)
        known = [close[n, pl.ds(first, H), :] for n in range(5 * (row_count - 2) + 8)]

        def received(n):
            return xrr[h, n, 0:H, :], xrr[h, n, H:2 * H, :]

        p0, q0 = received(row_count - 2)
        for i, n in enumerate(slots):
            p0, q0, _, _ = join_rhs(known[5 * i:5 * i + 5], p0, q0, *received(n))
        p1, p2, q1, q2, m12, m21, i11, i22 = known[5 * (row_count - 2):]
        a0, b0 = xrs[h, 0:H, :], xrs[h, H:2 * H, :]
        s1 = (p0 + p1 * b0) + p2 * a0
        s2 = (q0 + q1 * b0) + q2 * a0
        before = i22 * (s2 + m21 * s1)
        spread(cx, first, H, before, i11 * (s1 + m12 * before), edge)

    def put_x(b, f, rows, x):
        r1[b, f, rows, :] = x - r1[b, f, rows, :]

    def turn_in(b, n):
        c, f = n // F, n % F
        rows = pl.ds(pl.multiple_of(PAD + b * 128, 8), 128)
        square = r1[b, f, PAD + c * 128:PAD + c * 128 + 128, :].T
        y[c, f, rows, :] = square
        r = row_of(c, f)
        dots[r] = dots[r] + jnp.sum((square * weights[c, rows, :]).reshape(16, 8, 128), axis=0)

    alone, both, last = backward(xb, g, edge, put_x, turn_in)

    def solve(n, carry):
        @pl.when(n == 2)
        def _():
            close_line(1)

        both(block(n), block(n - 1))
        return carry

    close_line(0)
    alone(block(0))
    lax.fori_loop(1, NB, solve, 0)
    last(block(3))

    flat = dots.reshape(R * 8, 128)
    mine = flat[pl.ds(0, R, stride=8), :]
    for i in range(1, 8):
        mine = mine + flat[pl.ds(i, R, stride=8), :]
    yrs[...] = mine
    y_rhs = to_pair(1, yrs, yrr)

    def rhs_y(b, t):
        return [y[b, f, chunk_rows(t), :] for f in range(F)]

    forward(yk, rhs_y, g, sy, [0, 1])
    forward(yk, rhs_y, g, sy, [2, 3])
    reduce_rhs(sy, cy, 0, R, ends2)
    first = col == 0

    nothing = jnp.zeros((R, 128), F32)
    spread(cy, 0, R, nothing, nothing, edge)

    def put_y(b, f, rows, x):
        y[b, f, rows, :] = x

    alone, _, _ = backward(yb, g, edge, put_y, None)

    def solve_y(b, carry):
        alone(b)
        return carry

    lax.fori_loop(0, NB, solve_y, 0)
    one_left = jnp.where(first, 0.0, 1.0) + nothing
    spread(cy, 0, R, one_left, 1.0 - one_left, edge, False)
    near = [beside(edge, 0, b, 0) for b in range(NB)]

    def step_h(blocks, n, state):
        rows = chunk_rows(C - 1 - n)
        out = []
        for b in blocks:
            out.append(yb[V, b, rows, :] * near[b] + yb[NC, b, rows, :] * state[b])
            answer[b, rows, :] = out[b]
        return tuple(out)

    sweep(range(NB), step_h, tuple(beside(edge, 1, b, 0) for b in range(NB)))

    y_coef.wait()
    a1, b2 = cy[7, 0], cy[7, 3]
    c1, d2 = ycr[0:R, :], ycr[3 * R:4 * R, :]
    lb2 = jnp.where(first, b2, d2)
    ra1 = jnp.where(first, c1, a1)
    inv = 1.0 / (1.0 - lb2 * ra1)
    y_rhs.wait()
    mine = yrs[...]
    theirs = yrr[...]
    lb0 = jnp.where(first, mine, theirs)
    ra0 = jnp.where(first, theirs, mine)
    last_left = inv * (lb0 + lb2 * ra0)
    ends[...] = jnp.where(first, ra0 + ra1 * last_left, last_left)


def last_kernel(y, h, ends, out, o, out_sem):
    def copy_out(c, b):
        return pltpu.make_async_copy(o.at[b, pl.ds(pl.multiple_of(c * 128 * F, 8), 128 * F)].reshape(128, F, 128),
                                     out.at[pl.ds(c * 128, 128), b], out_sem.at[c, b])

    def turn_out(c, carry):
        for b in range(NB):
            part = h[c, PAD + b * 128:PAD + b * 128 + 128, :]
            for f in range(F):
                end = jnp.broadcast_to(ends[pl.ds(row_of(c, f), 1), :], (128, 128))
                o[b, pl.ds(c * 128 * F + f, 128, stride=F), :] = (
                    y[c, f, PAD + b * 128:PAD + b * 128 + 128, :] + part * end).T
            copy_out(c, b).start()
        return carry

    lax.fori_loop(0, NB, turn_out, 0)
    for c in range(NB):
        for b in range(NB):
            copy_out(c, b).wait()


def solution(mesh):
    row_count = mesh.shape["row"]
    field_spec = P(("batch", "row"), "col", None)
    coef_spec = P(("batch", "row"), "col")

    def local_step(field, x_lower, x_diag, x_upper, y_lower, y_diag, y_upper):
        words = field.reshape(T, NB, 128, F).transpose(0, 1, 3, 2)
        plane = (NB, ROWS, 128)
        fields = (NB, F, ROWS, 128)
        peers = row_count - 1
        in_vmem = pl.BlockSpec(memory_space=pltpu.VMEM)
        in_hbm = pl.BlockSpec(memory_space=pl.ANY)
        dma = pltpu.SemaphoreType.DMA
        parts = pl.pallas_call(
            functools.partial(main_kernel, row_count),
            out_shape=[pltpu.VMEM(fields, F32), pltpu.VMEM(plane, F32), pltpu.VMEM((R, 128), F32)],
            in_specs=[in_hbm] * 7,
            out_specs=[in_vmem] * 3,
            scratch_shapes=[
                pltpu.VMEM((NB + 1, ROWS * F, 128), F32),
                pltpu.VMEM((3,) + plane, F32),
                pltpu.VMEM((2,) + plane, F32),
                pltpu.VMEM((3,) + plane, F32),
                pltpu.VMEM((3,) + plane, F32),
                pltpu.VMEM((2,) + plane, F32),
                pltpu.VMEM(fields, F32),
                pltpu.VMEM(fields, F32),
                pltpu.VMEM((2, R * 8, 128), F32),
                pltpu.VMEM((6 * R, 8, 128), F32),
                pltpu.VMEM((6 * R, 8, 128), F32),
                pltpu.VMEM((8, 11, R, 128), F32),
                pltpu.VMEM((8, 11, R, 128), F32),
                pltpu.VMEM((2, 16, 128), F32),
                pltpu.VMEM((5 * (row_count - 2) + 8, R, 128), F32),
                pltpu.VMEM(plane, F32),
                pltpu.VMEM((R, 8, 128), F32),
                pltpu.VMEM((2 * R, 128), F32),
                pltpu.VMEM((4 * R, 128), F32),
                pltpu.VMEM((peers, 4 * R, 128), F32),
                pltpu.VMEM((2, R, 128), F32),
                pltpu.VMEM((2, peers, R, 128), F32),
                pltpu.VMEM((4 * R, 128), F32),
                pltpu.VMEM((4 * R, 128), F32),
                pltpu.VMEM((R, 128), F32),
                pltpu.VMEM((R, 128), F32),
                dma((3, NB)), dma((NB, NB)), dma((NB, 3)), dma, dma, dma((peers,)), dma((peers,)), dma((2, peers)), dma((2, peers)), dma((2,)), dma((2,)),
            ],
            compiler_params=pltpu.CompilerParams(
                collective_id=0, has_side_effects=True, vmem_limit_bytes=58 << 20),
        )(words, x_lower, x_diag, x_upper, y_lower, y_diag, y_upper)
        solved = pl.pallas_call(
            last_kernel,
            out_shape=jax.ShapeDtypeStruct((T, NB, F, 128), F32),
            in_specs=[in_vmem] * 3,
            out_specs=in_hbm,
            scratch_shapes=[pltpu.VMEM((NB, T * F, 128), F32), dma((NB, NB))],
            compiler_params=pltpu.CompilerParams(vmem_limit_bytes=16 << 20),
        )(*parts)
        return solved.transpose(0, 1, 3, 2).reshape(T, T, F)

    return jax.shard_map(local_step, mesh=mesh, in_specs=(field_spec,) + (coef_spec,) * 6,
                         out_specs=field_spec, check_vma=False)
```

```python
import functools

import jax
import jax.numpy as jnp
from jax import lax
from jax.experimental import pallas as pl
from jax.experimental.pallas import tpu as pltpu
from jax.sharding import PartitionSpec as P

MESH = pl.DeviceIdType.MESH
F32 = jnp.float32

T = 512
F = 4
C = 65
PAD = 8
ROWS = T + PAD
NB = T // 128
R = F * NB
UNROLL = 5

DIAG, LOW, UPP = 0, 1, 2
INV, NA, PR = 0, 1, 2
V, NC = 0, 1
A0, A1, A2, B0, B1, B2 = range(6)


H = R // 2
X_UNROLL = C


def chunk_rows(t):
    return pl.ds(t, 8, stride=C)


def row_of(b, f):
    if isinstance(b, int):
        return b // 2 * H + f * 2 + b % 2
    return lax.div(b, 2) * H + f * 2 + lax.rem(b, 2)


def beside(edge, side, b, f):
    return edge[side, pl.ds(pl.multiple_of(row_of(b, f) * 8, 8), 8), :]


def sweep(blocks, step, state, unroll=UNROLL):
    def steps(i, state):
        for n in range(unroll):
            state = step(blocks, i * unroll + n, state)
        return state
    return lax.fori_loop(0, C // unroll, steps, state)


def factor(k, kb, summ, scale):
    sub = lax.broadcasted_iota(jnp.int32, (8, 128), 0)
    zero = jnp.zeros((8, 128), F32)

    def step(blocks, t, state):
        out = []
        fresh = sub == jnp.where(t == PAD, 0, 8)
        for b in blocks:
            nc, v, pr, a1 = state[4 * b:4 * b + 4]
            rows = chunk_rows(t)
            low = k[LOW, b, rows, :]
            den = (1.0 + k[DIAG, b, rows, :]) + low * nc
            inv = 1.0 / den
            na = -(low * inv)
            nc = -(k[UPP, b, rows, :] * inv)
            v = na * v
            pr = jnp.where(fresh, 1.0, pr)
            k[INV, b, rows, :] = inv if scale == 1 else inv * scale
            k[NA, b, rows, :] = na
            k[PR, b, rows, :] = pr
            kb[NC, b, rows, :] = nc
            kb[V, b, rows, :] = v
            a1 = a1 + pr * v
            pr = pr * nc
            out += [nc, v, pr, a1]
        return tuple(out)

    state = (zero, zero + 1.0, jnp.where(sub == 0, 0.0, 1.0), zero) * NB
    state = sweep(range(NB), step, state)
    for b in range(NB):
        nc, v, pr, a1 = state[4 * b:4 * b + 4]
        for f in range(F):
            r = row_of(b, f)
            summ[A1 * R + r] = a1
            summ[A2 * R + r] = pr
            summ[B1 * R + r] = v
            summ[B2 * R + r] = nc


def of_chunk(summ, q, s, first=0, rows=R):
    return summ.reshape(6 * R * 8, 128)[pl.ds(q * R * 8 + first * 8 + s, rows, stride=8), :]


def join_coef(la1, la2, lb1, lb2, ra1, ra2, rb1, rb2):
    inv = 1.0 / (1.0 - ra1 * lb2)
    w = inv * ra1
    e1 = w * lb1
    e2 = inv * ra2
    m1 = lb1 + lb2 * e1
    m2 = lb2 * e2
    return (la1 + la2 * e1, la2 * e2, rb1 * m1, rb2 + rb1 * m2), (inv, w, lb2, la2, rb1), (e1, e2, m1, m2)


def join_rhs(part, la0, lb0, ra0, rb0):
    inv, w, lb2, la2, rb1 = part
    e0 = inv * ra0 + w * lb0
    m0 = lb0 + lb2 * e0
    return la0 + la2 * e0, rb0 + rb1 * m0, e0, m0


def reduce_coef(summ, co, send):
    def chunk(s):
        return tuple(of_chunk(summ, q, s) for q in (A1, A2, B1, B2))
    whole = chunk(0)
    for s in range(1, 8):
        whole, part, inner = join_coef(*whole, *chunk(s))
        for n, v in enumerate(part + inner):
            co[s - 1, n] = v
    for n, v in enumerate(whole):
        co[7, n] = v
        send[n * R:n * R + R, :] = v


def reduce_rhs(summ, co, first, rows, send):
    some = pl.ds(first, rows)
    a0, b0 = (of_chunk(summ, q, 0, first, rows) for q in (A0, B0))
    for s in range(1, 8):
        part = tuple(co[s - 1, n, some, :] for n in range(5))
        a0, b0, e0, m0 = join_rhs(part, a0, b0, *(of_chunk(summ, q, s, first, rows) for q in (A0, B0)))
        co[s - 1, 9, some, :] = e0
        co[s - 1, 10, some, :] = m0
    send[0:rows, :] = a0
    send[rows:2 * rows, :] = b0


def weigh(k, co, want_first, edge, weights):
    lam = (1.0 - want_first) + jnp.zeros((R, 128), F32)

    def at(s):
        return pl.ds(s, R, stride=8)

    for s in range(7, 0, -1):
        inv, w, lb2, la2, rb1 = (co[s - 1, n] for n in range(5))
        la2 = want_first * la2
        edge[1, at(s), :] = lam
        edge[0, at(s), :] = inv * (la2 + lam * (rb1 * lb2))
        lam = lam * (rb1 * (1.0 + lb2 * w)) + la2 * w
    edge[1, at(0), :] = lam
    edge[0, at(0), :] = want_first + jnp.zeros((R, 128), F32)
    parts = [(beside(edge, 0, b, 0), beside(edge, 1, b, 0)) for b in range(NB)]

    def step(blocks, n, state):
        rows = chunk_rows(C - 1 - n)
        out = []
        for b in blocks:
            first = k[PR, b, rows, :] + state[2 * b]
            last = state[2 * b + 1]
            na = k[NA, b, rows, :]
            weights[b, rows, :] = k[INV, b, rows, :] * (parts[b][0] * first + parts[b][1] * last)
            out += [na * first, na * last]
        return tuple(out)

    zero = jnp.zeros((8, 128), F32)
    return step, (zero, zero + 1.0) * NB


def spread(co, first, rows, before, after, edge, rhs=True):
    def at(s):
        return pl.ds(first * 8 + s, rows, stride=8)
    some = pl.ds(first, rows)
    nxt = after
    edge[1, at(7), :] = after
    edge[0, at(0), :] = before
    for s in range(7, 0, -1):
        e1, e2, m1, m2, e0, m0 = (co[s - 1, n, some, :] for n in range(5, 11))
        last = m1 * before + m2 * nxt
        nxt = e1 * before + e2 * nxt
        if rhs:
            last, nxt = m0 + last, e0 + nxt
        edge[0, at(s), :] = last
        edge[1, at(s - 1), :] = nxt


def forward(k, rhs_of, g, summ, blocks, unroll=UNROLL):
    zero = jnp.zeros((8, 128), F32)

    def step(blocks, t, state):
        out = []
        rows = chunk_rows(t)
        for j, b in enumerate(blocks):
            inv = k[INV, b, rows, :]
            na = k[NA, b, rows, :]
            pr = k[PR, b, rows, :]
            rhs = rhs_of(b, t)
            for f in range(F):
                last, first = state[2 * (j * F + f):2 * (j * F + f) + 2]
                last = inv * rhs[f] + na * last
                g[b, f, rows, :] = last
                out += [last, first + pr * last]
        return tuple(out)

    state = (zero,) * (2 * F * len(blocks))
    if unroll == C:
        for t in range(C):
            state = step(blocks, t, state)
    else:
        state = sweep(blocks, step, state, unroll)
    for j, b in enumerate(blocks):
        for f in range(F):
            summ[B0 * R + row_of(b, f)] = state[2 * (j * F + f)]
            summ[A0 * R + row_of(b, f)] = state[2 * (j * F + f) + 1]


def backward(kb, g, edge, put, turn):
    def start(b):
        return tuple(beside(edge, 1, b, f) for f in range(F))

    def stepper(b):
        near = [beside(edge, 0, b, f) for f in range(F)]

        def step(_, n, state):
            out = []
            rows = chunk_rows(C - 1 - n)
            v = kb[V, b, rows, :]
            nc = kb[NC, b, rows, :]
            for f in range(F):
                x = (g[b, f, rows, :] + v * near[f]) + nc * state[f]
                put(b, f, rows, x)
                out.append(x)
            return tuple(out)
        return step

    def alone(b, more=None, more_start=()):
        step = stepper(b)

        def step_all(blocks, n, state):
            state = step(blocks, n, state[:F]) + state[F:]
            return state if more is None else state[:F] + more(range(NB), n, state[F:])

        sweep(b, step_all, start(b) + more_start)

    def both(b, before):
        step = stepper(b)
        state = step(b, 0, start(b))
        for n in range(NB * F):
            turn(before, n)
            for m in range(4):
                state = step(b, 1 + 4 * n + m, state)

    def last(b):
        for n in range(NB * F):
            turn(b, n)

    return alone, both, last


def main_kernel(row_count, field, xl, xd, xu, yl, yd, yu, y, answer, ends,
                u, xk, xb, yn, yk, yb, r1, g, edge, sx, sy, cx, cy, pack, close, weights, dots, ends2, tilt,
                xcs, xcr, xrs, xrr, ycs, ycr, yrs, yrr,
                in_sem, field_sem, coef_sem, ps, pr, xcss, xcrs, xrss, xrrs, yss, yrsem):
    row = lax.axis_index("row")
    col = lax.axis_index("col")
    other = 1 - col
    lane = lax.broadcasted_iota(jnp.int32, (8, 128), 1)
    zero = jnp.zeros((8, 128), F32)
    src_block = (NB - 1) * other
    src_lane = 127 * other
    dst_lane = 127 * col

    def block(n):
        return n + col * (3 - 2 * n)

    def in_field(n):
        b = block(n)
        return [pltpu.make_async_copy(field.at[pl.ds(i * 128, 128), b],
                                      u.at[b, pl.ds((PAD + i * 128) * F, 128 * F)].reshape(128, F, 128), field_sem.at[n, i])
                for i in range(NB)]

    def in_coef(n):
        b = block(n)
        return [pltpu.make_async_copy(ref.at[:, pl.ds(pl.multiple_of(b * 128, 128), 128)], yn.at[i, b, pl.ds(PAD, T)], coef_sem.at[n, i])
                for i, ref in enumerate((yd, yl, yu))]

    in_x = [pltpu.make_async_copy(ref.at[:, pl.ds(b * 128, 128)], xk.at[n, b, pl.ds(PAD, T)], in_sem.at[n, b])
            for n, ref in enumerate((xd, xl, xu)) for b in range(NB)]

    def start(copies):
        for cp in copies:
            cp.start()

    def wait(copies):
        for cp in copies:
            cp.wait()

    start(in_field(3))

    barrier = pltpu.get_barrier_semaphore()
    for d in range(1, row_count):
        pl.semaphore_signal(barrier, inc=1, device_id={"row": lax.rem(row + d, row_count)}, device_id_type=MESH)
    pl.semaphore_signal(barrier, inc=1, device_id={"col": other}, device_id_type=MESH)

    for b in range(NB):
        for n in range(3):
            yn[n, b, 0:PAD, :] = zero
            xk[n, b, 0:PAD, :] = zero - 1.0 if n == LOW else zero
            yk[n, b, 0:PAD, :] = zero - 1.0 if n == LOW else zero
        for f in range(F):
            y[b, f, 0:PAD, :] = zero
    for b in range(NB):
        u[b, 0:PAD * F, :] = jnp.zeros((PAD * F, 128), F32)
    u[NB] = jnp.zeros((ROWS * F, 128), F32)

    def line_copies(send, recv, send_sem, recv_sem):
        return [pltpu.make_async_remote_copy(send, recv.at[d - 1], send_sem.at[d - 1], recv_sem.at[d - 1],
                                             device_id={"row": lax.rem(row + d, row_count)}, device_id_type=MESH)
                for d in range(1, row_count)]

    def to_line(*refs):
        copies = line_copies(*refs)
        for cp in copies:
            cp.start()
        return copies

    def to_pair(n, send, recv):
        cp = pltpu.make_async_remote_copy(send, recv, yss.at[n], yrsem.at[n], device_id={"col": other}, device_id_type=MESH)
        cp.start()
        return cp

    start(in_x)

    wait(in_field(3))
    start(in_field(0) + in_field(1) + in_coef(0))
    from_src = jnp.bitwise_and(lane - src_lane, 127)
    for h in range(2):
        acc = zero
        for p in range(128):
            w = PAD * F + 8 * (h * 128 + p)
            acc = jnp.where(from_src == p, pltpu.roll(u[src_block, w:w + 8, :], p, 1), acc)
        pack[0, h * 8:h * 8 + 8, :] = acc
    pl.semaphore_wait(barrier, row_count)
    column = pltpu.make_async_remote_copy(pack.at[0], pack.at[1], ps, pr, device_id={"col": other}, device_id_type=MESH)
    column.start()


    wait(in_x)
    start(in_field(2) + in_coef(1) + in_coef(2) + in_coef(3))
    factor(xk, xb, sx, 2.0)
    reduce_coef(sx, cx, xcs)
    coef_sends = to_line(xcs, xcr, xcss, xcrs)

    def stencil(b, t):
        rows = chunk_rows(t)
        cd = 1.0 - yn[DIAG, b, rows, :]
        cl = yn[LOW, b, rows, :]
        cu = yn[UPP, b, rows, :]
        left = lax.rem(b + NB, NB + 1)
        rhs = []
        for f in range(F):
            words = pl.ds(t * F + f, 8, stride=C * F)
            mid = u[b, words, :]
            prv = pltpu.roll(jnp.where(lane == 127, u[left, words, :], mid), 1, 1)
            nxt = pltpu.roll(jnp.where(lane == 0, u[b + 1, words, :], mid), 127, 1)
            v = (cd * mid - cl * prv) - cu * nxt
            r1[b, f, rows, :] = v
            rhs.append(v)
        return rhs

    halves = [col, other]

    def send_half(h):
        reduce_rhs(sx, cx, pl.multiple_of(halves[h] * H, 8), H, xrs.at[h])
        return to_line(xrs.at[h], xrr.at[h], xrss.at[h], xrrs.at[h])

    def eliminate(n, carry):
        wait(in_coef(n))

        @pl.when(n < 2)
        def _():
            wait(in_field(n + 1))

        @pl.when(n == 2)
        def _():
            send_half(0)

        @pl.when(n == 3)
        def _():
            column.wait()
            here = lane == dst_lane
            for i in range(2):
                got = pack[1, i * 8:i * 8 + 8, :]
                for p in range(128):
                    w = PAD * F + 8 * (i * 128 + p)
                    u[NB, w:w + 8, :] = jnp.where(here, pltpu.roll(got, (128 - p) % 128, 1), 0.0)

        forward(xk, stencil, g, sx, [block(n)], X_UNROLL)
        return carry

    wait(in_field(0))
    lax.fori_loop(0, NB, eliminate, 0)
    send_half(1)

    for b in range(NB):
        for c in range(NB):
            for n in range(3):
                yk[n, c, PAD + b * 128:PAD + b * 128 + 128, :] = yn[n, b, PAD + c * 128:PAD + c * 128 + 128, :].T
    factor(yk, yb, sy, 1)
    reduce_coef(sy, cy, ycs)
    y_coef = to_pair(0, ycs, ycr)
    weigh_step, weigh_start = weigh(yk, cy, jnp.where(col == 0, 0.0, 1.0), tilt, weights)
    dots[...] = jnp.zeros((R, 8, 128), F32)

    for cp in coef_sends:
        cp.wait()

    def coef_of(ref):
        return tuple(ref[q * R:q * R + R, :] for q in range(4))

    slots = range(row_count - 3, -1, -1)
    rest = coef_of(xcr.at[row_count - 2])
    known = []
    for n in slots:
        rest, part, _ = join_coef(*rest, *coef_of(xcr.at[n]))
        known += part
    p1, p2, q1, q2 = rest
    a1, a2, b1, b2 = (cx[7, n] for n in range(4))
    m12 = p1 * b1 + p2 * a1
    i11 = 1.0 / (1.0 - (p1 * b2 + p2 * a2))
    m21 = (q1 * b2 + q2 * a2) * i11
    i22 = 1.0 / ((1.0 - (q1 * b1 + q2 * a1)) - m21 * m12)
    for n, v in enumerate(known + [p1, p2, q1, q2, m12, m21, i11, i22]):
        close[n] = v

    def close_line(h):
        for cp in line_copies(xrs.at[h], xrr.at[h], xrss.at[h], xrrs.at[h]):
            cp.wait()
        first = pl.multiple_of(halves[h] * H, 8)
        known = [close[n, pl.ds(first, H), :] for n in range(5 * (row_count - 2) + 8)]

        def received(n):
            return xrr[h, n, 0:H, :], xrr[h, n, H:2 * H, :]

        p0, q0 = received(row_count - 2)
        for i, n in enumerate(slots):
            p0, q0, _, _ = join_rhs(known[5 * i:5 * i + 5], p0, q0, *received(n))
        p1, p2, q1, q2, m12, m21, i11, i22 = known[5 * (row_count - 2):]
        a0, b0 = xrs[h, 0:H, :], xrs[h, H:2 * H, :]
        s1 = (p0 + p1 * b0) + p2 * a0
        s2 = (q0 + q1 * b0) + q2 * a0
        before = i22 * (s2 + m21 * s1)
        spread(cx, first, H, before, i11 * (s1 + m12 * before), edge)

    def put_x(b, f, rows, x):
        r1[b, f, rows, :] = x - r1[b, f, rows, :]

    def turn_in(b, n):
        c, f = n // F, n % F
        rows = pl.ds(pl.multiple_of(PAD + b * 128, 8), 128)
        square = r1[b, f, PAD + c * 128:PAD + c * 128 + 128, :].T
        y[c, f, rows, :] = square
        r = row_of(c, f)
        dots[r] = dots[r] + jnp.sum((square * weights[c, rows, :]).reshape(16, 8, 128), axis=0)

    alone, both, last = backward(xb, g, edge, put_x, turn_in)

    def solve(n, carry):
        @pl.when(n == 2)
        def _():
            close_line(1)

        both(block(n), block(n - 1))
        return carry

    close_line(0)
    alone(block(0), weigh_step, weigh_start)
    lax.fori_loop(1, NB, solve, 0)
    last(block(3))

    flat = dots.reshape(R * 8, 128)
    mine = flat[pl.ds(0, R, stride=8), :]
    for i in range(1, 8):
        mine = mine + flat[pl.ds(i, R, stride=8), :]
    yrs[...] = mine
    y_rhs = to_pair(1, yrs, yrr)

    def rhs_y(b, t):
        return [y[b, f, chunk_rows(t), :] for f in range(F)]

    forward(yk, rhs_y, g, sy, [0, 1])
    forward(yk, rhs_y, g, sy, [2, 3])
    reduce_rhs(sy, cy, 0, R, ends2)
    first = col == 0

    nothing = jnp.zeros((R, 128), F32)
    spread(cy, 0, R, nothing, nothing, edge)

    def put_y(b, f, rows, x):
        y[b, f, rows, :] = x

    alone, _, _ = backward(yb, g, edge, put_y, None)

    def solve_y(b, carry):
        alone(b)
        return carry

    lax.fori_loop(0, NB, solve_y, 0)
    one_left = jnp.where(first, 0.0, 1.0) + nothing
    spread(cy, 0, R, one_left, 1.0 - one_left, edge, False)
    near = [beside(edge, 0, b, 0) for b in range(NB)]

    def step_h(blocks, n, state):
        rows = chunk_rows(C - 1 - n)
        out = []
        for b in blocks:
            out.append(yb[V, b, rows, :] * near[b] + yb[NC, b, rows, :] * state[b])
            answer[b, rows, :] = out[b]
        return tuple(out)

    sweep(range(NB), step_h, tuple(beside(edge, 1, b, 0) for b in range(NB)))

    y_coef.wait()
    a1, b2 = cy[7, 0], cy[7, 3]
    c1, d2 = ycr[0:R, :], ycr[3 * R:4 * R, :]
    lb2 = jnp.where(first, b2, d2)
    ra1 = jnp.where(first, c1, a1)
    inv = 1.0 / (1.0 - lb2 * ra1)
    y_rhs.wait()
    mine = yrs[...]
    theirs = yrr[...]
    lb0 = jnp.where(first, mine, theirs)
    ra0 = jnp.where(first, theirs, mine)
    last_left = inv * (lb0 + lb2 * ra0)
    ends[...] = jnp.where(first, ra0 + ra1 * last_left, last_left)


def last_kernel(y, h, ends, out, o, out_sem):
    def copy_out(c, b):
        return pltpu.make_async_copy(o.at[b, pl.ds(pl.multiple_of(c * 128 * F, 8), 128 * F)].reshape(128, F, 128),
                                     out.at[pl.ds(c * 128, 128), b], out_sem.at[c, b])

    def turn_out(c, carry):
        for b in range(NB):
            part = h[c, PAD + b * 128:PAD + b * 128 + 128, :]
            for f in range(F):
                end = jnp.broadcast_to(ends[pl.ds(row_of(c, f), 1), :], (128, 128))
                o[b, pl.ds(c * 128 * F + f, 128, stride=F), :] = (
                    y[c, f, PAD + b * 128:PAD + b * 128 + 128, :] + part * end).T
            copy_out(c, b).start()
        return carry

    lax.fori_loop(0, NB, turn_out, 0)
    for c in range(NB):
        for b in range(NB):
            copy_out(c, b).wait()


def solution(mesh):
    row_count = mesh.shape["row"]
    field_spec = P(("batch", "row"), "col", None)
    coef_spec = P(("batch", "row"), "col")

    def local_step(field, x_lower, x_diag, x_upper, y_lower, y_diag, y_upper):
        words = field.reshape(T, NB, 128, F).transpose(0, 1, 3, 2)
        plane = (NB, ROWS, 128)
        fields = (NB, F, ROWS, 128)
        peers = row_count - 1
        in_vmem = pl.BlockSpec(memory_space=pltpu.VMEM)
        in_hbm = pl.BlockSpec(memory_space=pl.ANY)
        dma = pltpu.SemaphoreType.DMA
        parts = pl.pallas_call(
            functools.partial(main_kernel, row_count),
            out_shape=[pltpu.VMEM(fields, F32), pltpu.VMEM(plane, F32), pltpu.VMEM((R, 128), F32)],
            in_specs=[in_hbm] * 7,
            out_specs=[in_vmem] * 3,
            scratch_shapes=[
                pltpu.VMEM((NB + 1, ROWS * F, 128), F32),
                pltpu.VMEM((3,) + plane, F32),
                pltpu.VMEM((2,) + plane, F32),
                pltpu.VMEM((3,) + plane, F32),
                pltpu.VMEM((3,) + plane, F32),
                pltpu.VMEM((2,) + plane, F32),
                pltpu.VMEM(fields, F32),
                pltpu.VMEM(fields, F32),
                pltpu.VMEM((2, R * 8, 128), F32),
                pltpu.VMEM((6 * R, 8, 128), F32),
                pltpu.VMEM((6 * R, 8, 128), F32),
                pltpu.VMEM((8, 11, R, 128), F32),
                pltpu.VMEM((8, 11, R, 128), F32),
                pltpu.VMEM((2, 16, 128), F32),
                pltpu.VMEM((5 * (row_count - 2) + 8, R, 128), F32),
                pltpu.VMEM(plane, F32),
                pltpu.VMEM((R, 8, 128), F32),
                pltpu.VMEM((2 * R, 128), F32),
                pltpu.VMEM((2, R * 8, 128), F32),
                pltpu.VMEM((4 * R, 128), F32),
                pltpu.VMEM((peers, 4 * R, 128), F32),
                pltpu.VMEM((2, R, 128), F32),
                pltpu.VMEM((2, peers, R, 128), F32),
                pltpu.VMEM((4 * R, 128), F32),
                pltpu.VMEM((4 * R, 128), F32),
                pltpu.VMEM((R, 128), F32),
                pltpu.VMEM((R, 128), F32),
                dma((3, NB)), dma((NB, NB)), dma((NB, 3)), dma, dma, dma((peers,)), dma((peers,)), dma((2, peers)), dma((2, peers)), dma((2,)), dma((2,)),
            ],
            compiler_params=pltpu.CompilerParams(
                collective_id=0, has_side_effects=True, vmem_limit_bytes=58 << 20),
        )(words, x_lower, x_diag, x_upper, y_lower, y_diag, y_upper)
        solved = pl.pallas_call(
            last_kernel,
            out_shape=jax.ShapeDtypeStruct((T, NB, F, 128), F32),
            in_specs=[in_vmem] * 3,
            out_specs=in_hbm,
            scratch_shapes=[pltpu.VMEM((NB, T * F, 128), F32), dma((NB, NB))],
            compiler_params=pltpu.CompilerParams(vmem_limit_bytes=16 << 20),
        )(*parts)
        return solved.transpose(0, 1, 3, 2).reshape(T, T, F)

    return jax.shard_map(local_step, mesh=mesh, in_specs=(field_spec,) + (coef_spec,) * 6,
                         out_specs=field_spec, check_vma=False)
```

```python
import functools

import jax
import jax.numpy as jnp
from jax import lax
from jax.experimental import pallas as pl
from jax.experimental.pallas import tpu as pltpu
from jax.sharding import PartitionSpec as P

MESH = pl.DeviceIdType.MESH
F32 = jnp.float32

T = 512
F = 4
C = 65
PAD = 8
ROWS = T + PAD
NB = T // 128
R = F * NB
UNROLL = 5

DIAG, LOW, UPP = 0, 1, 2
INV, NA, PR = 0, 1, 2
V, NC = 0, 1
A0, A1, A2, B0, B1, B2 = range(6)


H = R // 2
X_UNROLL = C


def chunk_rows(t):
    return pl.ds(t, 8, stride=C)


def row_of(b, f):
    if isinstance(b, int):
        return b // 2 * H + f * 2 + b % 2
    return lax.div(b, 2) * H + f * 2 + lax.rem(b, 2)


def beside(edge, side, b, f):
    return edge[side, pl.ds(pl.multiple_of(row_of(b, f) * 8, 8), 8), :]


def sweep(blocks, step, state, unroll=UNROLL):
    def steps(i, state):
        for n in range(unroll):
            state = step(blocks, i * unroll + n, state)
        return state
    return lax.fori_loop(0, C // unroll, steps, state)


def factor(k, kb, summ, scale):
    sub = lax.broadcasted_iota(jnp.int32, (8, 128), 0)
    zero = jnp.zeros((8, 128), F32)

    def step(blocks, t, state):
        out = []
        fresh = sub == jnp.where(t == PAD, 0, 8)
        for b in blocks:
            nc, v, pr, a1 = state[4 * b:4 * b + 4]
            rows = chunk_rows(t)
            low = k[LOW, b, rows, :]
            den = (1.0 + k[DIAG, b, rows, :]) + low * nc
            inv = 1.0 / den
            na = -(low * inv)
            nc = -(k[UPP, b, rows, :] * inv)
            v = na * v
            pr = jnp.where(fresh, 1.0, pr)
            k[INV, b, rows, :] = inv if scale == 1 else inv * scale
            k[NA, b, rows, :] = na
            k[PR, b, rows, :] = pr
            kb[NC, b, rows, :] = nc
            kb[V, b, rows, :] = v
            a1 = a1 + pr * v
            pr = pr * nc
            out += [nc, v, pr, a1]
        return tuple(out)

    state = (zero, zero + 1.0, jnp.where(sub == 0, 0.0, 1.0), zero) * NB
    state = sweep(range(NB), step, state)
    for b in range(NB):
        nc, v, pr, a1 = state[4 * b:4 * b + 4]
        for f in range(F):
            r = row_of(b, f)
            summ[A1 * R + r] = a1
            summ[A2 * R + r] = pr
            summ[B1 * R + r] = v
            summ[B2 * R + r] = nc


def of_chunk(summ, q, s, first=0, rows=R):
    return summ.reshape(6 * R * 8, 128)[pl.ds(q * R * 8 + first * 8 + s, rows, stride=8), :]


def join_coef(la1, la2, lb1, lb2, ra1, ra2, rb1, rb2):
    inv = 1.0 / (1.0 - ra1 * lb2)
    w = inv * ra1
    e1 = w * lb1
    e2 = inv * ra2
    m1 = lb1 + lb2 * e1
    m2 = lb2 * e2
    return (la1 + la2 * e1, la2 * e2, rb1 * m1, rb2 + rb1 * m2), (inv, w, lb2, la2, rb1), (e1, e2, m1, m2)


def join_rhs(part, la0, lb0, ra0, rb0):
    inv, w, lb2, la2, rb1 = part
    e0 = inv * ra0 + w * lb0
    m0 = lb0 + lb2 * e0
    return la0 + la2 * e0, rb0 + rb1 * m0, e0, m0


def reduce_coef(summ, co, send):
    def chunk(s):
        return tuple(of_chunk(summ, q, s) for q in (A1, A2, B1, B2))
    whole = chunk(0)
    for s in range(1, 8):
        whole, part, inner = join_coef(*whole, *chunk(s))
        for n, v in enumerate(part + inner):
            co[s - 1, n] = v
    for n, v in enumerate(whole):
        co[7, n] = v
        send[n * R:n * R + R, :] = v


def reduce_rhs(summ, co, first, rows, send):
    some = pl.ds(first, rows)
    a0, b0 = (of_chunk(summ, q, 0, first, rows) for q in (A0, B0))
    for s in range(1, 8):
        part = tuple(co[s - 1, n, some, :] for n in range(5))
        a0, b0, e0, m0 = join_rhs(part, a0, b0, *(of_chunk(summ, q, s, first, rows) for q in (A0, B0)))
        co[s - 1, 9, some, :] = e0
        co[s - 1, 10, some, :] = m0
    send[0:rows, :] = a0
    send[rows:2 * rows, :] = b0


def weigh(k, co, want_first, edge, weights):
    lam = (1.0 - want_first) + jnp.zeros((R, 128), F32)

    def at(s):
        return pl.ds(s, R, stride=8)

    for s in range(7, 0, -1):
        inv, w, lb2, la2, rb1 = (co[s - 1, n] for n in range(5))
        la2 = want_first * la2
        edge[1, at(s), :] = lam
        edge[0, at(s), :] = inv * (la2 + lam * (rb1 * lb2))
        lam = lam * (rb1 * (1.0 + lb2 * w)) + la2 * w
    edge[1, at(0), :] = lam
    edge[0, at(0), :] = want_first + jnp.zeros((R, 128), F32)
    parts = [(beside(edge, 0, b, 0), beside(edge, 1, b, 0)) for b in range(NB)]

    def step(blocks, n, state):
        rows = chunk_rows(C - 1 - n)
        out = []
        for b in blocks:
            first = k[PR, b, rows, :] + state[2 * b]
            last = state[2 * b + 1]
            na = k[NA, b, rows, :]
            weights[b, rows, :] = k[INV, b, rows, :] * (parts[b][0] * first + parts[b][1] * last)
            out += [na * first, na * last]
        return tuple(out)

    zero = jnp.zeros((8, 128), F32)
    return step, (zero, zero + 1.0) * NB


def spread(co, first, rows, before, after, edge, rhs=True):
    def at(s):
        return pl.ds(first * 8 + s, rows, stride=8)
    some = pl.ds(first, rows)
    nxt = after
    edge[1, at(7), :] = after
    edge[0, at(0), :] = before
    for s in range(7, 0, -1):
        e1, e2, m1, m2, e0, m0 = (co[s - 1, n, some, :] for n in range(5, 11))
        last = m1 * before + m2 * nxt
        nxt = e1 * before + e2 * nxt
        if rhs:
            last, nxt = m0 + last, e0 + nxt
        edge[0, at(s), :] = last
        edge[1, at(s - 1), :] = nxt


def forward(k, rhs_of, g, summ, blocks, unroll=UNROLL):
    zero = jnp.zeros((8, 128), F32)

    def step(blocks, t, state):
        out = []
        rows = chunk_rows(t)
        for j, b in enumerate(blocks):
            inv = k[INV, b, rows, :]
            na = k[NA, b, rows, :]
            pr = k[PR, b, rows, :]
            rhs = rhs_of(b, t)
            for f in range(F):
                last, first = state[2 * (j * F + f):2 * (j * F + f) + 2]
                last = inv * rhs[f] + na * last
                g[b, f, rows, :] = last
                out += [last, first + pr * last]
        return tuple(out)

    state = (zero,) * (2 * F * len(blocks))
    if unroll == C:
        for t in range(C):
            state = step(blocks, t, state)
    else:
        state = sweep(blocks, step, state, unroll)
    for j, b in enumerate(blocks):
        for f in range(F):
            summ[B0 * R + row_of(b, f)] = state[2 * (j * F + f)]
            summ[A0 * R + row_of(b, f)] = state[2 * (j * F + f) + 1]


def backward(kb, g, edge, put, turn):
    def start(b):
        return tuple(beside(edge, 1, b, f) for f in range(F))

    def stepper(b):
        near = [beside(edge, 0, b, f) for f in range(F)]

        def step(_, n, state):
            out = []
            rows = chunk_rows(C - 1 - n)
            v = kb[V, b, rows, :]
            nc = kb[NC, b, rows, :]
            for f in range(F):
                x = (g[b, f, rows, :] + v * near[f]) + nc * state[f]
                put(b, f, rows, x)
                out.append(x)
            return tuple(out)
        return step

    def alone(b, more=None, more_start=()):
        step = stepper(b)

        def step_all(blocks, n, state):
            state = step(blocks, n, state[:F]) + state[F:]
            return state if more is None else state[:F] + more(range(NB), n, state[F:])

        sweep(b, step_all, start(b) + more_start)

    def both(b, before):
        step = stepper(b)
        state = step(b, 0, start(b))
        for n in range(NB * F):
            turn(before, n)
            for m in range(4):
                state = step(b, 1 + 4 * n + m, state)

    def last(b):
        for n in range(NB * F):
            turn(b, n)

    return alone, both, last


def main_kernel(row_count, field, xl, xd, xu, yl, yd, yu, y, answer, ends,
                u, xk, xb, yn, yk, yb, r1, g, edge, sx, sy, cx, cy, pack, close, weights, dots, ends2, tilt,
                xcs, xcr, xrs, xrr, ycs, ycr, yrs, yrr,
                in_sem, field_sem, coef_sem, ps, pr, xcss, xcrs, xrss, xrrs, yss, yrsem):
    row = lax.axis_index("row")
    col = lax.axis_index("col")
    other = 1 - col
    lane = lax.broadcasted_iota(jnp.int32, (8, 128), 1)
    zero = jnp.zeros((8, 128), F32)
    src_block = (NB - 1) * other
    src_lane = 127 * other
    dst_lane = 127 * col

    def block(n):
        return n + col * (3 - 2 * n)

    def in_field(n):
        b = block(n)
        return [pltpu.make_async_copy(field.at[pl.ds(i * 128, 128), b],
                                      u.at[b, pl.ds((PAD + i * 128) * F, 128 * F)].reshape(128, F, 128), field_sem.at[n, i])
                for i in range(NB)]

    def in_coef(n):
        b = block(n)
        return [pltpu.make_async_copy(ref.at[:, pl.ds(pl.multiple_of(b * 128, 128), 128)], yn.at[i, b, pl.ds(PAD, T)], coef_sem.at[n, i])
                for i, ref in enumerate((yd, yl, yu))]

    in_x = [pltpu.make_async_copy(ref.at[:, pl.ds(b * 128, 128)], xk.at[n, b, pl.ds(PAD, T)], in_sem.at[n, b])
            for n, ref in enumerate((xd, xl, xu)) for b in range(NB)]

    def start(copies):
        for cp in copies:
            cp.start()

    def wait(copies):
        for cp in copies:
            cp.wait()

    start(in_field(3))

    barrier = pltpu.get_barrier_semaphore()
    for d in range(1, row_count):
        pl.semaphore_signal(barrier, inc=1, device_id={"row": lax.rem(row + d, row_count)}, device_id_type=MESH)
    pl.semaphore_signal(barrier, inc=1, device_id={"col": other}, device_id_type=MESH)

    for b in range(NB):
        for n in range(3):
            yn[n, b, 0:PAD, :] = zero
            xk[n, b, 0:PAD, :] = zero - 1.0 if n == LOW else zero
            yk[n, b, 0:PAD, :] = zero - 1.0 if n == LOW else zero
        for f in range(F):
            y[b, f, 0:PAD, :] = zero
    for b in range(NB):
        u[b, 0:PAD * F, :] = jnp.zeros((PAD * F, 128), F32)
    u[NB] = jnp.zeros((ROWS * F, 128), F32)

    def line_copies(send, recv, send_sem, recv_sem):
        return [pltpu.make_async_remote_copy(send, recv.at[d - 1], send_sem.at[d - 1], recv_sem.at[d - 1],
                                             device_id={"row": lax.rem(row + d, row_count)}, device_id_type=MESH)
                for d in range(1, row_count)]

    def to_line(*refs):
        copies = line_copies(*refs)
        for cp in copies:
            cp.start()
        return copies

    def to_pair(n, send, recv):
        cp = pltpu.make_async_remote_copy(send, recv, yss.at[n], yrsem.at[n], device_id={"col": other}, device_id_type=MESH)
        cp.start()
        return cp

    start(in_x)

    start(in_field(0) + in_field(1) + in_coef(0))
    wait(in_field(3))
    from_src = jnp.bitwise_and(lane - src_lane, 127)
    for h in range(2):
        acc = zero
        for p in range(128):
            w = PAD * F + 8 * (h * 128 + p)
            acc = jnp.where(from_src == p, pltpu.roll(u[src_block, w:w + 8, :], p, 1), acc)
        pack[0, h * 8:h * 8 + 8, :] = acc
    pl.semaphore_wait(barrier, row_count)
    column = pltpu.make_async_remote_copy(pack.at[0], pack.at[1], ps, pr, device_id={"col": other}, device_id_type=MESH)
    column.start()


    wait(in_x)
    start(in_field(2) + in_coef(1) + in_coef(2) + in_coef(3))
    factor(xk, xb, sx, 2.0)
    reduce_coef(sx, cx, xcs)
    coef_sends = to_line(xcs, xcr, xcss, xcrs)

    def stencil(b, t):
        rows = chunk_rows(t)
        cd = 1.0 - yn[DIAG, b, rows, :]
        cl = yn[LOW, b, rows, :]
        cu = yn[UPP, b, rows, :]
        left = lax.rem(b + NB, NB + 1)
        rhs = []
        for f in range(F):
            words = pl.ds(t * F + f, 8, stride=C * F)
            mid = u[b, words, :]
            prv = pltpu.roll(jnp.where(lane == 127, u[left, words, :], mid), 1, 1)
            nxt = pltpu.roll(jnp.where(lane == 0, u[b + 1, words, :], mid), 127, 1)
            v = (cd * mid - cl * prv) - cu * nxt
            r1[b, f, rows, :] = v
            rhs.append(v)
        return rhs

    halves = [col, other]

    def send_half(h):
        reduce_rhs(sx, cx, pl.multiple_of(halves[h] * H, 8), H, xrs.at[h])
        return to_line(xrs.at[h], xrr.at[h], xrss.at[h], xrrs.at[h])

    def eliminate(n, carry):
        wait(in_coef(n))

        @pl.when(n < 2)
        def _():
            wait(in_field(n + 1))

        @pl.when(n == 2)
        def _():
            send_half(0)

        @pl.when(n == 3)
        def _():
            column.wait()
            here = lane == dst_lane
            for i in range(2):
                got = pack[1, i * 8:i * 8 + 8, :]
                for p in range(128):
                    w = PAD * F + 8 * (i * 128 + p)
                    u[NB, w:w + 8, :] = jnp.where(here, pltpu.roll(got, (128 - p) % 128, 1), 0.0)

        forward(xk, stencil, g, sx, [block(n)], X_UNROLL)
        return carry

    wait(in_field(0))
    lax.fori_loop(0, NB, eliminate, 0)
    send_half(1)

    for b in range(NB):
        for c in range(NB):
            for n in range(3):
                yk[n, c, PAD + b * 128:PAD + b * 128 + 128, :] = yn[n, b, PAD + c * 128:PAD + c * 128 + 128, :].T
    factor(yk, yb, sy, 1)
    reduce_coef(sy, cy, ycs)
    y_coef = to_pair(0, ycs, ycr)
    weigh_step, weigh_start = weigh(yk, cy, jnp.where(col == 0, 0.0, 1.0), tilt, weights)
    dots[...] = jnp.zeros((R, 8, 128), F32)

    for cp in coef_sends:
        cp.wait()

    def coef_of(ref):
        return tuple(ref[q * R:q * R + R, :] for q in range(4))

    slots = range(row_count - 3, -1, -1)
    rest = coef_of(xcr.at[row_count - 2])
    known = []
    for n in slots:
        rest, part, _ = join_coef(*rest, *coef_of(xcr.at[n]))
        known += part
    p1, p2, q1, q2 = rest
    a1, a2, b1, b2 = (cx[7, n] for n in range(4))
    m12 = p1 * b1 + p2 * a1
    i11 = 1.0 / (1.0 - (p1 * b2 + p2 * a2))
    m21 = (q1 * b2 + q2 * a2) * i11
    i22 = 1.0 / ((1.0 - (q1 * b1 + q2 * a1)) - m21 * m12)
    for n, v in enumerate(known + [p1, p2, q1, q2, m12, m21, i11, i22]):
        close[n] = v

    def close_line(h):
        for cp in line_copies(xrs.at[h], xrr.at[h], xrss.at[h], xrrs.at[h]):
            cp.wait()
        first = pl.multiple_of(halves[h] * H, 8)
        known = [close[n, pl.ds(first, H), :] for n in range(5 * (row_count - 2) + 8)]

        def received(n):
            return xrr[h, n, 0:H, :], xrr[h, n, H:2 * H, :]

        p0, q0 = received(row_count - 2)
        for i, n in enumerate(slots):
            p0, q0, _, _ = join_rhs(known[5 * i:5 * i + 5], p0, q0, *received(n))
        p1, p2, q1, q2, m12, m21, i11, i22 = known[5 * (row_count - 2):]
        a0, b0 = xrs[h, 0:H, :], xrs[h, H:2 * H, :]
        s1 = (p0 + p1 * b0) + p2 * a0
        s2 = (q0 + q1 * b0) + q2 * a0
        before = i22 * (s2 + m21 * s1)
        spread(cx, first, H, before, i11 * (s1 + m12 * before), edge)

    def put_x(b, f, rows, x):
        r1[b, f, rows, :] = x - r1[b, f, rows, :]

    def turn_in(b, n):
        c, f = n // F, n % F
        rows = pl.ds(pl.multiple_of(PAD + b * 128, 8), 128)
        y[c, f, rows, :] = r1[b, f, PAD + c * 128:PAD + c * 128 + 128, :].T
        r = row_of(c, f)
        total = dots[r]
        for i in range(16):
            some = pl.ds(pl.multiple_of(PAD + b * 128 + i * 8, 8), 8)
            total = total + y[c, f, some, :] * weights[c, some, :]
        dots[r] = total

    alone, both, last = backward(xb, g, edge, put_x, turn_in)

    def solve(n, carry):
        @pl.when(n == 2)
        def _():
            close_line(1)

        both(block(n), block(n - 1))
        return carry

    close_line(0)
    alone(block(0), weigh_step, weigh_start)
    lax.fori_loop(1, NB, solve, 0)
    last(block(3))

    flat = dots.reshape(R * 8, 128)
    mine = flat[pl.ds(0, R, stride=8), :]
    for i in range(1, 8):
        mine = mine + flat[pl.ds(i, R, stride=8), :]
    yrs[...] = mine
    y_rhs = to_pair(1, yrs, yrr)

    def rhs_y(b, t):
        return [y[b, f, chunk_rows(t), :] for f in range(F)]

    forward(yk, rhs_y, g, sy, [0, 1])
    forward(yk, rhs_y, g, sy, [2, 3])
    reduce_rhs(sy, cy, 0, R, ends2)
    first = col == 0

    nothing = jnp.zeros((R, 128), F32)
    spread(cy, 0, R, nothing, nothing, edge)

    def put_y(b, f, rows, x):
        y[b, f, rows, :] = x

    alone, _, _ = backward(yb, g, edge, put_y, None)

    def solve_y(b, carry):
        alone(b)
        return carry

    lax.fori_loop(0, NB, solve_y, 0)
    one_left = jnp.where(first, 0.0, 1.0) + nothing
    spread(cy, 0, R, one_left, 1.0 - one_left, edge, False)
    near = [beside(edge, 0, b, 0) for b in range(NB)]

    def step_h(blocks, n, state):
        rows = chunk_rows(C - 1 - n)
        out = []
        for b in blocks:
            out.append(yb[V, b, rows, :] * near[b] + yb[NC, b, rows, :] * state[b])
            answer[b, rows, :] = out[b]
        return tuple(out)

    sweep(range(NB), step_h, tuple(beside(edge, 1, b, 0) for b in range(NB)))

    y_coef.wait()
    a1, b2 = cy[7, 0], cy[7, 3]
    c1, d2 = ycr[0:R, :], ycr[3 * R:4 * R, :]
    lb2 = jnp.where(first, b2, d2)
    ra1 = jnp.where(first, c1, a1)
    inv = 1.0 / (1.0 - lb2 * ra1)
    y_rhs.wait()
    mine = yrs[...]
    theirs = yrr[...]
    lb0 = jnp.where(first, mine, theirs)
    ra0 = jnp.where(first, theirs, mine)
    last_left = inv * (lb0 + lb2 * ra0)
    ends[...] = jnp.where(first, ra0 + ra1 * last_left, last_left)


def last_kernel(y, h, ends, out, o, out_sem):
    def copy_out(c, b):
        return pltpu.make_async_copy(o.at[b, pl.ds(pl.multiple_of(c * 128 * F, 8), 128 * F)].reshape(128, F, 128),
                                     out.at[pl.ds(c * 128, 128), b], out_sem.at[c, b])

    def turn_out(c, carry):
        for b in range(NB):
            part = h[c, PAD + b * 128:PAD + b * 128 + 128, :]
            for f in range(F):
                end = jnp.broadcast_to(ends[pl.ds(row_of(c, f), 1), :], (128, 128))
                o[b, pl.ds(c * 128 * F + f, 128, stride=F), :] = (
                    y[c, f, PAD + b * 128:PAD + b * 128 + 128, :] + part * end).T
            copy_out(c, b).start()
        return carry

    lax.fori_loop(0, NB, turn_out, 0)
    for c in range(NB):
        for b in range(NB):
            copy_out(c, b).wait()


def solution(mesh):
    row_count = mesh.shape["row"]
    field_spec = P(("batch", "row"), "col", None)
    coef_spec = P(("batch", "row"), "col")

    def local_step(field, x_lower, x_diag, x_upper, y_lower, y_diag, y_upper):
        words = field.reshape(T, NB, 128, F).transpose(0, 1, 3, 2)
        plane = (NB, ROWS, 128)
        fields = (NB, F, ROWS, 128)
        peers = row_count - 1
        in_vmem = pl.BlockSpec(memory_space=pltpu.VMEM)
        in_hbm = pl.BlockSpec(memory_space=pl.ANY)
        dma = pltpu.SemaphoreType.DMA
        parts = pl.pallas_call(
            functools.partial(main_kernel, row_count),
            out_shape=[pltpu.VMEM(fields, F32), pltpu.VMEM(plane, F32), pltpu.VMEM((R, 128), F32)],
            in_specs=[in_hbm] * 7,
            out_specs=[in_vmem] * 3,
            scratch_shapes=[
                pltpu.VMEM((NB + 1, ROWS * F, 128), F32),
                pltpu.VMEM((3,) + plane, F32),
                pltpu.VMEM((2,) + plane, F32),
                pltpu.VMEM((3,) + plane, F32),
                pltpu.VMEM((3,) + plane, F32),
                pltpu.VMEM((2,) + plane, F32),
                pltpu.VMEM(fields, F32),
                pltpu.VMEM(fields, F32),
                pltpu.VMEM((2, R * 8, 128), F32),
                pltpu.VMEM((6 * R, 8, 128), F32),
                pltpu.VMEM((6 * R, 8, 128), F32),
                pltpu.VMEM((8, 11, R, 128), F32),
                pltpu.VMEM((8, 11, R, 128), F32),
                pltpu.VMEM((2, 16, 128), F32),
                pltpu.VMEM((5 * (row_count - 2) + 8, R, 128), F32),
                pltpu.VMEM(plane, F32),
                pltpu.VMEM((R, 8, 128), F32),
                pltpu.VMEM((2 * R, 128), F32),
                pltpu.VMEM((2, R * 8, 128), F32),
                pltpu.VMEM((4 * R, 128), F32),
                pltpu.VMEM((peers, 4 * R, 128), F32),
                pltpu.VMEM((2, R, 128), F32),
                pltpu.VMEM((2, peers, R, 128), F32),
                pltpu.VMEM((4 * R, 128), F32),
                pltpu.VMEM((4 * R, 128), F32),
                pltpu.VMEM((R, 128), F32),
                pltpu.VMEM((R, 128), F32),
                dma((3, NB)), dma((NB, NB)), dma((NB, 3)), dma, dma, dma((peers,)), dma((peers,)), dma((2, peers)), dma((2, peers)), dma((2,)), dma((2,)),
            ],
            compiler_params=pltpu.CompilerParams(
                collective_id=0, has_side_effects=True, vmem_limit_bytes=58 << 20),
        )(words, x_lower, x_diag, x_upper, y_lower, y_diag, y_upper)
        solved = pl.pallas_call(
            last_kernel,
            out_shape=jax.ShapeDtypeStruct((T, NB, F, 128), F32),
            in_specs=[in_vmem] * 3,
            out_specs=in_hbm,
            scratch_shapes=[pltpu.VMEM((NB, T * F, 128), F32), dma((NB, NB))],
            compiler_params=pltpu.CompilerParams(vmem_limit_bytes=16 << 20),
        )(*parts)
        return solved.transpose(0, 1, 3, 2).reshape(T, T, F)

    return jax.shard_map(local_step, mesh=mesh, in_specs=(field_spec,) + (coef_spec,) * 6,
                         out_specs=field_spec, check_vma=False)
```

```python
import functools

import jax
import jax.numpy as jnp
from jax import lax
from jax.experimental import pallas as pl
from jax.experimental.pallas import tpu as pltpu
from jax.sharding import PartitionSpec as P

MESH = pl.DeviceIdType.MESH
F32 = jnp.float32

T = 512
F = 4
C = 65
PAD = 8
ROWS = T + PAD
NB = T // 128
R = F * NB
UNROLL = 5

DIAG, LOW, UPP = 0, 1, 2
INV, NA, PR = 0, 1, 2
V, NC = 0, 1
A0, A1, A2, B0, B1, B2 = range(6)


H = R // 2
X_UNROLL = C


def chunk_rows(t):
    return pl.ds(t, 8, stride=C)


def row_of(b, f):
    if isinstance(b, int):
        return b // 2 * H + f * 2 + b % 2
    return lax.div(b, 2) * H + f * 2 + lax.rem(b, 2)


def beside(edge, side, b, f):
    return edge[side, pl.ds(pl.multiple_of(row_of(b, f) * 8, 8), 8), :]


def sweep(blocks, step, state, unroll=UNROLL):
    def steps(i, state):
        for n in range(unroll):
            state = step(blocks, i * unroll + n, state)
        return state
    return lax.fori_loop(0, C // unroll, steps, state)


def factor(k, kb, summ, scale):
    sub = lax.broadcasted_iota(jnp.int32, (8, 128), 0)
    zero = jnp.zeros((8, 128), F32)

    def step(blocks, t, state):
        out = []
        fresh = sub == jnp.where(t == PAD, 0, 8)
        for b in blocks:
            nc, v, pr, a1 = state[4 * b:4 * b + 4]
            rows = chunk_rows(t)
            low = k[LOW, b, rows, :]
            den = (1.0 + k[DIAG, b, rows, :]) + low * nc
            inv = 1.0 / den
            na = -(low * inv)
            nc = -(k[UPP, b, rows, :] * inv)
            v = na * v
            pr = jnp.where(fresh, 1.0, pr)
            k[INV, b, rows, :] = inv if scale == 1 else inv * scale
            k[NA, b, rows, :] = na
            k[PR, b, rows, :] = pr
            kb[NC, b, rows, :] = nc
            kb[V, b, rows, :] = v
            a1 = a1 + pr * v
            pr = pr * nc
            out += [nc, v, pr, a1]
        return tuple(out)

    state = (zero, zero + 1.0, jnp.where(sub == 0, 0.0, 1.0), zero) * NB
    state = sweep(range(NB), step, state)
    for b in range(NB):
        nc, v, pr, a1 = state[4 * b:4 * b + 4]
        for f in range(F):
            r = row_of(b, f)
            summ[A1 * R + r] = a1
            summ[A2 * R + r] = pr
            summ[B1 * R + r] = v
            summ[B2 * R + r] = nc


def of_chunk(summ, q, s, first=0, rows=R):
    return summ.reshape(6 * R * 8, 128)[pl.ds(q * R * 8 + first * 8 + s, rows, stride=8), :]


def join_coef(la1, la2, lb1, lb2, ra1, ra2, rb1, rb2):
    inv = 1.0 / (1.0 - ra1 * lb2)
    w = inv * ra1
    e1 = w * lb1
    e2 = inv * ra2
    m1 = lb1 + lb2 * e1
    m2 = lb2 * e2
    return (la1 + la2 * e1, la2 * e2, rb1 * m1, rb2 + rb1 * m2), (inv, w, lb2, la2, rb1), (e1, e2, m1, m2)


def join_rhs(part, la0, lb0, ra0, rb0):
    inv, w, lb2, la2, rb1 = part
    e0 = inv * ra0 + w * lb0
    m0 = lb0 + lb2 * e0
    return la0 + la2 * e0, rb0 + rb1 * m0, e0, m0


def reduce_coef(summ, co, send):
    def chunk(s):
        return tuple(of_chunk(summ, q, s) for q in (A1, A2, B1, B2))
    whole = chunk(0)
    for s in range(1, 8):
        whole, part, inner = join_coef(*whole, *chunk(s))
        for n, v in enumerate(part + inner):
            co[s - 1, n] = v
    for n, v in enumerate(whole):
        co[7, n] = v
        send[n * R:n * R + R, :] = v


def reduce_rhs(summ, co, first, rows, send):
    some = pl.ds(first, rows)
    a0, b0 = (of_chunk(summ, q, 0, first, rows) for q in (A0, B0))
    for s in range(1, 8):
        part = tuple(co[s - 1, n, some, :] for n in range(5))
        a0, b0, e0, m0 = join_rhs(part, a0, b0, *(of_chunk(summ, q, s, first, rows) for q in (A0, B0)))
        co[s - 1, 9, some, :] = e0
        co[s - 1, 10, some, :] = m0
    send[0:rows, :] = a0
    send[rows:2 * rows, :] = b0


def weigh(k, co, want_first, edge, weights):
    lam = (1.0 - want_first) + jnp.zeros((R, 128), F32)

    def at(s):
        return pl.ds(s, R, stride=8)

    for s in range(7, 0, -1):
        inv, w, lb2, la2, rb1 = (co[s - 1, n] for n in range(5))
        la2 = want_first * la2
        edge[1, at(s), :] = lam
        edge[0, at(s), :] = inv * (la2 + lam * (rb1 * lb2))
        lam = lam * (rb1 * (1.0 + lb2 * w)) + la2 * w
    edge[1, at(0), :] = lam
    edge[0, at(0), :] = want_first + jnp.zeros((R, 128), F32)
    parts = [(beside(edge, 0, b, 0), beside(edge, 1, b, 0)) for b in range(NB)]

    def step(blocks, n, state):
        rows = chunk_rows(C - 1 - n)
        out = []
        for b in blocks:
            first = k[PR, b, rows, :] + state[2 * b]
            last = state[2 * b + 1]
            na = k[NA, b, rows, :]
            weights[b, rows, :] = k[INV, b, rows, :] * (parts[b][0] * first + parts[b][1] * last)
            out += [na * first, na * last]
        return tuple(out)

    zero = jnp.zeros((8, 128), F32)
    return step, (zero, zero + 1.0) * NB


def spread(co, first, rows, before, after, edge, rhs=True):
    def at(s):
        return pl.ds(first * 8 + s, rows, stride=8)
    some = pl.ds(first, rows)
    nxt = after
    edge[1, at(7), :] = after
    edge[0, at(0), :] = before
    for s in range(7, 0, -1):
        e1, e2, m1, m2, e0, m0 = (co[s - 1, n, some, :] for n in range(5, 11))
        last = m1 * before + m2 * nxt
        nxt = e1 * before + e2 * nxt
        if rhs:
            last, nxt = m0 + last, e0 + nxt
        edge[0, at(s), :] = last
        edge[1, at(s - 1), :] = nxt


def forward(k, rhs_of, g, summ, blocks, unroll=UNROLL):
    zero = jnp.zeros((8, 128), F32)

    def step(blocks, t, state):
        out = []
        rows = chunk_rows(t)
        for j, b in enumerate(blocks):
            inv = k[INV, b, rows, :]
            na = k[NA, b, rows, :]
            pr = k[PR, b, rows, :]
            rhs = rhs_of(b, t)
            for f in range(F):
                last, first = state[2 * (j * F + f):2 * (j * F + f) + 2]
                last = inv * rhs[f] + na * last
                g[b, f, rows, :] = last
                out += [last, first + pr * last]
        return tuple(out)

    state = (zero,) * (2 * F * len(blocks))
    if unroll == C:
        for t in range(C):
            state = step(blocks, t, state)
    else:
        state = sweep(blocks, step, state, unroll)
    for j, b in enumerate(blocks):
        for f in range(F):
            summ[B0 * R + row_of(b, f)] = state[2 * (j * F + f)]
            summ[A0 * R + row_of(b, f)] = state[2 * (j * F + f) + 1]


def backward(kb, g, edge, put, turn):
    def start(b):
        return tuple(beside(edge, 1, b, f) for f in range(F))

    def stepper(b):
        near = [beside(edge, 0, b, f) for f in range(F)]

        def step(_, n, state):
            out = []
            rows = chunk_rows(C - 1 - n)
            v = kb[V, b, rows, :]
            nc = kb[NC, b, rows, :]
            for f in range(F):
                x = (g[b, f, rows, :] + v * near[f]) + nc * state[f]
                put(b, f, rows, x)
                out.append(x)
            return tuple(out)
        return step

    def alone(b, more=None, more_start=()):
        step = stepper(b)

        def step_all(blocks, n, state):
            state = step(blocks, n, state[:F]) + state[F:]
            return state if more is None else state[:F] + more(range(NB), n, state[F:])

        sweep(b, step_all, start(b) + more_start)

    def both(b, before):
        step = stepper(b)
        state = step(b, 0, start(b))
        for n in range(NB * F):
            turn(before, n)
            for m in range(4):
                state = step(b, 1 + 4 * n + m, state)

    def last(b):
        for n in range(NB * F):
            turn(b, n)

    return alone, both, last


def main_kernel(row_count, field, xl, xd, xu, yl, yd, yu, y, answer, ends,
                u, xk, xb, yn, yk, yb, r1, g, edge, sx, sy, cx, cy, pack, close, weights, dots, ends2, tilt,
                xcs, xcr, xrs, xrr, ycs, ycr, yrs, yrr,
                in_sem, field_sem, coef_sem, ps, pr, xcss, xcrs, xrss, xrrs, yss, yrsem):
    row = lax.axis_index("row")
    col = lax.axis_index("col")
    other = 1 - col
    lane = lax.broadcasted_iota(jnp.int32, (8, 128), 1)
    zero = jnp.zeros((8, 128), F32)
    src_block = (NB - 1) * other
    src_lane = 127 * other
    dst_lane = 127 * col

    def block(n):
        return n + col * (3 - 2 * n)

    def in_field(n):
        b = block(n)
        return [pltpu.make_async_copy(field.at[pl.ds(i * 128, 128), b],
                                      u.at[b, pl.ds((PAD + i * 128) * F, 128 * F)].reshape(128, F, 128), field_sem.at[n, i])
                for i in range(NB)]

    def in_coef(n):
        b = block(n)
        return [pltpu.make_async_copy(ref.at[:, pl.ds(pl.multiple_of(b * 128, 128), 128)], yn.at[i, b, pl.ds(PAD, T)], coef_sem.at[n, i])
                for i, ref in enumerate((yd, yl, yu))]

    in_x = [pltpu.make_async_copy(ref.at[:, pl.ds(b * 128, 128)], xk.at[n, b, pl.ds(PAD, T)], in_sem.at[n, b])
            for n, ref in enumerate((xd, xl, xu)) for b in range(NB)]

    def start(copies):
        for cp in copies:
            cp.start()

    def wait(copies):
        for cp in copies:
            cp.wait()

    start(in_field(3))

    barrier = pltpu.get_barrier_semaphore()
    for d in range(1, row_count):
        pl.semaphore_signal(barrier, inc=1, device_id={"row": lax.rem(row + d, row_count)}, device_id_type=MESH)
    pl.semaphore_signal(barrier, inc=1, device_id={"col": other}, device_id_type=MESH)

    for b in range(NB):
        for n in range(3):
            yn[n, b, 0:PAD, :] = zero
            xk[n, b, 0:PAD, :] = zero - 1.0 if n == LOW else zero
            yk[n, b, 0:PAD, :] = zero - 1.0 if n == LOW else zero
        for f in range(F):
            y[b, f, 0:PAD, :] = zero
    for b in range(NB):
        u[b, 0:PAD * F, :] = jnp.zeros((PAD * F, 128), F32)
    u[NB] = jnp.zeros((ROWS * F, 128), F32)

    def line_copies(send, recv, send_sem, recv_sem):
        return [pltpu.make_async_remote_copy(send, recv.at[d - 1], send_sem.at[d - 1], recv_sem.at[d - 1],
                                             device_id={"row": lax.rem(row + d, row_count)}, device_id_type=MESH)
                for d in range(1, row_count)]

    def to_line(*refs):
        copies = line_copies(*refs)
        for cp in copies:
            cp.start()
        return copies

    def to_pair(n, send, recv):
        cp = pltpu.make_async_remote_copy(send, recv, yss.at[n], yrsem.at[n], device_id={"col": other}, device_id_type=MESH)
        cp.start()
        return cp

    start(in_x)

    wait(in_field(3))
    start(in_field(0) + in_field(1) + in_coef(0))
    from_src = jnp.bitwise_and(lane - src_lane, 127)
    for h in range(2):
        acc = zero
        for p in range(128):
            w = PAD * F + 8 * (h * 128 + p)
            acc = jnp.where(from_src == p, pltpu.roll(u[src_block, w:w + 8, :], p, 1), acc)
        pack[0, h * 8:h * 8 + 8, :] = acc
    pl.semaphore_wait(barrier, row_count)
    column = pltpu.make_async_remote_copy(pack.at[0], pack.at[1], ps, pr, device_id={"col": other}, device_id_type=MESH)
    column.start()


    wait(in_x)
    start(in_field(2) + in_coef(1) + in_coef(2) + in_coef(3))
    factor(xk, xb, sx, 2.0)
    reduce_coef(sx, cx, xcs)
    coef_sends = to_line(xcs, xcr, xcss, xcrs)

    def stencil(b, t):
        rows = chunk_rows(t)
        cd = 1.0 - yn[DIAG, b, rows, :]
        cl = yn[LOW, b, rows, :]
        cu = yn[UPP, b, rows, :]
        left = lax.rem(b + NB, NB + 1)
        rhs = []
        for f in range(F):
            words = pl.ds(t * F + f, 8, stride=C * F)
            mid = u[b, words, :]
            prv = pltpu.roll(jnp.where(lane == 127, u[left, words, :], mid), 1, 1)
            nxt = pltpu.roll(jnp.where(lane == 0, u[b + 1, words, :], mid), 127, 1)
            v = (cd * mid - cl * prv) - cu * nxt
            r1[b, f, rows, :] = v
            rhs.append(v)
        return rhs

    halves = [col, other]

    def send_half(h):
        reduce_rhs(sx, cx, pl.multiple_of(halves[h] * H, 8), H, xrs.at[h])
        return to_line(xrs.at[h], xrr.at[h], xrss.at[h], xrrs.at[h])

    def eliminate(n, carry):
        wait(in_coef(n))

        @pl.when(n < 2)
        def _():
            wait(in_field(n + 1))

        @pl.when(n == 2)
        def _():
            send_half(0)

        @pl.when(n == 3)
        def _():
            column.wait()
            here = lane == dst_lane
            for i in range(2):
                got = pack[1, i * 8:i * 8 + 8, :]
                for p in range(128):
                    w = PAD * F + 8 * (i * 128 + p)
                    u[NB, w:w + 8, :] = jnp.where(here, pltpu.roll(got, (128 - p) % 128, 1), 0.0)

        forward(xk, stencil, g, sx, [block(n)], X_UNROLL)
        return carry

    wait(in_field(0))
    lax.fori_loop(0, NB, eliminate, 0)
    send_half(1)

    for b in range(NB):
        for c in range(NB):
            for n in range(3):
                yk[n, c, PAD + b * 128:PAD + b * 128 + 128, :] = yn[n, b, PAD + c * 128:PAD + c * 128 + 128, :].T
    factor(yk, yb, sy, 1)
    reduce_coef(sy, cy, ycs)
    y_coef = to_pair(0, ycs, ycr)
    weigh_step, weigh_start = weigh(yk, cy, jnp.where(col == 0, 0.0, 1.0), tilt, weights)
    dots[...] = jnp.zeros((R, 8, 128), F32)

    for cp in coef_sends:
        cp.wait()

    def coef_of(ref):
        return tuple(ref[q * R:q * R + R, :] for q in range(4))

    slots = range(row_count - 3, -1, -1)
    rest = coef_of(xcr.at[row_count - 2])
    known = []
    for n in slots:
        rest, part, _ = join_coef(*rest, *coef_of(xcr.at[n]))
        known += part
    p1, p2, q1, q2 = rest
    a1, a2, b1, b2 = (cx[7, n] for n in range(4))
    m12 = p1 * b1 + p2 * a1
    i11 = 1.0 / (1.0 - (p1 * b2 + p2 * a2))
    m21 = (q1 * b2 + q2 * a2) * i11
    i22 = 1.0 / ((1.0 - (q1 * b1 + q2 * a1)) - m21 * m12)
    for n, v in enumerate(known + [p1, p2, q1, q2, m12, m21, i11, i22]):
        close[n] = v

    def close_line(h):
        for cp in line_copies(xrs.at[h], xrr.at[h], xrss.at[h], xrrs.at[h]):
            cp.wait()
        first = pl.multiple_of(halves[h] * H, 8)
        known = [close[n, pl.ds(first, H), :] for n in range(5 * (row_count - 2) + 8)]

        def received(n):
            return xrr[h, n, 0:H, :], xrr[h, n, H:2 * H, :]

        p0, q0 = received(row_count - 2)
        for i, n in enumerate(slots):
            p0, q0, _, _ = join_rhs(known[5 * i:5 * i + 5], p0, q0, *received(n))
        p1, p2, q1, q2, m12, m21, i11, i22 = known[5 * (row_count - 2):]
        a0, b0 = xrs[h, 0:H, :], xrs[h, H:2 * H, :]
        s1 = (p0 + p1 * b0) + p2 * a0
        s2 = (q0 + q1 * b0) + q2 * a0
        before = i22 * (s2 + m21 * s1)
        spread(cx, first, H, before, i11 * (s1 + m12 * before), edge)

    def put_x(b, f, rows, x):
        r1[b, f, rows, :] = x - r1[b, f, rows, :]

    def turn_in(b, n):
        c, f = n // F, n % F
        rows = pl.ds(pl.multiple_of(PAD + b * 128, 8), 128)
        y[c, f, rows, :] = r1[b, f, PAD + c * 128:PAD + c * 128 + 128, :].T
        r = row_of(c, f)
        total = dots[r]
        for i in range(16):
            some = pl.ds(pl.multiple_of(PAD + b * 128 + i * 8, 8), 8)
            total = total + y[c, f, some, :] * weights[c, some, :]
        dots[r] = total

    alone, both, last = backward(xb, g, edge, put_x, turn_in)

    def solve(n, carry):
        @pl.when(n == 2)
        def _():
            close_line(1)

        both(block(n), block(n - 1))
        return carry

    close_line(0)
    alone(block(0), weigh_step, weigh_start)
    lax.fori_loop(1, NB, solve, 0)
    last(block(3))

    flat = dots.reshape(R * 8, 128)
    mine = flat[pl.ds(0, R, stride=8), :]
    for i in range(1, 8):
        mine = mine + flat[pl.ds(i, R, stride=8), :]
    yrs[...] = mine
    y_rhs = to_pair(1, yrs, yrr)

    def rhs_y(b, t):
        return [y[b, f, chunk_rows(t), :] for f in range(F)]

    forward(yk, rhs_y, g, sy, [0, 1])
    forward(yk, rhs_y, g, sy, [2, 3])
    reduce_rhs(sy, cy, 0, R, ends2)
    first = col == 0

    nothing = jnp.zeros((R, 128), F32)
    spread(cy, 0, R, nothing, nothing, edge)

    def put_y(b, f, rows, x):
        y[b, f, rows, :] = x

    alone, _, _ = backward(yb, g, edge, put_y, None)

    def solve_y(b, carry):
        alone(b)
        return carry

    lax.fori_loop(0, NB, solve_y, 0)
    one_left = jnp.where(first, 0.0, 1.0) + nothing
    spread(cy, 0, R, one_left, 1.0 - one_left, edge, False)
    near = [beside(edge, 0, b, 0) for b in range(NB)]

    def step_h(blocks, n, state):
        rows = chunk_rows(C - 1 - n)
        out = []
        for b in blocks:
            out.append(yb[V, b, rows, :] * near[b] + yb[NC, b, rows, :] * state[b])
            answer[b, rows, :] = out[b]
        return tuple(out)

    sweep(range(NB), step_h, tuple(beside(edge, 1, b, 0) for b in range(NB)))

    y_coef.wait()
    a1, b2 = cy[7, 0], cy[7, 3]
    c1, d2 = ycr[0:R, :], ycr[3 * R:4 * R, :]
    lb2 = jnp.where(first, b2, d2)
    ra1 = jnp.where(first, c1, a1)
    inv = 1.0 / (1.0 - lb2 * ra1)
    y_rhs.wait()
    mine = yrs[...]
    theirs = yrr[...]
    lb0 = jnp.where(first, mine, theirs)
    ra0 = jnp.where(first, theirs, mine)
    last_left = inv * (lb0 + lb2 * ra0)
    ends[...] = jnp.where(first, ra0 + ra1 * last_left, last_left)


def last_kernel(y, h, ends, out, o, out_sem):
    def copy_out(c, b):
        return pltpu.make_async_copy(o.at[b, pl.ds(pl.multiple_of(c * 128 * F, 8), 128 * F)].reshape(128, F, 128),
                                     out.at[pl.ds(c * 128, 128), b], out_sem.at[c, b])

    def turn_out(c, carry):
        for b in range(NB):
            part = h[c, PAD + b * 128:PAD + b * 128 + 128, :]
            for f in range(F):
                end = jnp.broadcast_to(ends[pl.ds(row_of(c, f), 1), :], (128, 128))
                o[b, pl.ds(c * 128 * F + f, 128, stride=F), :] = (
                    y[c, f, PAD + b * 128:PAD + b * 128 + 128, :] + part * end).T
            copy_out(c, b).start()
        return carry

    lax.fori_loop(0, NB, turn_out, 0)
    for c in range(NB):
        for b in range(NB):
            copy_out(c, b).wait()


def solution(mesh):
    row_count = mesh.shape["row"]
    field_spec = P(("batch", "row"), "col", None)
    coef_spec = P(("batch", "row"), "col")

    def local_step(field, x_lower, x_diag, x_upper, y_lower, y_diag, y_upper):
        words = field.reshape(T, NB, 128, F).transpose(0, 1, 3, 2)
        plane = (NB, ROWS, 128)
        fields = (NB, F, ROWS, 128)
        peers = row_count - 1
        in_vmem = pl.BlockSpec(memory_space=pltpu.VMEM)
        in_hbm = pl.BlockSpec(memory_space=pl.ANY)
        dma = pltpu.SemaphoreType.DMA
        parts = pl.pallas_call(
            functools.partial(main_kernel, row_count),
            out_shape=[pltpu.VMEM(fields, F32), pltpu.VMEM(plane, F32), pltpu.VMEM((R, 128), F32)],
            in_specs=[in_hbm] * 7,
            out_specs=[in_vmem] * 3,
            scratch_shapes=[
                pltpu.VMEM((NB + 1, ROWS * F, 128), F32),
                pltpu.VMEM((3,) + plane, F32),
                pltpu.VMEM((2,) + plane, F32),
                pltpu.VMEM((3,) + plane, F32),
                pltpu.VMEM((3,) + plane, F32),
                pltpu.VMEM((2,) + plane, F32),
                pltpu.VMEM(fields, F32),
                pltpu.VMEM(fields, F32),
                pltpu.VMEM((2, R * 8, 128), F32),
                pltpu.VMEM((6 * R, 8, 128), F32),
                pltpu.VMEM((6 * R, 8, 128), F32),
                pltpu.VMEM((8, 11, R, 128), F32),
                pltpu.VMEM((8, 11, R, 128), F32),
                pltpu.VMEM((2, 16, 128), F32),
                pltpu.VMEM((5 * (row_count - 2) + 8, R, 128), F32),
                pltpu.VMEM(plane, F32),
                pltpu.VMEM((R, 8, 128), F32),
                pltpu.VMEM((2 * R, 128), F32),
                pltpu.VMEM((2, R * 8, 128), F32),
                pltpu.VMEM((4 * R, 128), F32),
                pltpu.VMEM((peers, 4 * R, 128), F32),
                pltpu.VMEM((2, R, 128), F32),
                pltpu.VMEM((2, peers, R, 128), F32),
                pltpu.VMEM((4 * R, 128), F32),
                pltpu.VMEM((4 * R, 128), F32),
                pltpu.VMEM((R, 128), F32),
                pltpu.VMEM((R, 128), F32),
                dma((3, NB)), dma((NB, NB)), dma((NB, 3)), dma, dma, dma((peers,)), dma((peers,)), dma((2, peers)), dma((2, peers)), dma((2,)), dma((2,)),
            ],
            compiler_params=pltpu.CompilerParams(
                collective_id=0, has_side_effects=True, vmem_limit_bytes=58 << 20),
        )(words, x_lower, x_diag, x_upper, y_lower, y_diag, y_upper)
        solved = pl.pallas_call(
            last_kernel,
            out_shape=jax.ShapeDtypeStruct((T, NB, F, 128), F32),
            in_specs=[in_vmem] * 3,
            out_specs=in_hbm,
            scratch_shapes=[pltpu.VMEM((NB, T * F, 128), F32), dma((NB, NB))],
            compiler_params=pltpu.CompilerParams(vmem_limit_bytes=16 << 20),
        )(*parts)
        return solved.transpose(0, 1, 3, 2).reshape(T, T, F)

    return jax.shard_map(local_step, mesh=mesh, in_specs=(field_spec,) + (coef_spec,) * 6,
                         out_specs=field_spec, check_vma=False)
```

```python
import functools

import jax
import jax.numpy as jnp
from jax import lax
from jax.experimental import pallas as pl
from jax.experimental.pallas import tpu as pltpu
from jax.sharding import PartitionSpec as P

MESH = pl.DeviceIdType.MESH
F32 = jnp.float32

T = 512
F = 4
C = 65
PAD = 8
ROWS = T + PAD
NB = T // 128
R = F * NB
UNROLL = 5

DIAG, LOW, UPP = 0, 1, 2
INV, NA, PR = 0, 1, 2
V, NC = 0, 1
A0, A1, A2, B0, B1, B2 = range(6)


H = R // 2
X_UNROLL = C


def chunk_rows(t):
    return pl.ds(t, 8, stride=C)


def row_of(b, f):
    if isinstance(b, int):
        return b // 2 * H + f * 2 + b % 2
    return lax.div(b, 2) * H + f * 2 + lax.rem(b, 2)


def beside(edge, side, b, f):
    return edge[side, pl.ds(pl.multiple_of(row_of(b, f) * 8, 8), 8), :]


def sweep(blocks, step, state, unroll=UNROLL):
    def steps(i, state):
        for n in range(unroll):
            state = step(blocks, i * unroll + n, state)
        return state
    return lax.fori_loop(0, C // unroll, steps, state)


def factor(k, kb, summ, scale):
    sub = lax.broadcasted_iota(jnp.int32, (8, 128), 0)
    zero = jnp.zeros((8, 128), F32)

    def step(blocks, t, state):
        out = []
        fresh = sub == jnp.where(t == PAD, 0, 8)
        for b in blocks:
            nc, v, pr, a1 = state[4 * b:4 * b + 4]
            rows = chunk_rows(t)
            low = k[LOW, b, rows, :]
            den = (1.0 + k[DIAG, b, rows, :]) + low * nc
            inv = 1.0 / den
            na = -(low * inv)
            nc = -(k[UPP, b, rows, :] * inv)
            v = na * v
            pr = jnp.where(fresh, 1.0, pr)
            k[INV, b, rows, :] = inv if scale == 1 else inv * scale
            k[NA, b, rows, :] = na
            k[PR, b, rows, :] = pr
            kb[NC, b, rows, :] = nc
            kb[V, b, rows, :] = v
            a1 = a1 + pr * v
            pr = pr * nc
            out += [nc, v, pr, a1]
        return tuple(out)

    state = (zero, zero + 1.0, jnp.where(sub == 0, 0.0, 1.0), zero) * NB
    state = sweep(range(NB), step, state)
    for b in range(NB):
        nc, v, pr, a1 = state[4 * b:4 * b + 4]
        for f in range(F):
            r = row_of(b, f)
            summ[A1 * R + r] = a1
            summ[A2 * R + r] = pr
            summ[B1 * R + r] = v
            summ[B2 * R + r] = nc


def of_chunk(summ, q, s, first=0, rows=R):
    return summ.reshape(6 * R * 8, 128)[pl.ds(q * R * 8 + first * 8 + s, rows, stride=8), :]


def join_coef(la1, la2, lb1, lb2, ra1, ra2, rb1, rb2):
    inv = 1.0 / (1.0 - ra1 * lb2)
    w = inv * ra1
    e1 = w * lb1
    e2 = inv * ra2
    m1 = lb1 + lb2 * e1
    m2 = lb2 * e2
    return (la1 + la2 * e1, la2 * e2, rb1 * m1, rb2 + rb1 * m2), (inv, w, lb2, la2, rb1), (e1, e2, m1, m2)


def join_rhs(part, la0, lb0, ra0, rb0):
    inv, w, lb2, la2, rb1 = part
    e0 = inv * ra0 + w * lb0
    m0 = lb0 + lb2 * e0
    return la0 + la2 * e0, rb0 + rb1 * m0, e0, m0


def reduce_coef(summ, co, send):
    def chunk(s):
        return tuple(of_chunk(summ, q, s) for q in (A1, A2, B1, B2))
    whole = chunk(0)
    for s in range(1, 8):
        whole, part, inner = join_coef(*whole, *chunk(s))
        for n, v in enumerate(part + inner):
            co[s - 1, n] = v
    for n, v in enumerate(whole):
        co[7, n] = v
        send[n * R:n * R + R, :] = v


def reduce_rhs(summ, co, first, rows, send):
    some = pl.ds(first, rows)
    a0, b0 = (of_chunk(summ, q, 0, first, rows) for q in (A0, B0))
    for s in range(1, 8):
        part = tuple(co[s - 1, n, some, :] for n in range(5))
        a0, b0, e0, m0 = join_rhs(part, a0, b0, *(of_chunk(summ, q, s, first, rows) for q in (A0, B0)))
        co[s - 1, 9, some, :] = e0
        co[s - 1, 10, some, :] = m0
    send[0:rows, :] = a0
    send[rows:2 * rows, :] = b0


def weigh(k, co, want_first, edge, weights):
    lam = (1.0 - want_first) + jnp.zeros((R, 128), F32)

    def at(s):
        return pl.ds(s, R, stride=8)

    for s in range(7, 0, -1):
        inv, w, lb2, la2, rb1 = (co[s - 1, n] for n in range(5))
        la2 = want_first * la2
        edge[1, at(s), :] = lam
        edge[0, at(s), :] = inv * (la2 + lam * (rb1 * lb2))
        lam = lam * (rb1 * (1.0 + lb2 * w)) + la2 * w
    edge[1, at(0), :] = lam
    edge[0, at(0), :] = want_first + jnp.zeros((R, 128), F32)
    parts = [(beside(edge, 0, b, 0), beside(edge, 1, b, 0)) for b in range(NB)]

    def step(blocks, n, state):
        rows = chunk_rows(C - 1 - n)
        out = []
        for b in blocks:
            first = k[PR, b, rows, :] + state[2 * b]
            last = state[2 * b + 1]
            na = k[NA, b, rows, :]
            weights[b, rows, :] = k[INV, b, rows, :] * (parts[b][0] * first + parts[b][1] * last)
            out += [na * first, na * last]
        return tuple(out)

    zero = jnp.zeros((8, 128), F32)
    return step, (zero, zero + 1.0) * NB


def spread(co, first, rows, before, after, edge, rhs=True):
    def at(s):
        return pl.ds(first * 8 + s, rows, stride=8)
    some = pl.ds(first, rows)
    nxt = after
    edge[1, at(7), :] = after
    edge[0, at(0), :] = before
    for s in range(7, 0, -1):
        e1, e2, m1, m2, e0, m0 = (co[s - 1, n, some, :] for n in range(5, 11))
        last = m1 * before + m2 * nxt
        nxt = e1 * before + e2 * nxt
        if rhs:
            last, nxt = m0 + last, e0 + nxt
        edge[0, at(s), :] = last
        edge[1, at(s - 1), :] = nxt


def forward(k, rhs_of, g, summ, blocks, unroll=UNROLL):
    zero = jnp.zeros((8, 128), F32)

    def step(blocks, t, state):
        out = []
        rows = chunk_rows(t)
        for j, b in enumerate(blocks):
            inv = k[INV, b, rows, :]
            na = k[NA, b, rows, :]
            pr = k[PR, b, rows, :]
            rhs = rhs_of(b, t)
            for f in range(F):
                last, first = state[2 * (j * F + f):2 * (j * F + f) + 2]
                last = inv * rhs[f] + na * last
                g[b, f, rows, :] = last
                out += [last, first + pr * last]
        return tuple(out)

    state = (zero,) * (2 * F * len(blocks))
    if unroll == C:
        for t in range(C):
            state = step(blocks, t, state)
    else:
        state = sweep(blocks, step, state, unroll)
    for j, b in enumerate(blocks):
        for f in range(F):
            summ[B0 * R + row_of(b, f)] = state[2 * (j * F + f)]
            summ[A0 * R + row_of(b, f)] = state[2 * (j * F + f) + 1]


def backward(kb, g, edge, put, turn):
    def start(b):
        return tuple(beside(edge, 1, b, f) for f in range(F))

    def stepper(b):
        near = [beside(edge, 0, b, f) for f in range(F)]

        def step(_, n, state):
            out = []
            rows = chunk_rows(C - 1 - n)
            v = kb[V, b, rows, :]
            nc = kb[NC, b, rows, :]
            for f in range(F):
                x = (g[b, f, rows, :] + v * near[f]) + nc * state[f]
                put(b, f, rows, x)
                out.append(x)
            return tuple(out)
        return step

    def alone(b, more=None, more_start=()):
        step = stepper(b)

        def step_all(blocks, n, state):
            state = step(blocks, n, state[:F]) + state[F:]
            return state if more is None else state[:F] + more(range(NB), n, state[F:])

        sweep(b, step_all, start(b) + more_start)

    def both(b, before):
        step = stepper(b)
        state = step(b, 0, start(b))
        for n in range(NB * F):
            turn(before, n)
            for m in range(4):
                state = step(b, 1 + 4 * n + m, state)

    def last(b):
        for n in range(NB * F):
            turn(b, n)

    return alone, both, last


def main_kernel(row_count, field, xl, xd, xu, yl, yd, yu, y, answer, ends,
                u, xk, xb, yn, yk, yb, r1, g, edge, sx, sy, cx, cy, pack, close, weights, dots, ends2, tilt,
                xcs, xcr, xrs, xrr, ycs, ycr, yrs, yrr,
                in_sem, field_sem, coef_sem, ps, pr, xcss, xcrs, xrss, xrrs, yss, yrsem):
    row = lax.axis_index("row")
    col = lax.axis_index("col")
    other = 1 - col
    lane = lax.broadcasted_iota(jnp.int32, (8, 128), 1)
    zero = jnp.zeros((8, 128), F32)
    src_block = (NB - 1) * other
    src_lane = 127 * other
    dst_lane = 127 * col

    def block(n):
        return n + col * (3 - 2 * n)

    def in_field(n):
        b = block(n)
        return [pltpu.make_async_copy(field.at[pl.ds(i * 128, 128), b],
                                      u.at[b, pl.ds((PAD + i * 128) * F, 128 * F)].reshape(128, F, 128), field_sem.at[n, i])
                for i in range(NB)]

    def in_coef(n):
        b = block(n)
        return [pltpu.make_async_copy(ref.at[:, pl.ds(pl.multiple_of(b * 128, 128), 128)], yn.at[i, b, pl.ds(PAD, T)], coef_sem.at[n, i])
                for i, ref in enumerate((yd, yl, yu))]

    in_x = [pltpu.make_async_copy(ref.at[:, pl.ds(b * 128, 128)], xk.at[n, b, pl.ds(PAD, T)], in_sem.at[n, b])
            for n, ref in enumerate((xd, xl, xu)) for b in range(NB)]

    def start(copies):
        for cp in copies:
            cp.start()

    def wait(copies):
        for cp in copies:
            cp.wait()

    start(in_field(3))

    barrier = pltpu.get_barrier_semaphore()
    for d in range(1, row_count):
        pl.semaphore_signal(barrier, inc=1, device_id={"row": lax.rem(row + d, row_count)}, device_id_type=MESH)
    pl.semaphore_signal(barrier, inc=1, device_id={"col": other}, device_id_type=MESH)

    for b in range(NB):
        for n in range(3):
            yn[n, b, 0:PAD, :] = zero
            xk[n, b, 0:PAD, :] = zero - 1.0 if n == LOW else zero
            yk[n, b, 0:PAD, :] = zero - 1.0 if n == LOW else zero
        for f in range(F):
            y[b, f, 0:PAD, :] = zero
    for b in range(NB):
        u[b, 0:PAD * F, :] = jnp.zeros((PAD * F, 128), F32)
    u[NB] = jnp.zeros((ROWS * F, 128), F32)

    def line_copies(send, recv, send_sem, recv_sem):
        return [pltpu.make_async_remote_copy(send, recv.at[d - 1], send_sem.at[d - 1], recv_sem.at[d - 1],
                                             device_id={"row": lax.rem(row + d, row_count)}, device_id_type=MESH)
                for d in range(1, row_count)]

    def to_line(*refs):
        copies = line_copies(*refs)
        for cp in copies:
            cp.start()
        return copies

    def to_pair(n, send, recv):
        cp = pltpu.make_async_remote_copy(send, recv, yss.at[n], yrsem.at[n], device_id={"col": other}, device_id_type=MESH)
        cp.start()
        return cp

    start(in_x)

    wait(in_field(3))
    start(in_field(0) + in_field(1) + in_coef(0))
    from_src = jnp.bitwise_and(lane - src_lane, 127)
    for h in range(2):
        acc = zero
        for p in range(128):
            w = PAD * F + 8 * (h * 128 + p)
            acc = jnp.where(from_src == p, pltpu.roll(u[src_block, w:w + 8, :], p, 1), acc)
        pack[0, h * 8:h * 8 + 8, :] = acc
    pl.semaphore_wait(barrier, row_count)
    column = pltpu.make_async_remote_copy(pack.at[0], pack.at[1], ps, pr, device_id={"col": other}, device_id_type=MESH)
    column.start()


    wait(in_x)
    start(in_field(2) + in_coef(1) + in_coef(2) + in_coef(3))
    factor(xk, xb, sx, 2.0)
    reduce_coef(sx, cx, xcs)
    coef_sends = to_line(xcs, xcr, xcss, xcrs)

    def stencil(b, t):
        rows = chunk_rows(t)
        cd = 1.0 - yn[DIAG, b, rows, :]
        cl = yn[LOW, b, rows, :]
        cu = yn[UPP, b, rows, :]
        left = lax.rem(b + NB, NB + 1)
        rhs = []
        for f in range(F):
            words = pl.ds(t * F + f, 8, stride=C * F)
            mid = u[b, words, :]
            prv = pltpu.roll(jnp.where(lane == 127, u[left, words, :], mid), 1, 1)
            nxt = pltpu.roll(jnp.where(lane == 0, u[b + 1, words, :], mid), 127, 1)
            v = (cd * mid - cl * prv) - cu * nxt
            r1[b, f, rows, :] = v
            rhs.append(v)
        return rhs

    halves = [col, other]

    def send_half(h):
        reduce_rhs(sx, cx, pl.multiple_of(halves[h] * H, 8), H, xrs.at[h])
        return to_line(xrs.at[h], xrr.at[h], xrss.at[h], xrrs.at[h])

    def eliminate(n, carry):
        wait(in_coef(n))

        @pl.when(n < 2)
        def _():
            wait(in_field(n + 1))

        @pl.when(n == 2)
        def _():
            send_half(0)

        @pl.when(n == 3)
        def _():
            column.wait()
            here = lane == dst_lane
            for i in range(2):
                got = pack[1, i * 8:i * 8 + 8, :]
                for p in range(128):
                    w = PAD * F + 8 * (i * 128 + p)
                    u[NB, w:w + 8, :] = jnp.where(here, pltpu.roll(got, (128 - p) % 128, 1), 0.0)

        forward(xk, stencil, g, sx, [block(n)], X_UNROLL)
        return carry

    wait(in_field(0))
    lax.fori_loop(0, NB, eliminate, 0)
    send_half(1)

    for b in range(NB):
        for c in range(NB):
            for n in range(3):
                yk[n, c, PAD + b * 128:PAD + b * 128 + 128, :] = yn[n, b, PAD + c * 128:PAD + c * 128 + 128, :].T
    factor(yk, yb, sy, 1)
    reduce_coef(sy, cy, ycs)
    y_coef = to_pair(0, ycs, ycr)
    weigh_step, weigh_start = weigh(yk, cy, jnp.where(col == 0, 0.0, 1.0), tilt, weights)
    dots[...] = jnp.zeros((R, 8, 128), F32)

    for cp in coef_sends:
        cp.wait()

    def coef_of(ref):
        return tuple(ref[q * R:q * R + R, :] for q in range(4))

    slots = range(row_count - 3, -1, -1)
    rest = coef_of(xcr.at[row_count - 2])
    known = []
    for n in slots:
        rest, part, _ = join_coef(*rest, *coef_of(xcr.at[n]))
        known += part
    p1, p2, q1, q2 = rest
    a1, a2, b1, b2 = (cx[7, n] for n in range(4))
    m12 = p1 * b1 + p2 * a1
    i11 = 1.0 / (1.0 - (p1 * b2 + p2 * a2))
    m21 = (q1 * b2 + q2 * a2) * i11
    i22 = 1.0 / ((1.0 - (q1 * b1 + q2 * a1)) - m21 * m12)
    for n, v in enumerate(known + [p1, p2, q1, q2, m12, m21, i11, i22]):
        close[n] = v

    def close_line(h):
        for cp in line_copies(xrs.at[h], xrr.at[h], xrss.at[h], xrrs.at[h]):
            cp.wait()
        first = pl.multiple_of(halves[h] * H, 8)
        known = [close[n, pl.ds(first, H), :] for n in range(5 * (row_count - 2) + 8)]

        def received(n):
            return xrr[h, n, 0:H, :], xrr[h, n, H:2 * H, :]

        p0, q0 = received(row_count - 2)
        for i, n in enumerate(slots):
            p0, q0, _, _ = join_rhs(known[5 * i:5 * i + 5], p0, q0, *received(n))
        p1, p2, q1, q2, m12, m21, i11, i22 = known[5 * (row_count - 2):]
        a0, b0 = xrs[h, 0:H, :], xrs[h, H:2 * H, :]
        s1 = (p0 + p1 * b0) + p2 * a0
        s2 = (q0 + q1 * b0) + q2 * a0
        before = i22 * (s2 + m21 * s1)
        spread(cx, first, H, before, i11 * (s1 + m12 * before), edge)

    def put_x(b, f, rows, x):
        r1[b, f, rows, :] = x - r1[b, f, rows, :]

    def turn_in(b, n):
        c, f = n // F, n % F
        rows = pl.ds(pl.multiple_of(PAD + b * 128, 8), 128)
        y[c, f, rows, :] = r1[b, f, PAD + c * 128:PAD + c * 128 + 128, :].T
        r = row_of(c, f)
        total = dots[r]
        for i in range(16):
            some = pl.ds(pl.multiple_of(PAD + b * 128 + i * 8, 8), 8)
            total = total + y[c, f, some, :] * weights[c, some, :]
        dots[r] = total

    alone, both, last = backward(xb, g, edge, put_x, turn_in)

    def solve(n, carry):
        @pl.when(n == 2)
        def _():
            close_line(1)

        both(block(n), block(n - 1))
        return carry

    close_line(0)
    alone(block(0), weigh_step, weigh_start)
    lax.fori_loop(1, NB, solve, 0)
    last(block(3))

    flat = dots.reshape(R * 8, 128)
    mine = flat[pl.ds(0, R, stride=8), :]
    for i in range(1, 8):
        mine = mine + flat[pl.ds(i, R, stride=8), :]
    yrs[...] = mine
    y_rhs = to_pair(1, yrs, yrr)

    def rhs_y(b, t):
        return [y[b, f, chunk_rows(t), :] for f in range(F)]

    forward(yk, rhs_y, g, sy, [0, 1])
    forward(yk, rhs_y, g, sy, [2, 3])
    reduce_rhs(sy, cy, 0, R, ends2)
    first = col == 0

    nothing = jnp.zeros((R, 128), F32)
    spread(cy, 0, R, nothing, nothing, edge)

    def put_y(b, f, rows, x):
        y[b, f, rows, :] = x

    alone, _, _ = backward(yb, g, edge, put_y, None)

    def solve_y(b, carry):
        alone(b)
        return carry

    lax.fori_loop(0, NB, solve_y, 0)
    one_left = jnp.where(first, 0.0, 1.0) + nothing
    spread(cy, 0, R, one_left, 1.0 - one_left, edge, False)
    near = [beside(edge, 0, b, 0) for b in range(NB)]

    def step_h(blocks, n, state):
        rows = chunk_rows(C - 1 - n)
        out = []
        for b in blocks:
            out.append(yb[V, b, rows, :] * near[b] + yb[NC, b, rows, :] * state[b])
            answer[b, rows, :] = out[b]
        return tuple(out)

    sweep(range(NB), step_h, tuple(beside(edge, 1, b, 0) for b in range(NB)))

    y_coef.wait()
    a1, b2 = cy[7, 0], cy[7, 3]
    c1, d2 = ycr[0:R, :], ycr[3 * R:4 * R, :]
    lb2 = jnp.where(first, b2, d2)
    ra1 = jnp.where(first, c1, a1)
    inv = 1.0 / (1.0 - lb2 * ra1)
    y_rhs.wait()
    mine = yrs[...]
    theirs = yrr[...]
    lb0 = jnp.where(first, mine, theirs)
    ra0 = jnp.where(first, theirs, mine)
    last_left = inv * (lb0 + lb2 * ra0)
    ends[...] = jnp.where(first, ra0 + ra1 * last_left, last_left)


def last_kernel(y, h, ends, out, o, out_sem):
    def copy_out(c, b):
        return pltpu.make_async_copy(o.at[b, pl.ds(pl.multiple_of(c * 128 * F, 8), 128 * F)].reshape(128, F, 128),
                                     out.at[pl.ds(c * 128, 128), b], out_sem.at[c, b])

    def turn_out(c, carry):
        for b in range(NB):
            part = h[c, PAD + b * 128:PAD + b * 128 + 128, :]
            for f in range(F):
                end = jnp.broadcast_to(ends[pl.ds(row_of(c, f), 1), :], (128, 128))
                o[b, pl.ds(c * 128 * F + f, 128, stride=F), :] = (
                    y[c, f, PAD + b * 128:PAD + b * 128 + 128, :] + part * end).T
            copy_out(c, b).start()
        return carry

    for c in range(NB):
        turn_out(c, 0)
    for c in range(NB):
        for b in range(NB):
            copy_out(c, b).wait()


def solution(mesh):
    row_count = mesh.shape["row"]
    field_spec = P(("batch", "row"), "col", None)
    coef_spec = P(("batch", "row"), "col")

    def local_step(field, x_lower, x_diag, x_upper, y_lower, y_diag, y_upper):
        words = field.reshape(T, NB, 128, F).transpose(0, 1, 3, 2)
        plane = (NB, ROWS, 128)
        fields = (NB, F, ROWS, 128)
        peers = row_count - 1
        in_vmem = pl.BlockSpec(memory_space=pltpu.VMEM)
        in_hbm = pl.BlockSpec(memory_space=pl.ANY)
        dma = pltpu.SemaphoreType.DMA
        parts = pl.pallas_call(
            functools.partial(main_kernel, row_count),
            out_shape=[pltpu.VMEM(fields, F32), pltpu.VMEM(plane, F32), pltpu.VMEM((R, 128), F32)],
            in_specs=[in_hbm] * 7,
            out_specs=[in_vmem] * 3,
            scratch_shapes=[
                pltpu.VMEM((NB + 1, ROWS * F, 128), F32),
                pltpu.VMEM((3,) + plane, F32),
                pltpu.VMEM((2,) + plane, F32),
                pltpu.VMEM((3,) + plane, F32),
                pltpu.VMEM((3,) + plane, F32),
                pltpu.VMEM((2,) + plane, F32),
                pltpu.VMEM(fields, F32),
                pltpu.VMEM(fields, F32),
                pltpu.VMEM((2, R * 8, 128), F32),
                pltpu.VMEM((6 * R, 8, 128), F32),
                pltpu.VMEM((6 * R, 8, 128), F32),
                pltpu.VMEM((8, 11, R, 128), F32),
                pltpu.VMEM((8, 11, R, 128), F32),
                pltpu.VMEM((2, 16, 128), F32),
                pltpu.VMEM((5 * (row_count - 2) + 8, R, 128), F32),
                pltpu.VMEM(plane, F32),
                pltpu.VMEM((R, 8, 128), F32),
                pltpu.VMEM((2 * R, 128), F32),
                pltpu.VMEM((2, R * 8, 128), F32),
                pltpu.VMEM((4 * R, 128), F32),
                pltpu.VMEM((peers, 4 * R, 128), F32),
                pltpu.VMEM((2, R, 128), F32),
                pltpu.VMEM((2, peers, R, 128), F32),
                pltpu.VMEM((4 * R, 128), F32),
                pltpu.VMEM((4 * R, 128), F32),
                pltpu.VMEM((R, 128), F32),
                pltpu.VMEM((R, 128), F32),
                dma((3, NB)), dma((NB, NB)), dma((NB, 3)), dma, dma, dma((peers,)), dma((peers,)), dma((2, peers)), dma((2, peers)), dma((2,)), dma((2,)),
            ],
            compiler_params=pltpu.CompilerParams(
                collective_id=0, has_side_effects=True, vmem_limit_bytes=58 << 20),
        )(words, x_lower, x_diag, x_upper, y_lower, y_diag, y_upper)
        solved = pl.pallas_call(
            last_kernel,
            out_shape=jax.ShapeDtypeStruct((T, NB, F, 128), F32),
            in_specs=[in_vmem] * 3,
            out_specs=in_hbm,
            scratch_shapes=[pltpu.VMEM((NB, T * F, 128), F32), dma((NB, NB))],
            compiler_params=pltpu.CompilerParams(vmem_limit_bytes=16 << 20),
        )(*parts)
        return solved.transpose(0, 1, 3, 2).reshape(T, T, F)

    return jax.shard_map(local_step, mesh=mesh, in_specs=(field_spec,) + (coef_spec,) * 6,
                         out_specs=field_spec, check_vma=False)
```
